8 devices in a mesh: dp: 2 (over z, y), sp: 4 (over x, core).
Axes of the slice: x: 2, y: 2, z: 1, core: 2. Of those that a mesh axis runs over, the one named last changes fastest.
Arguments:
- x_in: bfloat16 [6144, 1536], P(('dp', 'sp')), parts along dimension 0
- seg_ids: int32 [6144], P(('dp', 'sp')), parts along dimension 0
- norm_gains: float32 [4, 1536], replicated
- w_in: bfloat16 [1536, 6448], replicated
- ssm_head: float32 [3, 48], replicated
- y_gain: float32 [3072], replicated
- w_out: bfloat16 [3072, 1536], replicated
- mlp_up: bfloat16 [2, 1536, 12288], replicated
- mlp_down: bfloat16 [2, 6144, 1536], replicated
- w_qkv: bfloat16 [1536, 36, 128], replicated
- w_attn_out: bfloat16 [12, 128, 1536], replicated
Outputs:
- output: bfloat16 [6144, 1536], P(('dp', 'sp')), parts along dimension 0
There are 2 independent parts. The reference program is written for one: setup_inputs(seed, part) draws one part's arguments, and reference() takes and returns one part's arrays. A program takes and returns all parts, laid end to end along the dimension named above; an argument that names none is the same for every part.
All inputs are finite; a program needn't handle non-finite values.
Results may differ from the reference program's by a relative error of at most 0.017019.
Values are sent between devices in bfloat16 or wider.
A program may use at most 1 GiB of HBM per device.

```python
import jax
import jax.numpy as jnp
from jax import lax

D_MODEL = 1536
SSM_HEADS = 48
SSM_HEADDIM = 64
D_STATE = 128
Q_HEADS = 12
KV_HEADS = 12
HEAD_DIM = 128
FF_DIM = 6144
TOKENS_DEV = 768
GROUP_SIZE = 4
DOC_CUTS = 4
CHUNK = 64
QUERY_BLOCK = 16
NORM_EPS = 1e-6
ROPE_BASE = 10000.0
SEQ_LEN = TOKENS_DEV * GROUP_SIZE
INNER_DIM = SSM_HEADS * SSM_HEADDIM
IN_WIDTH = 2 * INNER_DIM + 2 * D_STATE + SSM_HEADS
GQA_GROUP = Q_HEADS // KV_HEADS
BC_SCALE = (TOKENS_DEV / D_STATE) ** 0.25
OUT_SCALE = (Q_HEADS * HEAD_DIM) ** -0.5 * TOKENS_DEV ** 0.5 * 0.25


def draw_segments(seg_key):
    cut_order = jax.random.permutation(seg_key, SEQ_LEN - 1)
    starts = jnp.zeros((SEQ_LEN,), jnp.int32).at[cut_order[:DOC_CUTS] + 1].set(1)
    return jnp.cumsum(starts).astype(jnp.int32)


def setup_inputs(seed: int = 0, part: int = 0) -> dict:
    base_key = jax.random.key(seed)
    shared = jax.random.split(base_key, 12)
    own = jax.random.split(jax.random.fold_in(base_key, part), 2)
    x_in = jax.random.normal(own[0], (SEQ_LEN, D_MODEL), jnp.float32).astype(jnp.bfloat16)
    seg_ids = draw_segments(own[1])
    norm_gains = jax.random.uniform(shared[0], (4, D_MODEL), jnp.float32, 0.5, 1.5)
    col_scale = jnp.concatenate([jnp.full((2 * INNER_DIM,), 1.0, jnp.float32), jnp.full((2 * D_STATE,), BC_SCALE, jnp.float32), jnp.full((SSM_HEADS,), 0.5, jnp.float32)]) * D_MODEL ** -0.5
    w_in = (jax.random.normal(shared[1], (D_MODEL, IN_WIDTH), jnp.float32) * col_scale).astype(jnp.bfloat16)
    dt_mean = jax.random.uniform(shared[2], (SSM_HEADS,), jnp.float32, 1.0, 3.0) / TOKENS_DEV
    a_rate = -jax.random.uniform(shared[3], (SSM_HEADS,), jnp.float32, 0.1, 0.4)
    d_skip = jax.random.uniform(shared[4], (SSM_HEADS,), jnp.float32, 0.5, 1.5)
    ssm_head = jnp.stack([jnp.log(dt_mean), a_rate, d_skip])
    y_gain = jax.random.uniform(shared[5], (INNER_DIM,), jnp.float32, 0.5, 1.5)
    w_out = (jax.random.normal(shared[6], (INNER_DIM, D_MODEL), jnp.float32) * INNER_DIM ** -0.5).astype(jnp.bfloat16)
    mlp_up = (jax.random.normal(shared[7], (2, D_MODEL, 2 * FF_DIM), jnp.float32) * D_MODEL ** -0.5).astype(jnp.bfloat16)
    mlp_down = (jax.random.normal(shared[8], (2, FF_DIM, D_MODEL), jnp.float32) * FF_DIM ** -0.5).astype(jnp.bfloat16)
    w_qkv = (jax.random.normal(shared[9], (D_MODEL, Q_HEADS + 2 * KV_HEADS, HEAD_DIM), jnp.float32) * D_MODEL ** -0.5).astype(jnp.bfloat16)
    w_attn_out = (jax.random.normal(shared[10], (Q_HEADS, HEAD_DIM, D_MODEL), jnp.float32) * OUT_SCALE).astype(jnp.bfloat16)
    return {'x_in': x_in, 'seg_ids': seg_ids, 'norm_gains': norm_gains, 'w_in': w_in, 'ssm_head': ssm_head, 'y_gain': y_gain, 'w_out': w_out, 'mlp_up': mlp_up, 'mlp_down': mlp_down, 'w_qkv': w_qkv, 'w_attn_out': w_attn_out}


def rms_norm(values, norm_gain):
    vals32 = values.astype(jnp.float32)
    inv_rms = lax.rsqrt(jnp.mean(vals32 * vals32, axis=-1, keepdims=True) + NORM_EPS)
    return (vals32 * inv_rms * norm_gain).astype(jnp.bfloat16)


def swiglu_mlp(hidden, w_up, w_down):
    gate_up = jnp.dot(hidden, w_up, preferred_element_type=jnp.float32)
    act_vals = (jax.nn.silu(gate_up[:, :FF_DIM]) * gate_up[:, FF_DIM:]).astype(jnp.bfloat16)
    return jnp.dot(act_vals, w_down, preferred_element_type=jnp.float32)


def apply_rope(values, positions):
    half_dim = HEAD_DIM // 2
    inv_freq = ROPE_BASE ** (-jnp.arange(half_dim, dtype=jnp.float32) * 2.0 / HEAD_DIM)
    rot_angle = positions[:, None] * inv_freq[None, :]
    cos_part = jnp.cos(rot_angle)[:, None, :]
    sin_part = jnp.sin(rot_angle)[:, None, :]
    first_half = values[..., :half_dim]
    second_half = values[..., half_dim:]
    return jnp.concatenate([first_half * cos_part - second_half * sin_part, second_half * cos_part + first_half * sin_part], axis=-1)


def reference(x_in, seg_ids, norm_gains, w_in, ssm_head, y_gain, w_out, mlp_up, mlp_down, w_qkv, w_attn_out):
    proj_out = jnp.dot(rms_norm(x_in, norm_gains[0]), w_in, preferred_element_type=jnp.float32)
    x_ssm = proj_out[:, :INNER_DIM].astype(jnp.bfloat16)
    z_gate = proj_out[:, INNER_DIM:2 * INNER_DIM]
    b_in = proj_out[:, 2 * INNER_DIM:2 * INNER_DIM + D_STATE].astype(jnp.bfloat16)
    c_out = proj_out[:, 2 * INNER_DIM + D_STATE:2 * INNER_DIM + 2 * D_STATE].astype(jnp.bfloat16)
    dt_step = jax.nn.softplus(proj_out[:, 2 * INNER_DIM + 2 * D_STATE:] + ssm_head[0])
    a_neg = ssm_head[1]
    d_skip = ssm_head[2]
    n_chunks = SEQ_LEN // CHUNK
    step_ids = jnp.arange(CHUNK)
    lower_tri = step_ids[:, None] >= step_ids[None, :]

    def ssd_step(run_state, chunk_in):
        ssm_state, prev_seg = run_state
        x_chunk, b_chunk, c_chunk, dt_chunk, seg_chunk = chunk_in
        cum_decay = jnp.cumsum(dt_chunk * a_neg, axis=0)
        visible = (seg_chunk[:, None] == seg_chunk[None, :]) & lower_tri
        pair_decay = jnp.where(visible[:, :, None], jnp.exp(jnp.minimum(cum_decay[:, None, :] - cum_decay[None, :, :], 0.0)), 0.0)
        cb_scores = jnp.dot(c_chunk, b_chunk.T, preferred_element_type=jnp.float32)
        mix_weights = (cb_scores[:, :, None] * pair_decay * dt_chunk[None, :, :]).astype(jnp.bfloat16)
        x_wide = x_chunk.astype(jnp.float32)
        y_intra = jnp.einsum('tsh,shp->thp', mix_weights.astype(jnp.float32), x_wide)
        carry_in = jnp.where((seg_chunk == prev_seg)[:, None], jnp.exp(cum_decay), 0.0)
        state_low = ssm_state.astype(jnp.bfloat16).astype(jnp.float32)
        y_carry = jnp.einsum('tn,hpn->thp', c_chunk.astype(jnp.float32), state_low) * carry_in[:, :, None]
        last_seg = seg_chunk[CHUNK - 1]
        end_weight = jnp.where((seg_chunk == last_seg)[:, None], jnp.exp(cum_decay[CHUNK - 1][None, :] - cum_decay), 0.0) * dt_chunk
        x_weighted = (x_wide * end_weight[:, :, None]).astype(jnp.bfloat16)
        chunk_state = jnp.einsum('shp,sn->hpn', x_weighted.astype(jnp.float32), b_chunk.astype(jnp.float32))
        chunk_decay = jnp.where(last_seg == prev_seg, jnp.exp(cum_decay[CHUNK - 1]), 0.0)
        new_state = chunk_decay[:, None, None] * ssm_state + chunk_state
        y_chunk = y_intra + y_carry + d_skip[:, None] * x_wide
        return (new_state, last_seg), y_chunk

    chunk_inputs = (x_ssm.reshape(n_chunks, CHUNK, SSM_HEADS, SSM_HEADDIM), b_in.reshape(n_chunks, CHUNK, D_STATE), c_out.reshape(n_chunks, CHUNK, D_STATE), dt_step.reshape(n_chunks, CHUNK, SSM_HEADS), seg_ids.reshape(n_chunks, CHUNK))
    init_state = (jnp.zeros((SSM_HEADS, SSM_HEADDIM, D_STATE), jnp.float32), jnp.array(-1, jnp.int32))
    final_state, y_chunks = lax.scan(ssd_step, init_state, chunk_inputs)
    y_all = y_chunks.reshape(SEQ_LEN, INNER_DIM)
    inv_rms = lax.rsqrt(jnp.mean(y_all * y_all, axis=-1, keepdims=True) + NORM_EPS)
    gated_y = (y_all * inv_rms * y_gain * jax.nn.silu(z_gate)).astype(jnp.bfloat16)
    x_one = (x_in.astype(jnp.float32) + jnp.dot(gated_y, w_out, preferred_element_type=jnp.float32)).astype(jnp.bfloat16)
    x_two = (x_one.astype(jnp.float32) + swiglu_mlp(rms_norm(x_one, norm_gains[1]), mlp_up[0], mlp_down[0])).astype(jnp.bfloat16)
    qkv_flat = jnp.dot(rms_norm(x_two, norm_gains[2]), w_qkv.reshape(D_MODEL, (Q_HEADS + 2 * KV_HEADS) * HEAD_DIM), preferred_element_type=jnp.float32)
    qkv_all = qkv_flat.reshape(SEQ_LEN, Q_HEADS + 2 * KV_HEADS, HEAD_DIM)
    positions = jnp.arange(SEQ_LEN).astype(jnp.float32)
    q_rot = apply_rope(qkv_all[:, :Q_HEADS], positions).astype(jnp.bfloat16)
    k_rot = apply_rope(qkv_all[:, Q_HEADS:Q_HEADS + KV_HEADS], positions).astype(jnp.bfloat16)
    v_all = qkv_all[:, Q_HEADS + KV_HEADS:].astype(jnp.bfloat16)
    k_wide = k_rot.astype(jnp.float32)
    v_wide = v_all.astype(jnp.float32)
    key_pos = jnp.arange(SEQ_LEN)
    n_qblocks = SEQ_LEN // QUERY_BLOCK
    q_blocks = q_rot.reshape(n_qblocks, QUERY_BLOCK, KV_HEADS, GQA_GROUP, HEAD_DIM)
    seg_blocks = seg_ids.reshape(n_qblocks, QUERY_BLOCK)
    pos_blocks = key_pos.reshape(n_qblocks, QUERY_BLOCK)
    qk_scale = HEAD_DIM ** -0.5

    def attend(q_inputs):
        q_block, seg_q, pos_q = q_inputs
        scores = jnp.einsum('qkgd,skd->kgqs', q_block.astype(jnp.float32), k_wide) * qk_scale
        allowed = (seg_q[:, None] == seg_ids[None, :]) & (key_pos[None, :] <= pos_q[:, None])
        masked = jnp.where(allowed, scores, -jnp.inf)
        row_max = jnp.max(masked, axis=-1, keepdims=True)
        exp_scores = jnp.exp(masked - row_max)
        row_sum = jnp.sum(exp_scores, axis=-1)
        attn_vals = jnp.einsum('kgqs,skd->qkgd', exp_scores.astype(jnp.bfloat16).astype(jnp.float32), v_wide)
        return (attn_vals / jnp.transpose(row_sum, (2, 0, 1))[..., None]).astype(jnp.bfloat16)

    attn_all = lax.map(attend, (q_blocks, seg_blocks, pos_blocks)).reshape(SEQ_LEN, Q_HEADS * HEAD_DIM)
    attn_res = jnp.dot(attn_all, w_attn_out.reshape(Q_HEADS * HEAD_DIM, D_MODEL), preferred_element_type=jnp.float32)
    x_three = (x_two.astype(jnp.float32) + attn_res).astype(jnp.bfloat16)
    x_four = (x_three.astype(jnp.float32) + swiglu_mlp(rms_norm(x_three, norm_gains[3]), mlp_up[1], mlp_down[1])).astype(jnp.bfloat16)
    return x_four
```

```python
import functools
import math

import jax
import jax.numpy as jnp
from jax import lax
from jax.experimental import pallas as pl
from jax.experimental.pallas import tpu as pltpu
from jax.sharding import PartitionSpec as P

CHUNK = 64
NORM_EPS = 1e-6
ROPE_BASE = 10000.0
F32 = jnp.float32
BF16 = jnp.bfloat16
VMEM_LIMIT = 60 * 1024 * 1024
NT = (((1,), (1,)), ((), ()))
TN = (((0,), (0,)), ((), ()))


def dot(a, b, dims=(((1,), (0,)), ((), ()))):
    return lax.dot_general(a, b, dims, preferred_element_type=F32)


def params(sem):
    return pltpu.CompilerParams(dimension_semantics=sem, vmem_limit_bytes=VMEM_LIMIT)


def cost(flops, bytes_accessed, trans=0):
    return pl.CostEstimate(flops=int(flops), bytes_accessed=int(bytes_accessed), transcendentals=int(trans))


def norm_rows(values, gain):
    wide = values.astype(F32)
    inv = lax.rsqrt(jnp.mean(wide * wide, axis=-1, keepdims=True) + NORM_EPS)
    return (wide * inv * gain).astype(BF16)


def full_spec(shape):
    zeros = (0,) * len(shape)
    return pl.BlockSpec(shape, lambda *_: zeros)


def in_proj_kernel(n_heads, x_ref, gain_ref, w_ref, bias_ref, rate_ref, h_ref, xs_ref, bc_ref, dt_ref, cum_ref):
    step = pl.program_id(0)

    @pl.when(step == 0)
    def _():
        hid = norm_rows(x_ref[...], gain_ref[...])
        h_ref[...] = hid
        out = dot(hid, w_ref[...], NT)
        n_bc = bc_ref.shape[1]
        bc_ref[...] = out[:, :n_bc].astype(BF16)
        lanes = dt_ref.shape[1]
        raw = out[:, n_bc:n_bc + lanes] + bias_ref[...]
        dt = jnp.maximum(raw, 0.0) + jnp.log1p(jnp.exp(-jnp.abs(raw)))
        lane = lax.broadcasted_iota(jnp.int32, dt.shape, 1)
        dt = jnp.where(lane < n_heads, dt, 0.0)
        dt_ref[...] = dt
        cum = dt * rate_ref[...]
        row = lax.broadcasted_iota(jnp.int32, dt.shape, 0) % CHUNK
        shift = 1
        while shift < CHUNK:
            cum = cum + jnp.where(row >= shift, pltpu.roll(cum, shift, 0), 0.0)
            shift *= 2
        cum_ref[...] = cum

    @pl.when(step > 0)
    def _():
        xs_ref[...] = dot(h_ref[...], w_ref[...], NT).astype(BF16)


def in_proj(x_rows, gain, w_in_t, bias, rate, inner, n_heads):
    tokens, dim = x_rows.shape
    tile = 512
    n_x = inner // tile
    last = 2 * inner // tile
    out_shape = (
        jax.ShapeDtypeStruct((tokens, dim), BF16),
        jax.ShapeDtypeStruct((tokens, inner), BF16),
        jax.ShapeDtypeStruct((tokens, 256), BF16),
        jax.ShapeDtypeStruct((tokens, 128), F32),
        jax.ShapeDtypeStruct((tokens, 128), F32),
    )
    return pl.pallas_call(
        functools.partial(in_proj_kernel, n_heads),
        grid=(n_x + 1,),
        in_specs=[
            full_spec((tokens, dim)),
            full_spec((1, dim)),
            pl.BlockSpec((tile, dim), lambda i: (jnp.where(i == 0, last, i - 1), 0)),
            full_spec((1, 128)),
            full_spec((1, 128)),
        ],
        out_specs=(
            full_spec((tokens, dim)),
            pl.BlockSpec((tokens, tile), lambda i: (0, jnp.maximum(i - 1, 0))),
            full_spec((tokens, 256)),
            full_spec((tokens, 128)),
            full_spec((tokens, 128)),
        ),
        out_shape=out_shape,
        compiler_params=params(("arbitrary",)),
        cost_estimate=cost(2 * tokens * dim * (inner + tile), 16e6),
        name="in_proj",
    )(x_rows, gain, w_in_t, bias, rate)


def z_proj_kernel(h_ref, w_ref, z_ref):
    z_ref[...] = dot(h_ref[...], w_ref[...], NT)


def z_proj(hid, w_in_t, inner):
    tokens, dim = hid.shape
    tile = 512
    first = inner // tile
    return pl.pallas_call(
        z_proj_kernel,
        grid=(inner // tile,),
        in_specs=[full_spec((tokens, dim)), pl.BlockSpec((tile, dim), lambda i: (i + first, 0))],
        out_specs=pl.BlockSpec((tokens, tile), lambda i: (0, i)),
        out_shape=jax.ShapeDtypeStruct((tokens, inner), F32),
        compiler_params=params(("arbitrary",)),
        cost_estimate=cost(2 * tokens * dim * inner, 21e6),
        name="z_proj",
    )(hid, w_in_t)


def head_lanes(cols, first, width):
    rows = cols.shape[0]
    lane = lax.broadcasted_iota(jnp.int32, (rows, 128), 1)
    parts = []
    for k in range(width // 128):
        left = jnp.broadcast_to(cols[:, first + 2 * k:first + 2 * k + 1], (rows, 128))
        right = jnp.broadcast_to(cols[:, first + 2 * k + 1:first + 2 * k + 2], (rows, 128))
        parts.append(jnp.where(lane < 64, left, right))
    return jnp.concatenate(parts, axis=1)


def chunk_weights(dt, cum, rel):
    last_rel = rel[CHUNK - 1:CHUNK, :]
    pos = lax.broadcasted_iota(jnp.int32, cum.shape, 0)
    last_cum = cum[CHUNK - 1:CHUNK, :]
    end_w = jnp.where(pos >= last_rel, jnp.exp(last_cum - cum), 0.0) * dt
    carry = jnp.where(rel < 0, jnp.exp(cum), 0.0)
    return end_w, carry


def state_step(state_ref, cols, xg, bt, end_w, dec_row, first):
    xw = (xg.astype(F32) * head_lanes(end_w, first, xg.shape[1])).astype(BF16)
    state_ref[:, cols] = dec_row * state_ref[:, cols] + dot(bt, xw)


def ssd_state_kernel(x_ref, bc_ref, dt_ref, cum_ref, rel_ref, end_ref, decay_ref):
    step = pl.program_id(0)

    @pl.when(step == 0)
    def _():
        end_ref[...] = jnp.zeros_like(end_ref)
        decay_ref[...] = jnp.ones_like(decay_ref)

    end_w, carry = chunk_weights(dt_ref[...], cum_ref[...], rel_ref[...])
    bt = bc_ref[:, :128].astype(F32).T.astype(BF16)
    for g in range(x_ref.shape[1] // 256):
        cols = slice(g * 256, (g + 1) * 256)
        dec_row = head_lanes(carry[CHUNK - 8:, :], 4 * g, 256)[7:8]
        state_step(end_ref, cols, x_ref[:, cols], bt, end_w, dec_row, 4 * g)
        decay_ref[:, cols] = decay_ref[:, cols] * dec_row


def ssd_state(xs, bc, dt, cum, rel):
    tokens, inner = xs.shape
    row = lambda width: pl.BlockSpec((CHUNK, width), lambda i: (i, 0))
    return pl.pallas_call(
        ssd_state_kernel,
        grid=(tokens // CHUNK,),
        in_specs=[row(inner), row(256), row(128), row(128), row(128)],
        out_specs=(full_spec((128, inner)), full_spec((1, inner))),
        out_shape=(jax.ShapeDtypeStruct((128, inner), F32), jax.ShapeDtypeStruct((1, inner), F32)),
        compiler_params=params(("arbitrary",)),
        cost_estimate=cost(2 * tokens * 256 * inner, 8e6),
        name="ssd_state",
    )(xs, bc, dt, cum, rel)


def ssd_full_kernel(x_ref, bc_ref, dt_ref, cum_ref, rel_ref, pack_ref, z_ref, hin_ref, skip_ref, gain_ref, out_ref, state_ref, y_ref):
    step = pl.program_id(0)

    @pl.when(step == 0)
    def _():
        state_ref[...] = hin_ref[...]

    inner = x_ref.shape[1]
    cum = cum_ref[...]
    rel = rel_ref[...]
    end_w, carry = chunk_weights(dt_ref[...], cum, rel)
    b_blk = bc_ref[:, :128]
    c_blk = bc_ref[:, 128:]
    bt = b_blk.astype(F32).T.astype(BF16)
    row_id = lax.broadcasted_iota(jnp.int32, (CHUNK, 128), 0)
    lane_id = lax.broadcasted_iota(jnp.int32, (CHUNK, 128), 1)
    src = jnp.where(lane_id < 64, lane_id, lane_id - 64)
    visible = (src >= rel) & (src <= row_id)
    scores = dot(c_blk, jnp.concatenate([b_blk, b_blk], axis=0), NT)
    scores = jnp.where(visible, scores, 0.0)
    blk_row = lax.broadcasted_iota(jnp.int32, (256, 256), 0) // 64
    blk_col = lax.broadcasted_iota(jnp.int32, (256, 256), 1) // 64
    diag = blk_row == blk_col
    n_pairs = inner // 128
    sumsq = jnp.zeros((CHUNK, 128), F32)
    for g in range(inner // 256):
        cols = slice(g * 256, (g + 1) * 256)
        xg = x_ref[:, cols]
        carry_x = head_lanes(carry, 4 * g, 256)
        cum_x = head_lanes(cum, 4 * g, 256)
        mixes = []
        for k in range(2):
            pair = 2 * g + k
            cum_s = pack_ref[0, pair:pair + 1, :]
            dt_s = pack_ref[0, n_pairs + pair:n_pairs + pair + 1, :]
            decay = jnp.exp(jnp.minimum(cum_x[:, k * 128:(k + 1) * 128] - cum_s, 0.0))
            mixes.append((scores * decay * dt_s).astype(BF16))
        mix = jnp.concatenate(mixes, axis=1)
        x_diag = jnp.where(diag, jnp.concatenate([xg, xg, xg, xg], axis=0), jnp.zeros((), BF16))
        y_in = dot(mix, x_diag)
        y_carry = dot(c_blk, state_ref[:, cols].astype(BF16)) * carry_x
        y = y_in + skip_ref[:, cols] * xg.astype(F32) + y_carry
        y_ref[:, cols] = y
        sq = y * y
        sumsq = sumsq + sq[:, :128] + sq[:, 128:]
        state_step(state_ref, cols, xg, bt, end_w, carry_x[CHUNK - 1:CHUNK, :], 4 * g)
    inv = lax.rsqrt(jnp.sum(sumsq, axis=-1, keepdims=True) * (1.0 / inner) + NORM_EPS)
    for g in range(inner // 512):
        cols = slice(g * 512, (g + 1) * 512)
        z = z_ref[:, cols]
        out_ref[:, cols] = (y_ref[:, cols] * inv * gain_ref[:, cols] * (z * jax.nn.sigmoid(z))).astype(BF16)


def ssd_full(xs, bc, dt, cum, rel, pack, z, h_in, skip, gain):
    tokens, inner = xs.shape
    row = lambda width: pl.BlockSpec((CHUNK, width), lambda i: (i, 0))
    return pl.pallas_call(
        ssd_full_kernel,
        grid=(tokens // CHUNK,),
        in_specs=[
            row(inner), row(256), row(128), row(128), row(128),
            pl.BlockSpec((1, pack.shape[1], 128), lambda i: (i, 0, 0)),
            row(inner), full_spec((128, inner)), full_spec((1, inner)), full_spec((1, inner)),
        ],
        out_specs=row(inner),
        out_shape=jax.ShapeDtypeStruct((tokens, inner), BF16),
        scratch_shapes=[pltpu.VMEM((128, inner), F32), pltpu.VMEM((CHUNK, inner), F32)],
        compiler_params=params(("arbitrary",)),
        cost_estimate=cost(12e9, 20e6),
        name="ssd_full",
    )(xs, bc, dt, cum, rel, pack, z, h_in, skip, gain)


def proj_add_kernel(a_ref, w_ref, res_ref, out_ref):
    out_ref[...] = (res_ref[...].astype(F32) + dot(a_ref[...], w_ref[...])).astype(BF16)


def proj_add(a, w, res):
    tokens, depth = a.shape
    dim = w.shape[1]
    tile = 256
    col = lambda rows: pl.BlockSpec((rows, tile), lambda i: (0, i))
    return pl.pallas_call(
        proj_add_kernel,
        grid=(dim // tile,),
        in_specs=[full_spec((tokens, depth)), col(depth), col(tokens)],
        out_specs=col(tokens),
        out_shape=jax.ShapeDtypeStruct((tokens, dim), BF16),
        compiler_params=params(("arbitrary",)),
        cost_estimate=cost(2 * tokens * depth * dim, 2 * (tokens * depth + depth * dim + 2 * tokens * dim)),
        name="proj_add",
    )(a, w, res)


def mlp_kernel(x_ref, gain_ref, wg_ref, wu_ref, wd_ref, out_ref, h_ref, acc_ref):
    step = pl.program_id(0)

    @pl.when(step == 0)
    def _():
        h_ref[...] = norm_rows(x_ref[...], gain_ref[...])
        acc_ref[...] = jnp.zeros_like(acc_ref)

    hid = h_ref[...]
    gate = dot(hid, wg_ref[0])
    up = dot(hid, wu_ref[0])
    act = (gate * jax.nn.sigmoid(gate) * up).astype(BF16)
    acc_ref[...] += dot(act, wd_ref[0])

    @pl.when(step == pl.num_programs(0) - 1)
    def _():
        out_ref[...] = (x_ref[...].astype(F32) + acc_ref[...]).astype(BF16)


def mlp(x_rows, gain, mlp_up, mlp_down, layer):
    tokens, dim = x_rows.shape
    ff = mlp_down.shape[1]
    tile = 512
    n_ff = ff // tile
    return pl.pallas_call(
        mlp_kernel,
        grid=(n_ff,),
        in_specs=[
            full_spec((tokens, dim)),
            full_spec((1, dim)),
            pl.BlockSpec((1, dim, tile), lambda i: (layer, 0, i)),
            pl.BlockSpec((1, dim, tile), lambda i: (layer, 0, i + n_ff)),
            pl.BlockSpec((1, tile, dim), lambda i: (layer, i, 0)),
        ],
        out_specs=full_spec((tokens, dim)),
        out_shape=jax.ShapeDtypeStruct((tokens, dim), BF16),
        scratch_shapes=[pltpu.VMEM((tokens, dim), BF16), pltpu.VMEM((tokens, dim), F32)],
        compiler_params=params(("arbitrary",)),
        cost_estimate=cost(6 * tokens * dim * ff, 6 * dim * ff),
        name="mlp",
    )(x_rows, gain, mlp_up, mlp_up, mlp_down)


def rope_tables(positions, head_dim):
    half = head_dim // 2
    inv_freq = ROPE_BASE ** (-jnp.arange(half, dtype=F32) * 2.0 / head_dim)
    angle = positions[:, None] * inv_freq[None, :]
    cos, sin = jnp.cos(angle), jnp.sin(angle)
    return jnp.concatenate([cos, cos], axis=1), jnp.concatenate([-sin, sin], axis=1)


def qkv_kernel(n_q, n_rot, x_ref, gain_ref, cos_ref, sin_ref, w_ref, *refs):
    h_ref = refs[-1]
    kv_ref = refs[-2]
    step = pl.program_id(0)

    @pl.when(step == 0)
    def _():
        h_ref[...] = norm_rows(x_ref[...], gain_ref[...])

    heads, _, head_dim = w_ref.shape
    w_all = jnp.concatenate([w_ref[k] for k in range(heads)], axis=1)
    out = dot(h_ref[...], w_all)

    def rotated(k):
        val = out[:, k * head_dim:(k + 1) * head_dim]
        return (val * cos_ref[...] + pltpu.roll(val, head_dim // 2, 1) * sin_ref[...]).astype(BF16)

    if n_q:
        @pl.when(step < n_q)
        def _():
            for k in range(heads):
                refs[0][k] = rotated(k)

    @pl.when((step >= n_q) & (step < n_rot))
    def _():
        for k in range(heads):
            kv_ref[k] = rotated(k)

    @pl.when(step >= n_rot)
    def _():
        for k in range(heads):
            kv_ref[k] = out[:, k * head_dim:(k + 1) * head_dim].astype(BF16)


def qkv_proj(x_rows, gain, cos, sin, w_heads, n_query, with_q):
    tokens, dim = x_rows.shape
    n_heads, _, head_dim = w_heads.shape
    n_kv = n_heads - n_query
    per = 4
    n_q = n_query // per if with_q else 0
    skip = 0 if with_q else n_query // per
    n_rot = n_q + n_kv // 2 // per
    steps = n_heads // per - skip
    out_specs = [pl.BlockSpec((per, tokens, head_dim), lambda i: (jnp.maximum(i - n_q, 0), 0, 0))]
    out_shape = [jax.ShapeDtypeStruct((n_kv, tokens, head_dim), BF16)]
    if with_q:
        out_specs.insert(0, pl.BlockSpec((per, tokens, head_dim), lambda i: (jnp.minimum(i, n_q - 1), 0, 0)))
        out_shape.insert(0, jax.ShapeDtypeStruct((n_query, tokens, head_dim), BF16))
    return pl.pallas_call(
        functools.partial(qkv_kernel, n_q, n_rot),
        grid=(steps,),
        in_specs=[
            full_spec((tokens, dim)), full_spec((1, dim)), full_spec((tokens, head_dim)), full_spec((tokens, head_dim)),
            pl.BlockSpec((per, dim, head_dim), lambda i: (i + skip, 0, 0)),
        ],
        out_specs=tuple(out_specs),
        out_shape=tuple(out_shape),
        scratch_shapes=[pltpu.VMEM((tokens, dim), BF16)],
        compiler_params=params(("arbitrary",)),
        cost_estimate=cost(2 * tokens * dim * steps * per * head_dim, 2 * dim * steps * per * head_dim + 8e6),
        name="qkv" if with_q else "kv",
    )(x_rows, gain, cos, sin, w_heads)


BLOCK_Q = 256
BLOCK_K = 256
NEG = -1e30


def attn_kernel(sc_ref, q_ref, start_ref, *refs):
    n_src = 4
    kv_refs = refs[:2 * n_src]
    o_ref, m_ref, l_ref, acc_ref = refs[2 * n_src:]
    j = pl.program_id(1)
    head_dim = q_ref.shape[-1]
    scale = (head_dim ** -0.5) * math.log2(math.e)
    m_ref[...] = jnp.full_like(m_ref, NEG)
    l_ref[...] = jnp.zeros_like(l_ref)
    acc_ref[...] = jnp.zeros_like(acc_ref)
    q0 = sc_ref[n_src] + j * BLOCK_Q
    first_start = sc_ref[n_src + 1 + 2 * j]
    last_start = sc_ref[n_src + 2 + 2 * j]
    q = q_ref[0]

    def update(k_ref, v_ref, kb, base, masked):
        rows = pl.ds(pl.multiple_of(kb * BLOCK_K, BLOCK_K), BLOCK_K)
        s = dot(q, k_ref[0, rows, :], NT)
        if masked:
            col = base + kb * BLOCK_K + lax.broadcasted_iota(jnp.int32, s.shape, 1)
            row = q0 + lax.broadcasted_iota(jnp.int32, s.shape, 0)
            start = jnp.concatenate([start_ref[...], start_ref[...]], axis=1)
            s = jnp.where((col >= start) & (col <= row), s, NEG)
        m_old = m_ref[...]
        m_new = jnp.maximum(m_old, jnp.max(s, axis=-1, keepdims=True))
        wide = jnp.concatenate([m_new, m_new], axis=1)
        p = jnp.exp2((s - wide) * scale)
        if masked:
            p = jnp.where(s > 0.5 * NEG, p, 0.0)
        alpha = jnp.exp2((m_old - m_new) * scale)
        l_ref[...] = l_ref[...] * alpha + jnp.sum(p, axis=-1, keepdims=True)
        acc_ref[...] = acc_ref[...] * alpha + dot(p.astype(BF16), v_ref[0, rows, :])
        m_ref[...] = m_new

    for i in range(n_src):
        base = sc_ref[i]
        k_ref, v_ref = kv_refs[2 * i], kv_refs[2 * i + 1]
        tokens = k_ref.shape[1]
        lo = jnp.maximum(first_start - base, 0) // BLOCK_K
        top = jnp.clip(q0 + BLOCK_Q - base, 0, tokens)
        hi = (top + BLOCK_K - 1) // BLOCK_K

        def body(kb, carry, k_ref=k_ref, v_ref=v_ref, base=base):
            k_first = base + kb * BLOCK_K
            inside = (k_first >= last_start) & (k_first + BLOCK_K - 1 <= q0)

            @pl.when(inside)
            def _():
                update(k_ref, v_ref, kb, base, False)

            @pl.when(jnp.logical_not(inside))
            def _():
                update(k_ref, v_ref, kb, base, True)

            return carry

        lax.fori_loop(lo, hi, body, 0)
    o_ref[...] = (acc_ref[...] / l_ref[...]).astype(BF16)


def attention(scalars, q, starts, kv_list):
    n_heads, tokens, head_dim = q.shape
    in_specs = [
        pl.BlockSpec((1, BLOCK_Q, head_dim), lambda h, j, sc: (h, j, 0)),
        pl.BlockSpec((BLOCK_Q, 128), lambda h, j, sc: (j, 0)),
    ]
    args = [q, starts]
    for kv in kv_list:
        in_specs.append(pl.BlockSpec((1, tokens, head_dim), lambda h, j, sc: (h, 0, 0)))
        in_specs.append(pl.BlockSpec((1, tokens, head_dim), lambda h, j, sc: (h + n_heads, 0, 0)))
        args += [kv, kv]
    return pl.pallas_call(
        attn_kernel,
        grid_spec=pltpu.PrefetchScalarGridSpec(
            num_scalar_prefetch=1,
            grid=(n_heads, tokens // BLOCK_Q),
            in_specs=in_specs,
            out_specs=pl.BlockSpec((BLOCK_Q, head_dim), lambda h, j, sc: (j, h)),
            scratch_shapes=[pltpu.VMEM((BLOCK_Q, 128), F32)] * 2 + [pltpu.VMEM((BLOCK_Q, head_dim), F32)],
        ),
        out_shape=jax.ShapeDtypeStruct((tokens, n_heads * head_dim), BF16),
        compiler_params=params(("arbitrary", "arbitrary")),
        cost_estimate=cost(4 * n_heads * tokens * 2 * tokens * head_dim, 20e6, n_heads * tokens * tokens),
        name="attention",
    )(scalars, *args)


def solution(mesh):
    n_dev = mesh.shape['sp']
    swap_perm = [(d, d ^ 1) for d in range(n_dev)]
    cross_perm = [(d, d + 2) for d in range(n_dev - 2)]
    row_spec = P(('dp', 'sp'), None)
    tok_spec = P(('dp', 'sp'))
    replicated = P()

    def device_fn(x_rows, seg_ids, norm_gains, w_in, ssm_head, y_gain, w_out, mlp_up, mlp_down, w_qkv, w_attn_out):
        dev = lax.axis_index('sp')
        tokens, dim = x_rows.shape
        inner = y_gain.shape[0]
        n_heads = ssm_head.shape[1]
        n_chunks = tokens // CHUNK
        n_query, head_dim = w_attn_out.shape[:2]

        seg_all = lax.all_gather(seg_ids, 'sp', tiled=True)
        doc_starts = jnp.sum((seg_all[None, :] < jnp.arange(1, 5, dtype=jnp.int32)[:, None]).astype(jnp.int32), axis=1)
        start = jnp.zeros_like(seg_ids)
        for doc in range(4):
            start = jnp.where(seg_ids > doc, doc_starts[doc], start)
        first_pos = dev * tokens
        chunk_first = first_pos + (jnp.arange(tokens, dtype=jnp.int32) // CHUNK) * CHUNK
        rel = jnp.broadcast_to((start - chunk_first)[:, None], (tokens, 128))
        start_wide = jnp.broadcast_to(start[:, None], (tokens, 128))

        pad_heads = ((0, 0), (0, 128 - n_heads))
        bias = jnp.pad(ssm_head[0:1], pad_heads)
        rate = jnp.pad(ssm_head[1:2], pad_heads)
        skip = jnp.repeat(ssm_head[2:3], inner // n_heads, axis=1)
        w_in_t = w_in.T
        hid, xs, bc, dt, cum = in_proj(x_rows, norm_gains[0:1], w_in_t, bias, rate, inner, n_heads)
        state_end, decay = ssd_state(xs, bc, dt, cum, rel)

        odd = (dev % 2) == 1
        pair_state = lax.ppermute(state_end, 'sp', swap_perm)
        pair_decay = lax.ppermute(decay, 'sp', swap_perm)
        chip_state = jnp.where(odd, decay * pair_state + state_end, pair_decay * state_end + pair_state)
        half = state_end.shape[0] // 2
        mine = jnp.where(odd, chip_state[half:], chip_state[:half])
        got = lax.ppermute(mine, 'sp', cross_perm)
        other = lax.ppermute(got, 'sp', swap_perm)
        z = z_proj(hid, w_in_t, inner)
        chip_in = jnp.where(odd, jnp.concatenate([other, got], axis=0), jnp.concatenate([got, other], axis=0))
        h_in = jnp.where(odd, pair_decay * chip_in + pair_state, chip_in)

        pack = jnp.stack([cum[:, :n_heads], dt[:, :n_heads]]).reshape(2, n_chunks, CHUNK, n_heads)
        pack = pack.transpose(1, 0, 3, 2).reshape(n_chunks, n_heads, 2 * CHUNK)
        gated = ssd_full(xs, bc, dt, cum, rel, pack, z, h_in, skip, y_gain[None, :])
        x_one = proj_add(gated, w_out, x_rows)
        x_two = mlp(x_one, norm_gains[1:2], mlp_up, mlp_down, 0)

        x_far = lax.ppermute(x_two, 'sp', cross_perm)
        w_heads = w_qkv.transpose(1, 0, 2)
        pos = first_pos + jnp.arange(tokens)
        cos, sin = rope_tables(pos.astype(F32), head_dim)
        cos_far, sin_far = rope_tables((pos - 2 * tokens).astype(F32), head_dim)
        q, kv = qkv_proj(x_two, norm_gains[2:3], cos, sin, w_heads, n_query, True)
        kv_pair = lax.ppermute(kv, 'sp', swap_perm)
        kv_far, = qkv_proj(x_far, norm_gains[2:3], cos_far, sin_far, w_heads, n_query, False)
        kv_far_pair = lax.ppermute(kv_far, 'sp', swap_perm)
        far = jnp.int32(1 << 24)
        pair_pos = (dev ^ 1) * tokens
        scalars = jnp.stack([
            jnp.where(dev >= 2, first_pos - 2 * tokens, far),
            jnp.where(dev >= 2, pair_pos - 2 * tokens, far),
            pair_pos, first_pos, first_pos,
        ])
        edges = jnp.stack([start[::BLOCK_Q], start[BLOCK_Q - 1::BLOCK_Q]], axis=1).reshape(-1)
        scalars = jnp.concatenate([scalars, edges]).astype(jnp.int32)
        attn = attention(scalars, q, start_wide, [kv_far, kv_far_pair, kv_pair, kv])
        x_three = proj_add(attn, w_attn_out.reshape(n_query * head_dim, dim), x_two)
        return mlp(x_three, norm_gains[3:4], mlp_up, mlp_down, 1)

    return jax.shard_map(device_fn, mesh=mesh, in_specs=(row_spec, tok_spec) + (replicated,) * 9, out_specs=row_spec, check_vma=False)
```

```python
import functools
import math

import jax
import jax.numpy as jnp
from jax import lax
from jax.experimental import pallas as pl
from jax.experimental.pallas import tpu as pltpu
from jax.sharding import PartitionSpec as P


CHUNK = 64
NORM_EPS = 1e-6
ROPE_BASE = 10000.0
F32 = jnp.float32
BF16 = jnp.bfloat16
VMEM_LIMIT = 60 * 1024 * 1024
NT = (((1,), (1,)), ((), ()))


def dot(a, b, dims=(((1,), (0,)), ((), ()))):
    return lax.dot_general(a, b, dims, preferred_element_type=F32)


def params(sem):
    return pltpu.CompilerParams(dimension_semantics=sem, vmem_limit_bytes=VMEM_LIMIT)


def cost(flops, bytes_accessed, trans=0):
    return pl.CostEstimate(flops=int(flops), bytes_accessed=int(bytes_accessed), transcendentals=int(trans))


def norm_rows(values, gain):
    wide = values.astype(F32)
    inv = lax.rsqrt(jnp.mean(wide * wide, axis=-1, keepdims=True) + NORM_EPS)
    return (wide * inv * gain).astype(BF16)


SMEM_SPEC = pl.BlockSpec(memory_space=pltpu.SMEM)


def full_spec(shape):
    zeros = (0,) * len(shape)
    return pl.BlockSpec(shape, lambda *_: zeros)


def in_proj_kernel(n_heads, x_ref, gain_ref, w_ref, head_ref, h_ref, xs_ref, bc_ref, dt_ref, cum_ref):
    step = pl.program_id(0)

    @pl.when(step == 0)
    def _():
        hid = norm_rows(x_ref[...], gain_ref[0:1, :])
        h_ref[...] = hid
        out = dot(hid, w_ref[...], NT)
        n_bc = bc_ref.shape[1]
        bc_ref[...] = out[:, :n_bc].astype(BF16)
        lanes = dt_ref.shape[1]
        raw = out[:, n_bc:n_bc + lanes] + head_ref[0:1, :]
        dt = jnp.maximum(raw, 0.0) + jnp.log1p(jnp.exp(-jnp.abs(raw)))
        lane = lax.broadcasted_iota(jnp.int32, dt.shape, 1)
        dt = jnp.where(lane < n_heads, dt, 0.0)
        dt_ref[...] = dt
        cum = dt * head_ref[1:2, :]
        row = lax.broadcasted_iota(jnp.int32, dt.shape, 0) % CHUNK
        shift = 1
        while shift < CHUNK:
            cum = cum + jnp.where(row >= shift, pltpu.roll(cum, shift, 0), 0.0)
            shift *= 2
        cum_ref[...] = cum

    @pl.when(step > 0)
    def _():
        xs_ref[...] = dot(h_ref[...], w_ref[...], NT).astype(BF16)


def in_proj(x_rows, gains, w_in_t, head_pad, inner, n_heads):
    tokens, dim = x_rows.shape
    tile = 512
    n_x = inner // tile
    last = 2 * inner // tile
    out_shape = (
        jax.ShapeDtypeStruct((tokens, dim), BF16),
        jax.ShapeDtypeStruct((tokens, inner), BF16),
        jax.ShapeDtypeStruct((tokens, 256), BF16),
        jax.ShapeDtypeStruct((tokens, 128), F32),
        jax.ShapeDtypeStruct((tokens, 128), F32),
    )
    return pl.pallas_call(
        functools.partial(in_proj_kernel, n_heads),
        grid=(n_x + 1,),
        in_specs=[
            full_spec((tokens, dim)),
            full_spec(gains.shape),
            pl.BlockSpec((tile, dim), lambda i: (jnp.where(i == 0, last, i - 1), 0)),
            full_spec((8, 128)),
        ],
        out_specs=(
            full_spec((tokens, dim)),
            pl.BlockSpec((tokens, tile), lambda i: (0, jnp.maximum(i - 1, 0))),
            full_spec((tokens, 256)),
            full_spec((tokens, 128)),
            full_spec((tokens, 128)),
        ),
        out_shape=out_shape,
        compiler_params=params(("arbitrary",)),
        cost_estimate=cost(2 * tokens * dim * (inner + tile), 16e6),
        name="in_proj",
    )(x_rows, gains, w_in_t, head_pad)


def z_proj_kernel(h_ref, w_ref, z_ref):
    z_ref[...] = dot(h_ref[...], w_ref[...], NT)


def z_proj(hid, w_in_t, inner):
    tokens, dim = hid.shape
    tile = 512
    first = inner // tile
    return pl.pallas_call(
        z_proj_kernel,
        grid=(inner // tile,),
        in_specs=[full_spec((tokens, dim)), pl.BlockSpec((tile, dim), lambda i: (i + first, 0))],
        out_specs=pl.BlockSpec((tokens, tile), lambda i: (0, i)),
        out_shape=jax.ShapeDtypeStruct((tokens, inner), F32),
        compiler_params=params(("arbitrary",)),
        cost_estimate=cost(2 * tokens * dim * inner, 21e6),
        name="z_proj",
    )(hid, w_in_t)


def head_lanes(cols, first, width):
    rows = cols.shape[0]
    lane = lax.broadcasted_iota(jnp.int32, (rows, 128), 1)
    parts = []
    for k in range(width // 128):
        left = jnp.broadcast_to(cols[:, first + 2 * k:first + 2 * k + 1], (rows, 128))
        right = jnp.broadcast_to(cols[:, first + 2 * k + 1:first + 2 * k + 2], (rows, 128))
        parts.append(jnp.where(lane < 64, left, right))
    return jnp.concatenate(parts, axis=1)


def chunk_weights(dt, cum, rel):
    last_rel = rel[CHUNK - 1:CHUNK, :]
    pos = lax.broadcasted_iota(jnp.int32, cum.shape, 0)
    last_cum = cum[CHUNK - 1:CHUNK, :]
    end_w = jnp.where(pos >= last_rel, jnp.exp(last_cum - cum), 0.0) * dt
    carry = jnp.where(rel < 0, jnp.exp(cum), 0.0)
    return end_w, carry


def state_step(state_ref, cols, xg, bt, end_w, dec_row, first):
    xw = (xg.astype(F32) * head_lanes(end_w, first, xg.shape[1])).astype(BF16)
    state_ref[:, cols] = dec_row * state_ref[:, cols] + dot(bt, xw)


def block_rel(sc_ref, seg_ref):
    return doc_start(seg_ref[...], sc_ref, N_SRC) - (sc_ref[N_SRC - 1] + pl.program_id(0) * CHUNK)


def ssd_state_kernel(sc_ref, x_ref, bc_ref, dt_ref, cum_ref, seg_ref, end_ref, decay_ref):
    step = pl.program_id(0)

    @pl.when(step == 0)
    def _():
        end_ref[...] = jnp.zeros_like(end_ref)
        decay_ref[...] = jnp.ones_like(decay_ref)

    end_w, carry = chunk_weights(dt_ref[...], cum_ref[...], block_rel(sc_ref, seg_ref))
    bt = bc_ref[:, :128].astype(F32).T.astype(BF16)
    for g in range(x_ref.shape[1] // 256):
        cols = slice(g * 256, (g + 1) * 256)
        dec_row = head_lanes(carry[CHUNK - 8:, :], 4 * g, 256)[7:8]
        state_step(end_ref, cols, x_ref[:, cols], bt, end_w, dec_row, 4 * g)
        decay_ref[:, cols] = decay_ref[:, cols] * dec_row


def ssd_state(scalars, xs, bc, dt, cum, seg_wide):
    tokens, inner = xs.shape
    row = lambda width: pl.BlockSpec((CHUNK, width), lambda i: (i, 0))
    return pl.pallas_call(
        ssd_state_kernel,
        grid=(tokens // CHUNK,),
        in_specs=[SMEM_SPEC, row(inner), row(256), row(128), row(128), row(128)],
        out_specs=(full_spec((128, inner)), full_spec((1, inner))),
        out_shape=(jax.ShapeDtypeStruct((128, inner), F32), jax.ShapeDtypeStruct((1, inner), F32)),
        compiler_params=params(("arbitrary",)),
        cost_estimate=cost(2 * tokens * 256 * inner, 8e6),
        name="ssd_state",
    )(scalars, xs, bc, dt, cum, seg_wide)


def ssd_full_kernel(sc_ref, x_ref, bc_ref, dt_ref, cum_ref, seg_ref, pack_ref, z_ref, hin_ref, skip_ref, gain_ref, out_ref, state_ref, y_ref):
    step = pl.program_id(0)

    @pl.when(step == 0)
    def _():
        state_ref[...] = hin_ref[...]

    inner = x_ref.shape[1]
    cum = cum_ref[...]
    rel = block_rel(sc_ref, seg_ref)
    end_w, carry = chunk_weights(dt_ref[...], cum, rel)
    b_blk = bc_ref[:, :128]
    c_blk = bc_ref[:, 128:]
    bt = b_blk.astype(F32).T.astype(BF16)
    row_id = lax.broadcasted_iota(jnp.int32, (CHUNK, 128), 0)
    lane_id = lax.broadcasted_iota(jnp.int32, (CHUNK, 128), 1)
    src = jnp.where(lane_id < 64, lane_id, lane_id - 64)
    visible = (src >= rel) & (src <= row_id)
    scores = dot(c_blk, jnp.concatenate([b_blk, b_blk], axis=0), NT)
    scores = jnp.where(visible, scores, 0.0)
    blk_row = lax.broadcasted_iota(jnp.int32, (256, 256), 0) // 64
    blk_col = lax.broadcasted_iota(jnp.int32, (256, 256), 1) // 64
    diag = blk_row == blk_col
    n_pairs = inner // 128
    sumsq = jnp.zeros((CHUNK, 128), F32)
    for g in range(inner // 256):
        cols = slice(g * 256, (g + 1) * 256)
        xg = x_ref[:, cols]
        carry_x = head_lanes(carry, 4 * g, 256)
        cum_x = head_lanes(cum, 4 * g, 256)
        mixes = []
        for k in range(2):
            pair = 2 * g + k
            cum_s = pack_ref[0, pair:pair + 1, :]
            dt_s = pack_ref[0, n_pairs + pair:n_pairs + pair + 1, :]
            decay = jnp.exp(jnp.minimum(cum_x[:, k * 128:(k + 1) * 128] - cum_s, 0.0))
            mixes.append((scores * decay * dt_s).astype(BF16))
        mix = jnp.concatenate(mixes, axis=1)
        x_diag = jnp.where(diag, jnp.concatenate([xg, xg, xg, xg], axis=0), jnp.zeros((), BF16))
        y_in = dot(mix, x_diag)
        y_carry = dot(c_blk, state_ref[:, cols].astype(BF16)) * carry_x
        y = y_in + skip_ref[:, cols] * xg.astype(F32) + y_carry
        y_ref[:, cols] = y
        sq = y * y
        sumsq = sumsq + sq[:, :128] + sq[:, 128:]
        state_step(state_ref, cols, xg, bt, end_w, carry_x[CHUNK - 1:CHUNK, :], 4 * g)
    inv = lax.rsqrt(jnp.sum(sumsq, axis=-1, keepdims=True) * (1.0 / inner) + NORM_EPS)
    for g in range(inner // 512):
        cols = slice(g * 512, (g + 1) * 512)
        z = z_ref[:, cols]
        out_ref[:, cols] = (y_ref[:, cols] * inv * gain_ref[:, cols] * (z * jax.nn.sigmoid(z))).astype(BF16)


def ssd_full(scalars, xs, bc, dt, cum, seg_wide, pack, z, h_in, skip, gain):
    tokens, inner = xs.shape
    row = lambda width: pl.BlockSpec((CHUNK, width), lambda i: (i, 0))
    return pl.pallas_call(
        ssd_full_kernel,
        grid=(tokens // CHUNK,),
        in_specs=[
            SMEM_SPEC, row(inner), row(256), row(128), row(128), row(128),
            pl.BlockSpec((1, pack.shape[1], 128), lambda i: (i, 0, 0)),
            row(inner), full_spec((128, inner)), full_spec((1, inner)), full_spec((1, inner)),
        ],
        out_specs=row(inner),
        out_shape=jax.ShapeDtypeStruct((tokens, inner), BF16),
        scratch_shapes=[pltpu.VMEM((128, inner), F32), pltpu.VMEM((CHUNK, inner), F32)],
        compiler_params=params(("arbitrary",)),
        cost_estimate=cost(12e9, 20e6),
        name="ssd_full",
    )(scalars, xs, bc, dt, cum, seg_wide, pack, z, h_in, skip, gain)


def proj_add_kernel(a_ref, w_ref, *refs):
    out_ref = refs[-1]
    res = jnp.concatenate([r[...] for r in refs[:-1]], axis=0)
    out_ref[...] = (res.astype(F32) + dot(a_ref[...], w_ref[...])).astype(BF16)


def proj_add(a, w, res):
    tokens, depth = a.shape
    dim = w.shape[1]
    tile = 256
    col = lambda rows: pl.BlockSpec((rows, tile), lambda i: (0, i))
    return pl.pallas_call(
        proj_add_kernel,
        grid=(dim // tile,),
        in_specs=[full_spec((tokens, depth)), col(depth)] + [col(r.shape[0]) for r in res],
        out_specs=col(tokens),
        out_shape=jax.ShapeDtypeStruct((tokens, dim), BF16),
        compiler_params=params(("arbitrary",)),
        cost_estimate=cost(2 * tokens * depth * dim, 2 * (tokens * depth + depth * dim + 2 * tokens * dim)),
        name="proj_add",
    )(a, w, *res)


def mlp_kernel(layer, x_ref, gain_ref, wg_ref, wu_ref, wd_ref, out_ref, h_ref, acc_ref):
    step = pl.program_id(0)

    @pl.when(step == 0)
    def _():
        h_ref[...] = norm_rows(x_ref[...], gain_ref[2 * layer + 1:2 * layer + 2, :])
        acc_ref[...] = jnp.zeros_like(acc_ref)

    hid = h_ref[...]
    gate = dot(hid, wg_ref[0])
    up = dot(hid, wu_ref[0])
    act = (gate * jax.nn.sigmoid(gate) * up).astype(BF16)
    acc_ref[...] += dot(act, wd_ref[0])

    @pl.when(step == pl.num_programs(0) - 1)
    def _():
        out_ref[...] = (x_ref[...].astype(F32) + acc_ref[...]).astype(BF16)


def mlp(x_rows, gains, mlp_up, mlp_down, layer, part, parts):
    tokens, dim = x_rows.shape
    tokens //= parts
    ff = mlp_down.shape[1]
    tile = 512
    n_ff = ff // tile
    return pl.pallas_call(
        functools.partial(mlp_kernel, layer),
        grid=(n_ff,),
        in_specs=[
            pl.BlockSpec((tokens, dim), lambda i: (part, 0)),
            full_spec(gains.shape),
            pl.BlockSpec((1, dim, tile), lambda i: (layer, 0, i)),
            pl.BlockSpec((1, dim, tile), lambda i: (layer, 0, i + n_ff)),
            pl.BlockSpec((1, tile, dim), lambda i: (layer, i, 0)),
        ],
        out_specs=full_spec((tokens, dim)),
        out_shape=jax.ShapeDtypeStruct((tokens, dim), BF16),
        scratch_shapes=[pltpu.VMEM((tokens, dim), BF16), pltpu.VMEM((tokens, dim), F32)],
        compiler_params=params(("arbitrary",)),
        cost_estimate=cost(6 * tokens * dim * ff, 6 * dim * ff),
        name="mlp",
    )(x_rows, gains, mlp_up, mlp_up, mlp_down)


def rope_tables(positions, head_dim):
    half = head_dim // 2
    inv_freq = ROPE_BASE ** (-jnp.arange(half, dtype=F32) * 2.0 / head_dim)
    angle = positions[:, None] * inv_freq[None, :]
    cos, sin = jnp.cos(angle), jnp.sin(angle)
    return jnp.concatenate([cos, cos], axis=1), jnp.concatenate([-sin, sin], axis=1)


def qkv_kernel(n_q, n_rot, xa_ref, xb_ref, gain_ref, cos_ref, sin_ref, w_ref, *refs):
    h_ref = refs[-1]
    kv_ref = refs[-2]
    step = pl.program_id(0)

    @pl.when(step == 0)
    def _():
        rows = xa_ref.shape[0]
        h_ref[:rows] = norm_rows(xa_ref[...], gain_ref[2:3, :])
        h_ref[rows:] = norm_rows(xb_ref[...], gain_ref[2:3, :])

    heads, _, head_dim = w_ref.shape
    w_all = jnp.concatenate([w_ref[k] for k in range(heads)], axis=1)
    out = dot(h_ref[...], w_all)

    def rotated(k):
        val = out[:, k * head_dim:(k + 1) * head_dim]
        return (val * cos_ref[...] + pltpu.roll(val, head_dim // 2, 1) * sin_ref[...]).astype(BF16)

    if n_q:
        @pl.when(step < n_q)
        def _():
            for k in range(heads):
                refs[0][k] = rotated(k)

    @pl.when((step >= n_q) & (step < n_rot))
    def _():
        for k in range(heads):
            kv_ref[k] = rotated(k)

    @pl.when(step >= n_rot)
    def _():
        for k in range(heads):
            kv_ref[k] = out[:, k * head_dim:(k + 1) * head_dim].astype(BF16)


def qkv_proj(x_a, x_b, gains, cos, sin, w_heads, n_query, with_q):
    tokens, dim = x_a.shape
    tokens *= 2
    n_heads, _, head_dim = w_heads.shape
    n_kv = n_heads - n_query
    per = 4
    n_q = n_query // per if with_q else 0
    skip = 0 if with_q else n_query // per
    n_rot = n_q + n_kv // 2 // per
    steps = n_heads // per - skip
    out_specs = [pl.BlockSpec((per, tokens, head_dim), lambda i: (jnp.maximum(i - n_q, 0), 0, 0))]
    out_shape = [jax.ShapeDtypeStruct((n_kv, tokens, head_dim), BF16)]
    if with_q:
        out_specs.insert(0, pl.BlockSpec((per, tokens, head_dim), lambda i: (jnp.minimum(i, n_q - 1), 0, 0)))
        out_shape.insert(0, jax.ShapeDtypeStruct((n_query, tokens, head_dim), BF16))
    return pl.pallas_call(
        functools.partial(qkv_kernel, n_q, n_rot),
        grid=(steps,),
        in_specs=[
            full_spec(x_a.shape), full_spec(x_a.shape), full_spec(gains.shape), full_spec((tokens, head_dim)),
            full_spec((tokens, head_dim)),
            pl.BlockSpec((per, dim, head_dim), lambda i: (i + skip, 0, 0)),
        ],
        out_specs=tuple(out_specs),
        out_shape=tuple(out_shape),
        scratch_shapes=[pltpu.VMEM((tokens, dim), BF16)],
        compiler_params=params(("arbitrary",)),
        cost_estimate=cost(2 * tokens * dim * steps * per * head_dim, 2 * dim * steps * per * head_dim + 8e6),
        name="qkv" if with_q else "kv",
    )(x_a, x_b, gains, cos, sin, w_heads)


BLOCK = 256
HEAD_GROUP = 4
N_SRC = 4
NEG = -1e30


def doc_start(seg, sc_ref, first):
    start = jnp.zeros_like(seg)
    for doc in range(4):
        start = jnp.where(seg > doc, sc_ref[first + doc], start)
    return start


def attn_kernel(sc_ref, q_ref, seg_ref, *refs):
    kv_refs = refs[:2 * N_SRC]
    o_ref, m_ref, l_ref, acc_ref, bias_ref = refs[2 * N_SRC:]
    j = pl.program_id(1)
    heads, _, head_dim = q_ref.shape
    scale = (head_dim ** -0.5) * math.log2(math.e)
    q0 = sc_ref[N_SRC - 1] + j * BLOCK
    first_start = doc_start(sc_ref[N_SRC + 4 + j], sc_ref, N_SRC)
    start = doc_start(seg_ref[...], sc_ref, N_SRC)
    start = jnp.concatenate([start, start], axis=1)
    col_id = lax.broadcasted_iota(jnp.int32, (BLOCK, BLOCK), 1)
    row_id = lax.broadcasted_iota(jnp.int32, (BLOCK, BLOCK), 0)

    def weights(h, k_ref, rows, bias):
        s = dot(q_ref[h], k_ref[h, rows, :], NT) + bias
        return s, jnp.max(s, axis=-1, keepdims=True)

    k_ref, v_ref = kv_refs[2 * N_SRC - 2:]
    rows = pl.ds(pl.multiple_of(j * BLOCK, BLOCK), BLOCK)
    bias_ref[...] = jnp.where((col_id + q0 >= start) & (col_id <= row_id), 0.0, NEG)
    for h in range(heads):
        s, top = weights(h, k_ref, rows, bias_ref[...])
        m_new = jnp.broadcast_to(top, (BLOCK, 128))
        p = jnp.exp2((s - jnp.concatenate([m_new, m_new], axis=1)) * scale)
        m_ref[h] = m_new
        l_ref[h] = p[:, :128] + p[:, 128:]
        acc_ref[h] = dot(p.astype(BF16), v_ref[h, rows, :])

    for i in reversed(range(N_SRC)):
        base = sc_ref[i]
        k_ref, v_ref = kv_refs[2 * i], kv_refs[2 * i + 1]
        lo = jnp.maximum(first_start - base, 0) // BLOCK
        hi = jnp.clip(q0 - base, 0, k_ref.shape[1]) // BLOCK

        def body(kb, carry, k_ref=k_ref, v_ref=v_ref, base=base):
            rows = pl.ds(pl.multiple_of(kb * BLOCK, BLOCK), BLOCK)
            bias_ref[...] = jnp.where(col_id + (base + kb * BLOCK) >= start, 0.0, NEG)
            for h in range(heads):
                s, top = weights(h, k_ref, rows, bias_ref[...])
                m_old = m_ref[h]
                m_new = jnp.maximum(m_old, top)
                p = jnp.exp2((s - jnp.concatenate([m_new, m_new], axis=1)) * scale)
                alpha = jnp.exp2((m_old - m_new) * scale)
                m_ref[h] = m_new
                l_ref[h] = l_ref[h] * alpha + (p[:, :128] + p[:, 128:])
                acc_ref[h] = acc_ref[h] * alpha + dot(p.astype(BF16), v_ref[h, rows, :])
            return carry

        lax.fori_loop(lo, hi, body, 0)
    for h in range(heads):
        total = jnp.sum(l_ref[h], axis=-1, keepdims=True)
        o_ref[:, h * head_dim:(h + 1) * head_dim] = (acc_ref[h] / total).astype(BF16)


def attention(scalars, q, seg_wide, kv_list):
    n_heads, tokens, head_dim = q.shape
    per = HEAD_GROUP
    groups = n_heads // per
    in_specs = [
        pl.BlockSpec((per, BLOCK, head_dim), lambda h, j, sc: (h, j, 0)),
        pl.BlockSpec((BLOCK, 128), lambda h, j, sc: (j, 0)),
    ]
    args = [q, seg_wide]
    for kv in kv_list:
        in_specs.append(pl.BlockSpec((per, tokens, head_dim), lambda h, j, sc: (h, 0, 0)))
        in_specs.append(pl.BlockSpec((per, tokens, head_dim), lambda h, j, sc: (h + groups, 0, 0)))
        args += [kv, kv]
    return pl.pallas_call(
        attn_kernel,
        grid_spec=pltpu.PrefetchScalarGridSpec(
            num_scalar_prefetch=1,
            grid=(groups, tokens // BLOCK),
            in_specs=in_specs,
            out_specs=pl.BlockSpec((BLOCK, per * head_dim), lambda h, j, sc: (j, h)),
            scratch_shapes=[pltpu.VMEM((per, BLOCK, 128), F32)] * 2
            + [pltpu.VMEM((per, BLOCK, head_dim), F32), pltpu.VMEM((BLOCK, BLOCK), F32)],
        ),
        out_shape=jax.ShapeDtypeStruct((tokens, n_heads * head_dim), BF16),
        compiler_params=params(("arbitrary", "arbitrary")),
        cost_estimate=cost(4 * n_heads * tokens * 2 * tokens * head_dim, 20e6, n_heads * tokens * tokens),
        name="attention",
    )(scalars, *args)


def solution(mesh):
    n_dev = mesh.shape['sp']
    swap_perm = [(d, d ^ 1) for d in range(n_dev)]
    cross_perm = [(d, d + 2) for d in range(n_dev - 2)]
    row_spec = P(('dp', 'sp'), None)
    tok_spec = P(('dp', 'sp'))
    replicated = P()

    def layers(x_rows, seg_ids, norm_gains, w_in, ssm_head, y_gain, w_out, mlp_up, mlp_down, w_qkv, w_attn_out):
        dev = lax.axis_index('sp')
        tokens, dim = x_rows.shape
        inner = y_gain.shape[0]
        n_heads = ssm_head.shape[1]
        n_chunks = tokens // CHUNK
        n_query, head_dim = w_attn_out.shape[:2]

        counts = jnp.sum((seg_ids[None, :] <= jnp.arange(4, dtype=jnp.int32)[:, None]).astype(jnp.int32), axis=1)
        earlier = [lax.ppermute(counts, 'sp', [(d, d + k) for d in range(n_dev - k)]) for k in range(1, n_dev)]
        seg_wide = jnp.broadcast_to(seg_ids[:, None], (tokens, 128))
        head_pad = jnp.pad(ssm_head, ((0, 5), (0, 128 - n_heads)))
        skip = jnp.repeat(ssm_head[2:3], inner // n_heads, axis=1)
        w_in_t = w_in.T
        hid, xs, bc, dt, cum = in_proj(x_rows, norm_gains, w_in_t, head_pad, inner, n_heads)
        first_pos = dev * tokens
        far = jnp.int32(1 << 24)
        pair_pos = (dev ^ 1) * tokens
        earlier, cum = lax.optimization_barrier((earlier, cum))
        doc_starts = counts + sum(earlier)
        slot = jnp.arange(4, dtype=jnp.int32)
        bases = jnp.where(slot == 3, first_pos, pair_pos)
        bases = jnp.where(slot >= 2, bases, jnp.where(dev >= 2, jnp.where(slot == 0, first_pos, pair_pos) - 2 * tokens, far))
        edge_seg = jnp.pad(seg_ids[::BLOCK], (0, 8 - tokens // BLOCK))
        scalars = jnp.concatenate([bases, doc_starts, edge_seg])
        state_end, decay = ssd_state(scalars, xs, bc, dt, cum, seg_wide)

        odd = (dev % 2) == 1
        pair_state = lax.ppermute(state_end, 'sp', swap_perm)
        pair_decay = lax.ppermute(decay, 'sp', swap_perm)
        chip_state = jnp.where(odd, decay * pair_state + state_end, pair_decay * state_end + pair_state)
        half = state_end.shape[0] // 2
        mine = jnp.where(odd, chip_state[half:], chip_state[:half])
        mine, hid, cum = lax.optimization_barrier((mine, hid, cum))
        got = lax.ppermute(mine, 'sp', cross_perm)
        z = z_proj(hid, w_in_t, inner)
        pack = jnp.stack([cum[:, :n_heads], dt[:, :n_heads]]).reshape(2, n_chunks, CHUNK, n_heads)
        pack = pack.transpose(1, 0, 3, 2).reshape(n_chunks, n_heads, 2 * CHUNK)
        pos = (first_pos + jnp.arange(tokens)).astype(F32)
        cos, sin = rope_tables(pos, head_dim)
        cos_far, sin_far = rope_tables(pos - 2.0 * tokens, head_dim)
        got, z, pack, cos, sin, cos_far, sin_far = lax.optimization_barrier((got, z, pack, cos, sin, cos_far, sin_far))
        other = lax.ppermute(got, 'sp', swap_perm)
        chip_in = jnp.where(odd, jnp.concatenate([other, got], axis=0), jnp.concatenate([got, other], axis=0))
        h_in = jnp.where(odd, pair_decay * chip_in + pair_state, chip_in)

        gated = ssd_full(scalars, xs, bc, dt, cum, seg_wide, pack, z, h_in, skip, y_gain[None, :])
        x_one = proj_add(gated, w_out, [x_rows])
        x_a = mlp(x_one, norm_gains, mlp_up, mlp_down, 0, 0, 2)
        far_a = lax.ppermute(x_a, 'sp', cross_perm)
        x_one, x_a = lax.optimization_barrier((x_one, x_a))
        x_b = mlp(x_one, norm_gains, mlp_up, mlp_down, 0, 1, 2)
        far_b = lax.ppermute(x_b, 'sp', cross_perm)
        w_heads = w_qkv.transpose(1, 0, 2)
        q, kv = qkv_proj(x_a, x_b, norm_gains, cos, sin, w_heads, n_query, True)
        kv_pair = lax.ppermute(kv, 'sp', swap_perm)
        far_a, far_b, q = lax.optimization_barrier((far_a, far_b, q))
        kv_far, = qkv_proj(far_a, far_b, norm_gains, cos_far, sin_far, w_heads, n_query, False)
        kv_far_pair = lax.ppermute(kv_far, 'sp', swap_perm)
        attn = attention(scalars, q, seg_wide, [kv_far, kv_far_pair, kv_pair, kv])
        x_three = proj_add(attn, w_attn_out.reshape(n_query * head_dim, dim), [x_a, x_b])
        return mlp(x_three, norm_gains, mlp_up, mlp_down, 1, 0, 1)

    return jax.shard_map(layers, mesh=mesh, in_specs=(row_spec, tok_spec) + (replicated,) * 9, out_specs=row_spec, check_vma=False)
```

```python
import functools
import math

import jax
import jax.numpy as jnp
from jax import lax
from jax.experimental import pallas as pl
from jax.experimental.pallas import tpu as pltpu
from jax.sharding import PartitionSpec as P


CHUNK = 64
NORM_EPS = 1e-6
ROPE_BASE = 10000.0
F32 = jnp.float32
BF16 = jnp.bfloat16
VMEM_LIMIT = 60 * 1024 * 1024
NT = (((1,), (1,)), ((), ()))


def dot(a, b, dims=(((1,), (0,)), ((), ()))):
    return lax.dot_general(a, b, dims, preferred_element_type=F32)


def params(sem):
    return pltpu.CompilerParams(dimension_semantics=sem, vmem_limit_bytes=VMEM_LIMIT)


def cost(flops, bytes_accessed, trans=0):
    return pl.CostEstimate(flops=int(flops), bytes_accessed=int(bytes_accessed), transcendentals=int(trans))


def norm_rows(values, gain):
    wide = values.astype(F32)
    inv = lax.rsqrt(jnp.mean(wide * wide, axis=-1, keepdims=True) + NORM_EPS)
    return (wide * inv * gain).astype(BF16)


SMEM_SPEC = pl.BlockSpec(memory_space=pltpu.SMEM)


def full_spec(shape):
    zeros = (0,) * len(shape)
    return pl.BlockSpec(shape, lambda *_: zeros)


def in_proj_kernel(n_heads, x_ref, gain_ref, w_ref, head_ref, h_ref, xs_ref, bc_ref, dt_ref, cum_ref):
    step = pl.program_id(0)

    @pl.when(step == 0)
    def _():
        hid = norm_rows(x_ref[...], gain_ref[0:1, :])
        h_ref[...] = hid
        n_bc = bc_ref.shape[1]
        out = dot(hid, w_ref[:n_bc + dt_ref.shape[1], :], NT)
        bc_ref[...] = out[:, :n_bc].astype(BF16)
        lanes = dt_ref.shape[1]
        raw = out[:, n_bc:n_bc + lanes] + head_ref[0:1, :]
        dt = jnp.maximum(raw, 0.0) + jnp.log1p(jnp.exp(-jnp.abs(raw)))
        lane = lax.broadcasted_iota(jnp.int32, dt.shape, 1)
        dt = jnp.where(lane < n_heads, dt, 0.0)
        dt_ref[...] = dt
        cum = dt * head_ref[1:2, :]
        row = lax.broadcasted_iota(jnp.int32, dt.shape, 0) % CHUNK
        shift = 1
        while shift < CHUNK:
            cum = cum + jnp.where(row >= shift, pltpu.roll(cum, shift, 0), 0.0)
            shift *= 2
        cum_ref[...] = cum

    @pl.when(step > 0)
    def _():
        xs_ref[...] = dot(h_ref[...], w_ref[...], NT).astype(BF16)


def in_proj(x_rows, gains, w_in_t, head_pad, inner, n_heads):
    tokens, dim = x_rows.shape
    tile = 1024
    n_x = inner // tile
    last = 2 * inner // tile
    out_shape = (
        jax.ShapeDtypeStruct((tokens, dim), BF16),
        jax.ShapeDtypeStruct((tokens, inner), BF16),
        jax.ShapeDtypeStruct((tokens, 256), BF16),
        jax.ShapeDtypeStruct((tokens, 128), F32),
        jax.ShapeDtypeStruct((tokens, 128), F32),
    )
    return pl.pallas_call(
        functools.partial(in_proj_kernel, n_heads),
        grid=(n_x + 1,),
        in_specs=[
            full_spec((tokens, dim)),
            full_spec(gains.shape),
            pl.BlockSpec((tile, dim), lambda i: (jnp.where(i == 0, last, i - 1), 0)),
            full_spec((8, 128)),
        ],
        out_specs=(
            full_spec((tokens, dim)),
            pl.BlockSpec((tokens, tile), lambda i: (0, jnp.maximum(i - 1, 0))),
            full_spec((tokens, 256)),
            full_spec((tokens, 128)),
            full_spec((tokens, 128)),
        ),
        out_shape=out_shape,
        compiler_params=params(("arbitrary",)),
        cost_estimate=cost(2 * tokens * dim * (inner + tile), 16e6),
        name="in_proj",
    )(x_rows, gains, w_in_t, head_pad)


def z_proj_kernel(h_ref, w_ref, z_ref):
    z = dot(h_ref[...], w_ref[...], NT)
    z_ref[...] = z * jax.nn.sigmoid(z)


def z_proj(hid, w_in_t, inner):
    tokens, dim = hid.shape
    tile = 1024
    first = inner // tile
    return pl.pallas_call(
        z_proj_kernel,
        grid=(inner // tile,),
        in_specs=[full_spec((tokens, dim)), pl.BlockSpec((tile, dim), lambda i: (i + first, 0))],
        out_specs=pl.BlockSpec((tokens, tile), lambda i: (0, i)),
        out_shape=jax.ShapeDtypeStruct((tokens, inner), F32),
        compiler_params=params(("arbitrary",)),
        cost_estimate=cost(2 * tokens * dim * inner, 21e6),
        name="z_proj",
    )(hid, w_in_t)


STEP = 2 * CHUNK
LOG2E = math.log2(math.e)


def split3(x):
    hi = x.astype(BF16).astype(F32)
    rest = x - hi
    mid = rest.astype(BF16).astype(F32)
    low = rest - mid
    return jnp.concatenate([hi + pltpu.roll(mid, 64, 1), low], axis=1).astype(BF16)


def fill_spread(e_ref):
    rows, width = e_ref.shape
    for g in range(width // 512):
        head = lax.broadcasted_iota(jnp.int32, (rows, 512), 0) % 64
        lane = lax.broadcasted_iota(jnp.int32, (rows, 512), 1) + g * 512
        e_ref[:, g * 512:(g + 1) * 512] = jnp.where(head == lane // 64, 1.0, 0.0).astype(BF16)


def step_weights(sc_ref, seg_ref, dt, cum2):
    row = lax.broadcasted_iota(jnp.int32, (STEP, 128), 0)
    start = doc_start(seg_ref[...], sc_ref, N_SRC) - (sc_ref[N_SRC - 1] + pl.program_id(0) * STEP)
    upper = row < CHUNK
    last = lambda v: jnp.where(upper, v[CHUNK - 1:CHUNK, :], v[STEP - 1:STEP, :])
    end_w = jnp.where(row >= last(start), jnp.exp2(last(cum2) - cum2), 0.0) * dt
    rel = jnp.where(upper, start, start - CHUNK)
    return rel, end_w


def half_rows(c):
    return slice(c * CHUNK, (c + 1) * CHUNK)


def b_transposed(bc_ref, c):
    return bc_ref[half_rows(c), :128].astype(F32).T.astype(BF16)


def ssd_state_kernel(sc_ref, x_ref, bc_ref, dt_ref, cum_ref, seg_ref, end_ref, decay_ref, e_ref, xp_ref, xw_ref):
    @pl.when(pl.program_id(0) == 0)
    def _():
        end_ref[...] = jnp.zeros_like(end_ref)
        decay_ref[...] = jnp.ones_like(decay_ref)
        fill_spread(e_ref)

    cum2 = cum_ref[...] * LOG2E
    rel, end_w = step_weights(sc_ref, seg_ref, dt_ref[...], cum2)
    lane = lax.broadcasted_iota(jnp.int32, (STEP, 128), 1)
    carry = jnp.where((rel < 0) & (lane < 64), jnp.exp2(cum2), 0.0)
    ends = [jnp.broadcast_to(carry[r:r + 1, :], (8, 128)) for r in (CHUNK - 1, STEP - 1)]
    xp_ref[...] = dot(split3(jnp.concatenate([end_w] + ends, axis=0)), e_ref[...])
    xw_ref[...] = (x_ref[...].astype(F32) * xp_ref[:STEP, :]).astype(BF16)
    add = [dot(b_transposed(bc_ref, c), xw_ref[half_rows(c), :]) for c in range(2)]
    dec = [xp_ref[STEP + 8 * c:STEP + 8 * c + 1, :] for c in range(2)]
    end_ref[...] = dec[1] * (dec[0] * end_ref[...] + add[0]) + add[1]
    decay_ref[...] = decay_ref[...] * dec[0] * dec[1]


def ssd_state(scalars, xs, bc, dt, cum, seg_wide):
    tokens, inner = xs.shape
    row = lambda width: pl.BlockSpec((STEP, width), lambda i: (i, 0))
    return pl.pallas_call(
        ssd_state_kernel,
        grid=(tokens // STEP,),
        in_specs=[SMEM_SPEC, row(inner), row(256), row(128), row(128), row(128)],
        out_specs=(full_spec((128, inner)), full_spec((1, inner))),
        out_shape=(jax.ShapeDtypeStruct((128, inner), F32), jax.ShapeDtypeStruct((1, inner), F32)),
        scratch_shapes=[pltpu.VMEM((256, inner), BF16), pltpu.VMEM((STEP + 16, inner), F32), pltpu.VMEM((STEP, inner), BF16)],
        compiler_params=params(("arbitrary",)),
        cost_estimate=cost(2 * tokens * 256 * inner, 8e6),
        name="ssd_state",
    )(scalars, xs, bc, dt, cum, seg_wide)


def ssd_full_kernel(sc_ref, x_ref, bc_ref, dt_ref, cum_ref, seg_ref, z_ref, hin_ref, skip_ref, gain_ref, out_ref,
                    state_ref, y_ref, e_ref, xp_ref, xw_ref, turn_ref, pack_ref):
    @pl.when(pl.program_id(0) == 0)
    def _():
        state_ref[...] = hin_ref[...]
        fill_spread(e_ref)

    inner = x_ref.shape[1]
    n_heads = inner // 64
    dt = dt_ref[...]
    cum2 = cum_ref[...] * LOG2E
    rel, end_w = step_weights(sc_ref, seg_ref, dt, cum2)
    xp_ref[...] = dot(split3(jnp.concatenate([cum2, end_w], axis=0)), e_ref[...])
    xw_ref[...] = (x_ref[...].astype(F32) * xp_ref[STEP:, :]).astype(BF16)

    turn_ref[0] = cum2.T
    turn_ref[1] = dt.T
    left = lax.broadcasted_iota(jnp.int32, (n_heads // 2, STEP), 1) < 64
    for k in range(2):
        even = turn_ref[k, pl.ds(0, n_heads // 2, stride=2), :]
        odd = turn_ref[k, pl.ds(1, n_heads // 2, stride=2), :]
        pack_ref[0, k] = jnp.where(left, even, pltpu.roll(odd, 64, 1))
        pack_ref[1, k] = jnp.where(left, pltpu.roll(even, 64, 1), odd)

    row_id = lax.broadcasted_iota(jnp.int32, (CHUNK, 128), 0)
    lane_id = lax.broadcasted_iota(jnp.int32, (CHUNK, 128), 1)
    left = lane_id < 64
    src = jnp.where(left, lane_id, lane_id - 64)
    for c in range(2):
        rows = half_rows(c)
        state = state_ref[...]
        opens = rel[rows] < 0
        c_open = jnp.where(opens, bc_ref[rows, 128:].astype(F32), 0.0).astype(BF16)
        carried = dot(c_open, state.astype(BF16))
        carry_x = jnp.exp2(xp_ref[rows, :])
        keep = jnp.where(opens[CHUNK - 1:CHUNK, :], 1.0, 0.0)
        dec = carry_x[CHUNK - 1:CHUNK, :] * jnp.concatenate([keep] * (inner // 128), axis=1)
        y_ref[rows, :] = carried * carry_x + skip_ref[...] * x_ref[rows, :].astype(F32)
        state_ref[...] = dec * state + dot(b_transposed(bc_ref, c), xw_ref[rows, :])

    for c in range(2):
        rows = half_rows(c)
        visible = (src >= rel[rows]) & (src <= row_id)
        b_blk = bc_ref[rows, :128]
        scores = dot(bc_ref[rows, 128:], jnp.concatenate([b_blk, b_blk], axis=0), NT)
        scores = jnp.where(visible, scores, 0.0)
        left16 = lax.broadcasted_iota(jnp.int32, (CHUNK, 128), 1) < 64
        zero = jnp.zeros((CHUNK, 128), BF16)
        for g in range(inner // 256):
            cols = slice(g * 256, (g + 1) * 256)
            mixes, diag = [], []
            for k in range(2):
                pair = 2 * g + k
                sub = slice(pair * 128, (pair + 1) * 128)
                cum_s = pack_ref[c, 0, pair:pair + 1, :]
                dt_s = pack_ref[c, 1, pair:pair + 1, :]
                decay = jnp.exp2(jnp.minimum(xp_ref[rows, sub] - cum_s, 0.0))
                mixes.append((scores * decay * dt_s).astype(BF16))
                xk = x_ref[rows, sub]
                for keep in (jnp.where(left16, xk, zero), jnp.where(left16, zero, xk)):
                    diag.append(jnp.concatenate([keep, zero] if k == 0 else [zero, keep], axis=1))
            y_ref[rows, cols] += dot(jnp.concatenate(mixes, axis=1), jnp.concatenate(diag, axis=0))

    y = y_ref[...]
    inv = lax.rsqrt(jnp.mean(y * y, axis=-1, keepdims=True) + NORM_EPS)
    out_ref[...] = (y * inv * gain_ref[...] * z_ref[...]).astype(BF16)


def ssd_full(scalars, xs, bc, dt, cum, seg_wide, z, h_in, skip, gain):
    tokens, inner = xs.shape
    row = lambda width: pl.BlockSpec((STEP, width), lambda i: (i, 0))
    return pl.pallas_call(
        ssd_full_kernel,
        grid=(tokens // STEP,),
        in_specs=[
            SMEM_SPEC, row(inner), row(256), row(128), row(128), row(128),
            row(inner), full_spec((128, inner)), full_spec((1, inner)), full_spec((1, inner)),
        ],
        out_specs=row(inner),
        out_shape=jax.ShapeDtypeStruct((tokens, inner), BF16),
        scratch_shapes=[
            pltpu.VMEM((128, inner), F32), pltpu.VMEM((STEP, inner), F32), pltpu.VMEM((256, inner), BF16),
            pltpu.VMEM((2 * STEP, inner), F32), pltpu.VMEM((STEP, inner), BF16), pltpu.VMEM((2, 128, STEP), F32),
            pltpu.VMEM((2, 2, inner // 128, STEP), F32),
        ],
        compiler_params=params(("arbitrary",)),
        cost_estimate=cost(12e9, 20e6),
        name="ssd_full",
    )(scalars, xs, bc, dt, cum, seg_wide, z, h_in, skip, gain)


def proj_add_kernel(a_ref, w_ref, *refs):
    out_ref = refs[-1]
    res = jnp.concatenate([r[...] for r in refs[:-1]], axis=0)
    out_ref[...] = (res.astype(F32) + dot(a_ref[...], w_ref[...])).astype(BF16)


def proj_add(a, w, res):
    tokens, depth = a.shape
    dim = w.shape[1]
    tile = 512
    col = lambda rows: pl.BlockSpec((rows, tile), lambda i: (0, i))
    return pl.pallas_call(
        proj_add_kernel,
        grid=(dim // tile,),
        in_specs=[full_spec((tokens, depth)), col(depth)] + [col(r.shape[0]) for r in res],
        out_specs=col(tokens),
        out_shape=jax.ShapeDtypeStruct((tokens, dim), BF16),
        compiler_params=params(("arbitrary",)),
        cost_estimate=cost(2 * tokens * depth * dim, 2 * (tokens * depth + depth * dim + 2 * tokens * dim)),
        name="proj_add",
    )(a, w, *res)


def mlp_kernel(layer, x_ref, gain_ref, wg_ref, wu_ref, wd_ref, out_ref, h_ref, acc_ref):
    step = pl.program_id(0)

    @pl.when(step == 0)
    def _():
        h_ref[...] = norm_rows(x_ref[...], gain_ref[2 * layer + 1:2 * layer + 2, :])
        acc_ref[...] = jnp.zeros_like(acc_ref)

    hid = h_ref[...]
    gate = dot(hid, wg_ref[0])
    up = dot(hid, wu_ref[0])
    act = (gate * jax.nn.sigmoid(gate) * up).astype(BF16)
    acc_ref[...] += dot(act, wd_ref[0])

    @pl.when(step == pl.num_programs(0) - 1)
    def _():
        out_ref[...] = (x_ref[...].astype(F32) + acc_ref[...]).astype(BF16)


def mlp(x_rows, gains, mlp_up, mlp_down, layer, part, parts):
    tokens, dim = x_rows.shape
    tokens //= parts
    ff = mlp_down.shape[1]
    tile = 1024
    n_ff = ff // tile
    return pl.pallas_call(
        functools.partial(mlp_kernel, layer),
        grid=(n_ff,),
        in_specs=[
            pl.BlockSpec((tokens, dim), lambda i: (part, 0)),
            full_spec(gains.shape),
            pl.BlockSpec((1, dim, tile), lambda i: (layer, 0, i)),
            pl.BlockSpec((1, dim, tile), lambda i: (layer, 0, i + n_ff)),
            pl.BlockSpec((1, tile, dim), lambda i: (layer, i, 0)),
        ],
        out_specs=full_spec((tokens, dim)),
        out_shape=jax.ShapeDtypeStruct((tokens, dim), BF16),
        scratch_shapes=[pltpu.VMEM((tokens, dim), BF16), pltpu.VMEM((tokens, dim), F32)],
        compiler_params=params(("arbitrary",)),
        cost_estimate=cost(6 * tokens * dim * ff, 6 * dim * ff),
        name="mlp",
    )(x_rows, gains, mlp_up, mlp_up, mlp_down)


def rope_tables(positions, head_dim):
    half = head_dim // 2
    inv_freq = ROPE_BASE ** (-jnp.arange(half, dtype=F32) * 2.0 / head_dim)
    angle = positions[:, None] * inv_freq[None, :]
    cos, sin = jnp.cos(angle), jnp.sin(angle)
    return jnp.concatenate([cos, cos], axis=1), jnp.concatenate([-sin, sin], axis=1)


def qkv_kernel(n_q, n_rot, n_parts, *refs):
    x_refs = refs[:n_parts]
    gain_ref, cos_ref, sin_ref, w_ref = refs[n_parts:n_parts + 4]
    kv_ref, h_ref = refs[-2:]
    step = pl.program_id(0)

    @pl.when(step == 0)
    def _():
        first = 0
        for x_ref in x_refs:
            h_ref[first:first + x_ref.shape[0]] = norm_rows(x_ref[...], gain_ref[2:3, :])
            first += x_ref.shape[0]

    heads, _, head_dim = w_ref.shape
    turns = step < n_rot
    cos = jnp.where(turns, cos_ref[...], 1.0)
    sin = jnp.where(turns, sin_ref[...], 0.0)
    for k in range(0, heads, 2):
        out = dot(h_ref[...], jnp.concatenate([w_ref[k], w_ref[k + 1]], axis=1))
        for i in range(2):
            val = out[:, i * head_dim:(i + 1) * head_dim]
            kv_ref[k + i] = (val * cos + pltpu.roll(val, head_dim // 2, 1) * sin).astype(BF16)

    if n_q:
        @pl.when(step < n_q)
        def _():
            refs[n_parts + 4][...] = kv_ref[...]


def qkv_proj(parts, gains, cos, sin, table_part, w_heads, n_query, with_q):
    tokens = sum(x.shape[0] for x in parts)
    dim = parts[0].shape[1]
    n_heads, _, head_dim = w_heads.shape
    n_kv = n_heads - n_query
    per = 6
    n_q = n_query // per if with_q else 0
    skip = 0 if with_q else n_query // per
    n_rot = n_q + n_kv // 2 // per
    steps = n_heads // per - skip
    out_specs = [pl.BlockSpec((per, tokens, head_dim), lambda i: (jnp.maximum(i - n_q, 0), 0, 0))]
    out_shape = [jax.ShapeDtypeStruct((n_kv, tokens, head_dim), BF16)]
    if with_q:
        out_specs.insert(0, pl.BlockSpec((per, tokens, head_dim), lambda i: (jnp.minimum(i, n_q - 1), 0, 0)))
        out_shape.insert(0, jax.ShapeDtypeStruct((n_query, tokens, head_dim), BF16))
    table = pl.BlockSpec((tokens, head_dim), lambda i: (table_part, 0))
    return pl.pallas_call(
        functools.partial(qkv_kernel, n_q, n_rot, len(parts)),
        grid=(steps,),
        in_specs=[full_spec(x.shape) for x in parts] + [
            full_spec(gains.shape), table, table, pl.BlockSpec((per, dim, head_dim), lambda i: (i + skip, 0, 0)),
        ],
        out_specs=tuple(out_specs),
        out_shape=tuple(out_shape),
        scratch_shapes=[pltpu.VMEM((tokens, dim), BF16)],
        compiler_params=params(("arbitrary",)),
        cost_estimate=cost(2 * tokens * dim * steps * per * head_dim, 2 * dim * steps * per * head_dim + 8e6),
        name="qkv" if with_q else "kv",
    )(*parts, gains, cos, sin, w_heads)


BLOCK = 256
HEAD_GROUP = 4
N_SRC = 4
NEG = -1e30


def doc_start(seg, sc_ref, first):
    start = jnp.zeros_like(seg)
    for doc in range(4):
        start = jnp.where(seg > doc, sc_ref[first + doc], start)
    return start


def attn_kernel(sc_ref, q_ref, seg_ref, *refs):
    far_refs, near_refs = refs[:8], refs[8:12]
    o_ref, m_ref, l_ref, acc_ref, bias_ref = refs[12:]
    j = pl.program_id(1)
    heads, _, head_dim = q_ref.shape
    every = range(heads)
    scale = (head_dim ** -0.5) * math.log2(math.e)
    q0 = sc_ref[N_SRC - 1] + j * BLOCK
    first_start = doc_start(sc_ref[N_SRC + 4 + j], sc_ref, N_SRC)
    start = doc_start(seg_ref[...], sc_ref, N_SRC)

    def lanes(x, width):
        return jnp.concatenate([x] * (width // 128), axis=1)

    def fold(x):
        return sum(x[:, i:i + 128] for i in range(128, x.shape[1], 128)) + x[:, :128]

    def weights(h, k_ref, rows, bias):
        s = dot(q_ref[h], k_ref[h, rows, :], NT) + bias
        return s, jnp.max(s, axis=-1, keepdims=True)

    k_ref, v_ref = near_refs[2:]
    rows = pl.ds(pl.multiple_of(j * BLOCK, BLOCK), BLOCK)
    col_id = lax.broadcasted_iota(jnp.int32, (BLOCK, BLOCK), 1)
    row_id = lax.broadcasted_iota(jnp.int32, (BLOCK, BLOCK), 0)
    bias_ref[...] = jnp.where((col_id + q0 >= lanes(start, BLOCK)) & (col_id <= row_id), 0.0, NEG)
    for h in every:
        s, top = weights(h, k_ref, rows, bias_ref[...])
        m_new = jnp.broadcast_to(top, (BLOCK, 128))
        p = jnp.exp2((s - lanes(m_new, BLOCK)) * scale)
        m_ref[h] = m_new
        l_ref[h] = fold(p)
        acc_ref[h] = dot(p.astype(BF16), v_ref[h, rows, :])

    def update(k_ref, v_ref, rows, width, first_col):
        col = lax.broadcasted_iota(jnp.int32, (BLOCK, width), 1) + first_col
        bias = jnp.where(col >= lanes(start, width), 0.0, NEG)
        old = [(m_ref[h], l_ref[h], acc_ref[h]) for h in every]
        scored = [weights(h, k_ref, rows, bias) for h in every]
        m_new = [jnp.maximum(old[h][0], scored[h][1]) for h in every]
        p = [jnp.exp2((scored[h][0] - lanes(m_new[h], width)) * scale) for h in every]
        alpha = [jnp.exp2((old[h][0] - m_new[h]) * scale) for h in every]
        l_new = [old[h][1] * alpha[h] + fold(p[h]) for h in every]
        a_new = [old[h][2] * alpha[h] + dot(p[h].astype(BF16), v_ref[h, rows, :]) for h in every]
        for h in every:
            m_ref[h] = m_new[h]
            l_ref[h] = l_new[h]
            acc_ref[h] = a_new[h]

    for i in (1, 0):
        base = sc_ref[N_SRC - 2 + i]
        k_ref, v_ref = near_refs[2 * i], near_refs[2 * i + 1]
        lo = jnp.maximum(first_start - base, 0) // BLOCK
        hi = jnp.clip(q0 - base, 0, k_ref.shape[1]) // BLOCK

        def body(kb, carry, k_ref=k_ref, v_ref=v_ref, base=base):
            update(k_ref, v_ref, pl.ds(pl.multiple_of(kb * BLOCK, BLOCK), BLOCK), BLOCK, base + kb * BLOCK)
            return carry

        lax.fori_loop(lo, hi, body, 0)

    for i in range(4):
        k_ref, v_ref = far_refs[2 * i], far_refs[2 * i + 1]
        width = k_ref.shape[1]
        base = sc_ref[i // 2] + (i % 2) * width

        @pl.when((base < q0) & (first_start < base + width))
        def _(k_ref=k_ref, v_ref=v_ref, base=base, width=width):
            update(k_ref, v_ref, slice(None), width, base)

    for h in every:
        total = jnp.sum(l_ref[h], axis=-1, keepdims=True)
        o_ref[:, h * head_dim:(h + 1) * head_dim] = (acc_ref[h] / total).astype(BF16)


def attention(scalars, q, seg_wide, kv_list):
    n_heads, tokens, head_dim = q.shape
    per = HEAD_GROUP
    groups = n_heads // per
    in_specs = [
        pl.BlockSpec((per, BLOCK, head_dim), lambda h, j, sc: (h, j, 0)),
        pl.BlockSpec((BLOCK, 128), lambda h, j, sc: (j, 0)),
    ]
    args = [q, seg_wide]
    for kv in kv_list:
        rows = kv.shape[1]
        in_specs.append(pl.BlockSpec((per, rows, head_dim), lambda h, j, sc: (h, 0, 0)))
        in_specs.append(pl.BlockSpec((per, rows, head_dim), lambda h, j, sc: (h + groups, 0, 0)))
        args += [kv, kv]
    return pl.pallas_call(
        attn_kernel,
        grid_spec=pltpu.PrefetchScalarGridSpec(
            num_scalar_prefetch=1,
            grid=(groups, tokens // BLOCK),
            in_specs=in_specs,
            out_specs=pl.BlockSpec((BLOCK, per * head_dim), lambda h, j, sc: (j, h)),
            scratch_shapes=[pltpu.VMEM((per, BLOCK, 128), F32)] * 2
            + [pltpu.VMEM((per, BLOCK, head_dim), F32), pltpu.VMEM((BLOCK, BLOCK), F32)],
        ),
        out_shape=jax.ShapeDtypeStruct((tokens, n_heads * head_dim), BF16),
        compiler_params=params(("arbitrary", "arbitrary")),
        cost_estimate=cost(4 * n_heads * tokens * 2 * tokens * head_dim, 20e6, n_heads * tokens * tokens),
        name="attention",
    )(scalars, *args)


def solution(mesh):
    n_dev = mesh.shape['sp']
    swap_perm = [(d, d ^ 1) for d in range(n_dev)]
    cross_perm = [(d, d + 2) for d in range(n_dev - 2)]
    row_spec = P(('dp', 'sp'), None)
    tok_spec = P(('dp', 'sp'))
    replicated = P()

    def layers(x_rows, seg_ids, norm_gains, w_in, ssm_head, y_gain, w_out, mlp_up, mlp_down, w_qkv, w_attn_out):
        dev = lax.axis_index('sp')
        tokens, dim = x_rows.shape
        inner = y_gain.shape[0]
        n_heads = ssm_head.shape[1]
        n_query, head_dim = w_attn_out.shape[:2]

        counts = jnp.sum((seg_ids[None, :] <= jnp.arange(4, dtype=jnp.int32)[:, None]).astype(jnp.int32), axis=1)
        earlier = [lax.ppermute(counts, 'sp', [(d, d + k) for d in range(n_dev - k)]) for k in range(1, n_dev)]
        seg_wide = jnp.broadcast_to(seg_ids[:, None], (tokens, 128))
        head_pad = jnp.pad(ssm_head, ((0, 5), (0, 128 - n_heads)))
        skip = jnp.repeat(ssm_head[2:3], inner // n_heads, axis=1)
        w_in_t = w_in.T
        hid, xs, bc, dt, cum = in_proj(x_rows, norm_gains, w_in_t, head_pad, inner, n_heads)
        first_pos = dev * tokens
        far = jnp.int32(1 << 24)
        pair_pos = (dev ^ 1) * tokens
        earlier, cum = lax.optimization_barrier((earlier, cum))
        doc_starts = counts + sum(earlier)
        slot = jnp.arange(4, dtype=jnp.int32)
        bases = jnp.where(slot == 3, first_pos, pair_pos)
        bases = jnp.where(slot >= 2, bases, jnp.where(dev >= 2, jnp.where(slot == 0, first_pos, pair_pos) - 2 * tokens, far))
        edge_seg = jnp.pad(seg_ids[::BLOCK], (0, 8 - tokens // BLOCK))
        scalars = jnp.concatenate([bases, doc_starts, edge_seg])
        state_end, decay = ssd_state(scalars, xs, bc, dt, cum, seg_wide)

        odd = (dev % 2) == 1
        pair_state = lax.ppermute(state_end, 'sp', swap_perm)
        pair_decay = lax.ppermute(decay, 'sp', swap_perm)
        chip_state = jnp.where(odd, decay * pair_state + state_end, pair_decay * state_end + pair_state)
        half = state_end.shape[0] // 2
        mine = jnp.where(odd, chip_state[half:], chip_state[:half])
        mine, hid = lax.optimization_barrier((mine, hid))
        got = lax.ppermute(mine, 'sp', cross_perm)
        z = z_proj(hid, w_in_t, inner)
        pos = (first_pos + jnp.arange(tokens)).astype(F32)
        cos, sin = rope_tables(pos, head_dim)
        cos_far, sin_far = rope_tables(pos - 2.0 * tokens, head_dim)
        got, z, cos, sin, cos_far, sin_far = lax.optimization_barrier((got, z, cos, sin, cos_far, sin_far))
        other = lax.ppermute(got, 'sp', swap_perm)
        chip_in = jnp.where(odd, jnp.concatenate([other, got], axis=0), jnp.concatenate([got, other], axis=0))
        h_in = jnp.where(odd, pair_decay * chip_in + pair_state, chip_in)

        gated = ssd_full(scalars, xs, bc, dt, cum, seg_wide, z, h_in, skip, y_gain[None, :])
        x_one = proj_add(gated, w_out, [x_rows])
        x_a = mlp(x_one, norm_gains, mlp_up, mlp_down, 0, 0, 2)
        far_a = lax.ppermute(x_a, 'sp', cross_perm)
        x_one, x_a = lax.optimization_barrier((x_one, x_a))
        x_b = mlp(x_one, norm_gains, mlp_up, mlp_down, 0, 1, 2)
        far_b = lax.ppermute(x_b, 'sp', cross_perm)
        w_heads = w_qkv.transpose(1, 0, 2)
        q, kv = qkv_proj([x_a, x_b], norm_gains, cos, sin, 0, w_heads, n_query, True)
        kv_pair = lax.ppermute(kv, 'sp', swap_perm)
        far_a, q = lax.optimization_barrier((far_a, q))
        kv_far_a, = qkv_proj([far_a], norm_gains, cos_far, sin_far, 0, w_heads, n_query, False)
        kv_fp_a = lax.ppermute(kv_far_a, 'sp', swap_perm)
        far_b, kv_far_a = lax.optimization_barrier((far_b, kv_far_a))
        kv_far_b, = qkv_proj([far_b], norm_gains, cos_far, sin_far, 1, w_heads, n_query, False)
        kv_fp_b = lax.ppermute(kv_far_b, 'sp', swap_perm)
        attn = attention(scalars, q, seg_wide, [kv_far_a, kv_far_b, kv_fp_a, kv_fp_b, kv_pair, kv])
        x_three = proj_add(attn, w_attn_out.reshape(n_query * head_dim, dim), [x_a, x_b])
        return mlp(x_three, norm_gains, mlp_up, mlp_down, 1, 0, 1)

    return jax.shard_map(layers, mesh=mesh, in_specs=(row_spec, tok_spec) + (replicated,) * 9, out_specs=row_spec, check_vma=False)
```

```python
import functools
import math

import jax
import jax.numpy as jnp
from jax import lax
from jax.experimental import pallas as pl
from jax.experimental.pallas import tpu as pltpu
from jax.sharding import PartitionSpec as P


CHUNK = 64
NORM_EPS = 1e-6
ROPE_BASE = 10000.0
F32 = jnp.float32
BF16 = jnp.bfloat16
NT = (((1,), (1,)), ((), ()))


def dot(a, b, dims=(((1,), (0,)), ((), ()))):
    return lax.dot_general(a, b, dims, preferred_element_type=F32)


def params(sem, mib):
    return pltpu.CompilerParams(dimension_semantics=sem, vmem_limit_bytes=mib * 1024 * 1024)


def cost(flops, bytes_accessed, trans=0):
    return pl.CostEstimate(flops=int(flops), bytes_accessed=int(bytes_accessed), transcendentals=int(trans))


def norm_rows(values, gain):
    wide = values.astype(F32)
    inv = lax.rsqrt(jnp.mean(wide * wide, axis=-1, keepdims=True) + NORM_EPS)
    return (wide * inv * gain).astype(BF16)


SMEM_SPEC = pl.BlockSpec(memory_space=pltpu.SMEM)


def full_spec(shape):
    zeros = (0,) * len(shape)
    return pl.BlockSpec(shape, lambda *_: zeros)


def in_proj_kernel(n_heads, x_ref, gain_ref, w_ref, head_ref, h_ref, xs_ref, bc_ref, dt_ref, cum_ref):
    step = pl.program_id(0)

    @pl.when(step == 0)
    def _():
        hid = norm_rows(x_ref[...], gain_ref[0:1, :])
        h_ref[...] = hid
        n_bc = bc_ref.shape[1]
        out = dot(hid, w_ref[:n_bc + dt_ref.shape[1], :], NT)
        bc_ref[...] = out[:, :n_bc].astype(BF16)
        lanes = dt_ref.shape[1]
        raw = out[:, n_bc:n_bc + lanes] + head_ref[0:1, :]
        dt = jnp.maximum(raw, 0.0) + jnp.log1p(jnp.exp(-jnp.abs(raw)))
        lane = lax.broadcasted_iota(jnp.int32, dt.shape, 1)
        dt = jnp.where(lane < n_heads, dt, 0.0)
        dt_ref[...] = dt
        cum = dt * head_ref[1:2, :]
        row = lax.broadcasted_iota(jnp.int32, dt.shape, 0) % CHUNK
        shift = 1
        while shift < CHUNK:
            cum = cum + jnp.where(row >= shift, pltpu.roll(cum, shift, 0), 0.0)
            shift *= 2
        cum_ref[...] = cum

    @pl.when(step > 0)
    def _():
        xs_ref[...] = dot(h_ref[...], w_ref[...], NT).astype(BF16)


def in_proj(x_rows, gains, w_in_t, head_pad, inner, n_heads):
    tokens, dim = x_rows.shape
    tile = 1024
    n_x = inner // tile
    last = 2 * inner // tile
    out_shape = (
        jax.ShapeDtypeStruct((tokens, dim), BF16),
        jax.ShapeDtypeStruct((tokens, inner), BF16),
        jax.ShapeDtypeStruct((tokens, 256), BF16),
        jax.ShapeDtypeStruct((tokens, 128), F32),
        jax.ShapeDtypeStruct((tokens, 128), F32),
    )
    return pl.pallas_call(
        functools.partial(in_proj_kernel, n_heads),
        grid=(n_x + 1,),
        in_specs=[
            full_spec((tokens, dim)),
            full_spec(gains.shape),
            pl.BlockSpec((tile, dim), lambda i: (jnp.where(i == 0, last, i - 1), 0)),
            full_spec((8, 128)),
        ],
        out_specs=(
            full_spec((tokens, dim)),
            pl.BlockSpec((tokens, tile), lambda i: (0, jnp.maximum(i - 1, 0))),
            full_spec((tokens, 256)),
            full_spec((tokens, 128)),
            full_spec((tokens, 128)),
        ),
        out_shape=out_shape,
        compiler_params=params(("arbitrary",), 40),
        cost_estimate=cost(2 * tokens * dim * (inner + tile), 16e6),
        name="in_proj",
    )(x_rows, gains, w_in_t, head_pad)


def z_proj_kernel(h_ref, w_ref, z_ref):
    z = dot(h_ref[...], w_ref[...], NT)
    z_ref[...] = z * jax.nn.sigmoid(z)


def z_proj(hid, w_in_t, inner):
    tokens, dim = hid.shape
    tile = 1024
    first = inner // tile
    return pl.pallas_call(
        z_proj_kernel,
        grid=(inner // tile,),
        in_specs=[full_spec((tokens, dim)), pl.BlockSpec((tile, dim), lambda i: (i + first, 0))],
        out_specs=pl.BlockSpec((tokens, tile), lambda i: (0, i)),
        out_shape=jax.ShapeDtypeStruct((tokens, inner), F32),
        compiler_params=params(("arbitrary",), 40),
        cost_estimate=cost(2 * tokens * dim * inner, 21e6),
        name="z_proj",
    )(hid, w_in_t)


STEP = 2 * CHUNK
LOG2E = math.log2(math.e)


def split3(x):
    hi = x.astype(BF16).astype(F32)
    rest = x - hi
    mid = rest.astype(BF16).astype(F32)
    low = rest - mid
    return jnp.concatenate([hi + pltpu.roll(mid, 64, 1), low], axis=1).astype(BF16)


def fill_spread(e_ref):
    rows, width = e_ref.shape
    for g in range(width // 512):
        head = lax.broadcasted_iota(jnp.int32, (rows, 512), 0) % 64
        lane = lax.broadcasted_iota(jnp.int32, (rows, 512), 1) + g * 512
        e_ref[:, g * 512:(g + 1) * 512] = jnp.where(head == lane // 64, 1.0, 0.0).astype(BF16)


def step_weights(sc_ref, seg_ref, dt, cum2):
    row = lax.broadcasted_iota(jnp.int32, (STEP, 128), 0)
    start = doc_start(seg_ref[...], sc_ref, N_SRC) - (sc_ref[N_SRC - 1] + pl.program_id(0) * STEP)
    upper = row < CHUNK
    last = lambda v: jnp.where(upper, v[CHUNK - 1:CHUNK, :], v[STEP - 1:STEP, :])
    end_w = jnp.where(row >= last(start), jnp.exp2(last(cum2) - cum2), 0.0) * dt
    rel = jnp.where(upper, start, start - CHUNK)
    return rel, end_w


def half_rows(c):
    return slice(c * CHUNK, (c + 1) * CHUNK)


def b_transposed(bc_ref, c):
    return bc_ref[half_rows(c), :128].astype(F32).T.astype(BF16)


def ssd_state_kernel(sc_ref, x_ref, bc_ref, dt_ref, cum_ref, seg_ref, end_ref, decay_ref, e_ref, xp_ref, xw_ref):
    @pl.when(pl.program_id(0) == 0)
    def _():
        end_ref[...] = jnp.zeros_like(end_ref)
        decay_ref[...] = jnp.ones_like(decay_ref)
        fill_spread(e_ref)

    cum2 = cum_ref[...] * LOG2E
    rel, end_w = step_weights(sc_ref, seg_ref, dt_ref[...], cum2)
    lane = lax.broadcasted_iota(jnp.int32, (STEP, 128), 1)
    carry = jnp.where((rel < 0) & (lane < 64), jnp.exp2(cum2), 0.0)
    ends = [jnp.broadcast_to(carry[r:r + 1, :], (8, 128)) for r in (CHUNK - 1, STEP - 1)]
    xp_ref[...] = dot(split3(jnp.concatenate([end_w] + ends, axis=0)), e_ref[...])
    xw_ref[...] = (x_ref[...].astype(F32) * xp_ref[:STEP, :]).astype(BF16)
    add = [dot(b_transposed(bc_ref, c), xw_ref[half_rows(c), :]) for c in range(2)]
    dec = [xp_ref[STEP + 8 * c:STEP + 8 * c + 1, :] for c in range(2)]
    end_ref[...] = dec[1] * (dec[0] * end_ref[...] + add[0]) + add[1]
    decay_ref[...] = decay_ref[...] * dec[0] * dec[1]


def ssd_state(scalars, xs, bc, dt, cum, seg_wide):
    tokens, inner = xs.shape
    row = lambda width: pl.BlockSpec((STEP, width), lambda i: (i, 0))
    return pl.pallas_call(
        ssd_state_kernel,
        grid=(tokens // STEP,),
        in_specs=[SMEM_SPEC, row(inner), row(256), row(128), row(128), row(128)],
        out_specs=(full_spec((128, inner)), full_spec((1, inner))),
        out_shape=(jax.ShapeDtypeStruct((128, inner), F32), jax.ShapeDtypeStruct((1, inner), F32)),
        scratch_shapes=[pltpu.VMEM((256, inner), BF16), pltpu.VMEM((STEP + 16, inner), F32), pltpu.VMEM((STEP, inner), BF16)],
        compiler_params=params(("arbitrary",), 40),
        cost_estimate=cost(2 * tokens * 256 * inner, 8e6),
        name="ssd_state",
    )(scalars, xs, bc, dt, cum, seg_wide)


def ssd_full_kernel(sc_ref, x_ref, bc_ref, dt_ref, cum_ref, seg_ref, z_ref, hin_ref, skip_ref, gain_ref, out_ref,
                    state_ref, y_ref, e_ref, xp_ref, xw_ref, turn_ref, pack_ref):
    @pl.when(pl.program_id(0) == 0)
    def _():
        state_ref[...] = hin_ref[...]
        fill_spread(e_ref)

    inner = x_ref.shape[1]
    n_heads = inner // 64
    dt = dt_ref[...]
    cum2 = cum_ref[...] * LOG2E
    rel, end_w = step_weights(sc_ref, seg_ref, dt, cum2)
    xp_ref[...] = dot(split3(jnp.concatenate([cum2, end_w], axis=0)), e_ref[...])
    xw_ref[...] = (x_ref[...].astype(F32) * xp_ref[STEP:, :]).astype(BF16)

    turn_ref[0] = cum2.T
    turn_ref[1] = dt.T
    left = lax.broadcasted_iota(jnp.int32, (n_heads // 2, STEP), 1) < 64
    for k in range(2):
        even = turn_ref[k, pl.ds(0, n_heads // 2, stride=2), :]
        odd = turn_ref[k, pl.ds(1, n_heads // 2, stride=2), :]
        pack_ref[0, k] = jnp.where(left, even, pltpu.roll(odd, 64, 1))
        pack_ref[1, k] = jnp.where(left, pltpu.roll(even, 64, 1), odd)

    row_id = lax.broadcasted_iota(jnp.int32, (CHUNK, 128), 0)
    lane_id = lax.broadcasted_iota(jnp.int32, (CHUNK, 128), 1)
    left = lane_id < 64
    src = jnp.where(left, lane_id, lane_id - 64)
    for c in range(2):
        rows = half_rows(c)
        state = state_ref[...]
        opens = rel[rows] < 0
        c_open = jnp.where(opens, bc_ref[rows, 128:].astype(F32), 0.0).astype(BF16)
        carried = dot(c_open, state.astype(BF16))
        carry_x = jnp.exp2(xp_ref[rows, :])
        keep = jnp.where(opens[CHUNK - 1:CHUNK, :], 1.0, 0.0)
        dec = carry_x[CHUNK - 1:CHUNK, :] * jnp.concatenate([keep] * (inner // 128), axis=1)
        y_ref[rows, :] = carried * carry_x + skip_ref[...] * x_ref[rows, :].astype(F32)
        state_ref[...] = dec * state + dot(b_transposed(bc_ref, c), xw_ref[rows, :])

    for c in range(2):
        rows = half_rows(c)
        visible = (src >= rel[rows]) & (src <= row_id)
        b_blk = bc_ref[rows, :128]
        scores = dot(bc_ref[rows, 128:], jnp.concatenate([b_blk, b_blk], axis=0), NT)
        scores = jnp.where(visible, scores, 0.0)
        left16 = lax.broadcasted_iota(jnp.int32, (CHUNK, 128), 1) < 64
        zero = jnp.zeros((CHUNK, 128), BF16)
        for g in range(inner // 256):
            cols = slice(g * 256, (g + 1) * 256)
            mixes, diag = [], []
            for k in range(2):
                pair = 2 * g + k
                sub = slice(pair * 128, (pair + 1) * 128)
                cum_s = pack_ref[c, 0, pair:pair + 1, :]
                dt_s = pack_ref[c, 1, pair:pair + 1, :]
                decay = jnp.exp2(jnp.minimum(xp_ref[rows, sub] - cum_s, 0.0))
                mixes.append((scores * decay * dt_s).astype(BF16))
                xk = x_ref[rows, sub]
                for keep in (jnp.where(left16, xk, zero), jnp.where(left16, zero, xk)):
                    diag.append(jnp.concatenate([keep, zero] if k == 0 else [zero, keep], axis=1))
            y_ref[rows, cols] += dot(jnp.concatenate(mixes, axis=1), jnp.concatenate(diag, axis=0))

    y = y_ref[...]
    inv = lax.rsqrt(jnp.mean(y * y, axis=-1, keepdims=True) + NORM_EPS)
    out_ref[...] = (y * inv * gain_ref[...] * z_ref[...]).astype(BF16)


def ssd_full(scalars, xs, bc, dt, cum, seg_wide, z, h_in, skip, gain):
    tokens, inner = xs.shape
    row = lambda width: pl.BlockSpec((STEP, width), lambda i: (i, 0))
    return pl.pallas_call(
        ssd_full_kernel,
        grid=(tokens // STEP,),
        in_specs=[
            SMEM_SPEC, row(inner), row(256), row(128), row(128), row(128),
            row(inner), full_spec((128, inner)), full_spec((1, inner)), full_spec((1, inner)),
        ],
        out_specs=row(inner),
        out_shape=jax.ShapeDtypeStruct((tokens, inner), BF16),
        scratch_shapes=[
            pltpu.VMEM((128, inner), F32), pltpu.VMEM((STEP, inner), F32), pltpu.VMEM((256, inner), BF16),
            pltpu.VMEM((2 * STEP, inner), F32), pltpu.VMEM((STEP, inner), BF16), pltpu.VMEM((2, 128, STEP), F32),
            pltpu.VMEM((2, 2, inner // 128, STEP), F32),
        ],
        compiler_params=params(("arbitrary",), 40),
        cost_estimate=cost(12e9, 20e6),
        name="ssd_full",
    )(scalars, xs, bc, dt, cum, seg_wide, z, h_in, skip, gain)


def proj_add_kernel(a_ref, w_ref, *refs):
    out_ref = refs[-1]
    res = jnp.concatenate([r[...] for r in refs[:-1]], axis=0)
    out_ref[...] = (res.astype(F32) + dot(a_ref[...], w_ref[...])).astype(BF16)


def proj_add(a, w, res):
    tokens, depth = a.shape
    dim = w.shape[1]
    tile = 512
    col = lambda rows: pl.BlockSpec((rows, tile), lambda i: (0, i))
    return pl.pallas_call(
        proj_add_kernel,
        grid=(dim // tile,),
        in_specs=[full_spec((tokens, depth)), col(depth)] + [col(r.shape[0]) for r in res],
        out_specs=col(tokens),
        out_shape=jax.ShapeDtypeStruct((tokens, dim), BF16),
        compiler_params=params(("arbitrary",), 40),
        cost_estimate=cost(2 * tokens * depth * dim, 2 * (tokens * depth + depth * dim + 2 * tokens * dim)),
        name="proj_add",
    )(a, w, *res)


def mlp_kernel(layer, x_ref, gain_ref, wg_ref, wu_ref, wd_ref, out_ref, h_ref, acc_ref):
    step = pl.program_id(0)

    @pl.when(step == 0)
    def _():
        h_ref[...] = norm_rows(x_ref[...], gain_ref[2 * layer + 1:2 * layer + 2, :])
        acc_ref[...] = jnp.zeros_like(acc_ref)

    hid = h_ref[...]
    gate = dot(hid, wg_ref[0])
    up = dot(hid, wu_ref[0])
    act = (gate * jax.nn.sigmoid(gate) * up).astype(BF16)
    acc_ref[...] += dot(act, wd_ref[0])

    @pl.when(step == pl.num_programs(0) - 1)
    def _():
        out_ref[...] = (x_ref[...].astype(F32) + acc_ref[...]).astype(BF16)


def mlp(x_rows, gains, mlp_up, mlp_down, layer, part, parts):
    tokens, dim = x_rows.shape
    tokens //= parts
    ff = mlp_down.shape[1]
    tile = 512 * parts
    n_ff = ff // tile
    return pl.pallas_call(
        functools.partial(mlp_kernel, layer),
        grid=(n_ff,),
        in_specs=[
            pl.BlockSpec((tokens, dim), lambda i: (part, 0)),
            full_spec(gains.shape),
            pl.BlockSpec((1, dim, tile), lambda i: (layer, 0, i)),
            pl.BlockSpec((1, dim, tile), lambda i: (layer, 0, i + n_ff)),
            pl.BlockSpec((1, tile, dim), lambda i: (layer, i, 0)),
        ],
        out_specs=full_spec((tokens, dim)),
        out_shape=jax.ShapeDtypeStruct((tokens, dim), BF16),
        scratch_shapes=[pltpu.VMEM((tokens, dim), BF16), pltpu.VMEM((tokens, dim), F32)],
        compiler_params=params(("arbitrary",), 40),
        cost_estimate=cost(6 * tokens * dim * ff, 6 * dim * ff),
        name="mlp",
    )(x_rows, gains, mlp_up, mlp_up, mlp_down)


def rope_tables(positions, head_dim):
    half = head_dim // 2
    inv_freq = ROPE_BASE ** (-jnp.arange(half, dtype=F32) * 2.0 / head_dim)
    angle = positions[:, None] * inv_freq[None, :]
    cos, sin = jnp.cos(angle), jnp.sin(angle)
    return jnp.concatenate([cos, cos], axis=1), jnp.concatenate([-sin, sin], axis=1)


def qkv_kernel(n_q, n_rot, n_parts, *refs):
    x_refs = refs[:n_parts]
    gain_ref, cos_ref, sin_ref, w_ref = refs[n_parts:n_parts + 4]
    kv_ref, h_ref = refs[-2:]
    step = pl.program_id(0)

    @pl.when(step == 0)
    def _():
        first = 0
        for x_ref in x_refs:
            h_ref[first:first + x_ref.shape[0]] = norm_rows(x_ref[...], gain_ref[2:3, :])
            first += x_ref.shape[0]

    heads, _, head_dim = w_ref.shape
    turns = step < n_rot
    cos = jnp.where(turns, cos_ref[...], 1.0)
    sin = jnp.where(turns, sin_ref[...], 0.0)
    for k in range(0, heads, 2):
        out = dot(h_ref[...], jnp.concatenate([w_ref[k], w_ref[k + 1]], axis=1))
        for i in range(2):
            val = out[:, i * head_dim:(i + 1) * head_dim]
            kv_ref[k + i] = (val * cos + pltpu.roll(val, head_dim // 2, 1) * sin).astype(BF16)

    if n_q:
        @pl.when(step < n_q)
        def _():
            refs[n_parts + 4][...] = kv_ref[...]


def qkv_proj(parts, gains, cos, sin, table_part, w_heads, n_query, with_q):
    tokens = sum(x.shape[0] for x in parts)
    dim = parts[0].shape[1]
    n_heads, _, head_dim = w_heads.shape
    n_kv = n_heads - n_query
    per = 6
    n_q = n_query // per if with_q else 0
    skip = 0 if with_q else n_query // per
    n_rot = n_q + n_kv // 2 // per
    steps = n_heads // per - skip
    out_specs = [pl.BlockSpec((per, tokens, head_dim), lambda i: (jnp.maximum(i - n_q, 0), 0, 0))]
    out_shape = [jax.ShapeDtypeStruct((n_kv, tokens, head_dim), BF16)]
    if with_q:
        out_specs.insert(0, pl.BlockSpec((per, tokens, head_dim), lambda i: (jnp.minimum(i, n_q - 1), 0, 0)))
        out_shape.insert(0, jax.ShapeDtypeStruct((n_query, tokens, head_dim), BF16))
    table = pl.BlockSpec((tokens, head_dim), lambda i: (table_part, 0))
    return pl.pallas_call(
        functools.partial(qkv_kernel, n_q, n_rot, len(parts)),
        grid=(steps,),
        in_specs=[full_spec(x.shape) for x in parts] + [
            full_spec(gains.shape), table, table, pl.BlockSpec((per, dim, head_dim), lambda i: (i + skip, 0, 0)),
        ],
        out_specs=tuple(out_specs),
        out_shape=tuple(out_shape),
        scratch_shapes=[pltpu.VMEM((tokens, dim), BF16)],
        compiler_params=params(("arbitrary",), 40),
        cost_estimate=cost(2 * tokens * dim * steps * per * head_dim, 2 * dim * steps * per * head_dim + 8e6),
        name="qkv" if with_q else "kv",
    )(*parts, gains, cos, sin, w_heads)


BLOCK = 256
HEAD_GROUP = 4
N_SRC = 4
NEG = -1e30


def doc_start(seg, sc_ref, first):
    start = jnp.zeros_like(seg)
    for doc in range(4):
        start = jnp.where(seg > doc, sc_ref[first + doc], start)
    return start


def attn_kernel(sc_ref, q_ref, seg_ref, *refs):
    far_refs, near_refs = refs[:8], refs[8:12]
    o_ref, m_ref, l_ref, acc_ref, bias_ref = refs[12:]
    j = pl.program_id(1)
    heads, _, head_dim = q_ref.shape
    every = range(heads)
    scale = (head_dim ** -0.5) * math.log2(math.e)
    q0 = sc_ref[N_SRC - 1] + j * BLOCK
    first_start = doc_start(sc_ref[N_SRC + 4 + j], sc_ref, N_SRC)
    start = doc_start(seg_ref[...], sc_ref, N_SRC)

    def lanes(x, width):
        return jnp.concatenate([x] * (width // 128), axis=1)

    def fold(x):
        return sum(x[:, i:i + 128] for i in range(128, x.shape[1], 128)) + x[:, :128]

    def weights(h, k_ref, rows, bias):
        s = dot(q_ref[h], k_ref[h, rows, :], NT) + bias
        return s, jnp.max(s, axis=-1, keepdims=True)

    k_ref, v_ref = near_refs[2:]
    rows = pl.ds(pl.multiple_of(j * BLOCK, BLOCK), BLOCK)
    col_id = lax.broadcasted_iota(jnp.int32, (BLOCK, BLOCK), 1)
    row_id = lax.broadcasted_iota(jnp.int32, (BLOCK, BLOCK), 0)
    bias_ref[...] = jnp.where((col_id + q0 >= lanes(start, BLOCK)) & (col_id <= row_id), 0.0, NEG)
    for h in every:
        s, top = weights(h, k_ref, rows, bias_ref[...])
        m_new = jnp.broadcast_to(top, (BLOCK, 128))
        p = jnp.exp2((s - lanes(m_new, BLOCK)) * scale)
        m_ref[h] = m_new
        l_ref[h] = fold(p)
        acc_ref[h] = dot(p.astype(BF16), v_ref[h, rows, :])

    def update(k_ref, v_ref, rows, width, first_col):
        col = lax.broadcasted_iota(jnp.int32, (BLOCK, width), 1) + first_col
        bias = jnp.where(col >= lanes(start, width), 0.0, NEG)
        old = [(m_ref[h], l_ref[h], acc_ref[h]) for h in every]
        scored = [weights(h, k_ref, rows, bias) for h in every]
        m_new = [jnp.maximum(old[h][0], scored[h][1]) for h in every]
        p = [jnp.exp2((scored[h][0] - lanes(m_new[h], width)) * scale) for h in every]
        alpha = [jnp.exp2((old[h][0] - m_new[h]) * scale) for h in every]
        l_new = [old[h][1] * alpha[h] + fold(p[h]) for h in every]
        a_new = [old[h][2] * alpha[h] + dot(p[h].astype(BF16), v_ref[h, rows, :]) for h in every]
        for h in every:
            m_ref[h] = m_new[h]
            l_ref[h] = l_new[h]
            acc_ref[h] = a_new[h]

    for i in (1, 0):
        base = sc_ref[N_SRC - 2 + i]
        k_ref, v_ref = near_refs[2 * i], near_refs[2 * i + 1]
        lo = jnp.maximum(first_start - base, 0) // BLOCK
        hi = jnp.clip(q0 - base, 0, k_ref.shape[1]) // BLOCK

        def body(kb, carry, k_ref=k_ref, v_ref=v_ref, base=base):
            update(k_ref, v_ref, pl.ds(pl.multiple_of(kb * BLOCK, BLOCK), BLOCK), BLOCK, base + kb * BLOCK)
            return carry

        lax.fori_loop(lo, hi, body, 0)

    for i in range(4):
        k_ref, v_ref = far_refs[2 * i], far_refs[2 * i + 1]
        width = k_ref.shape[1]
        base = sc_ref[i // 2] + (i % 2) * width

        @pl.when((base < q0) & (first_start < base + width))
        def _(k_ref=k_ref, v_ref=v_ref, base=base, width=width):
            update(k_ref, v_ref, slice(None), width, base)

    for h in every:
        total = jnp.sum(l_ref[h], axis=-1, keepdims=True)
        o_ref[:, h * head_dim:(h + 1) * head_dim] = (acc_ref[h] / total).astype(BF16)


def attention(scalars, q, seg_wide, kv_list):
    n_heads, tokens, head_dim = q.shape
    per = HEAD_GROUP
    groups = n_heads // per
    in_specs = [
        pl.BlockSpec((per, BLOCK, head_dim), lambda h, j, sc: (h, j, 0)),
        pl.BlockSpec((BLOCK, 128), lambda h, j, sc: (j, 0)),
    ]
    args = [q, seg_wide]
    for kv in kv_list:
        rows = kv.shape[1]
        in_specs.append(pl.BlockSpec((per, rows, head_dim), lambda h, j, sc: (h, 0, 0)))
        in_specs.append(pl.BlockSpec((per, rows, head_dim), lambda h, j, sc: (h + groups, 0, 0)))
        args += [kv, kv]
    return pl.pallas_call(
        attn_kernel,
        grid_spec=pltpu.PrefetchScalarGridSpec(
            num_scalar_prefetch=1,
            grid=(groups, tokens // BLOCK),
            in_specs=in_specs,
            out_specs=pl.BlockSpec((BLOCK, per * head_dim), lambda h, j, sc: (j, h)),
            scratch_shapes=[pltpu.VMEM((per, BLOCK, 128), F32)] * 2
            + [pltpu.VMEM((per, BLOCK, head_dim), F32), pltpu.VMEM((BLOCK, BLOCK), F32)],
        ),
        out_shape=jax.ShapeDtypeStruct((tokens, n_heads * head_dim), BF16),
        compiler_params=params(("arbitrary", "arbitrary"), 40),
        cost_estimate=cost(4 * n_heads * tokens * 2 * tokens * head_dim, 20e6, n_heads * tokens * tokens),
        name="attention",
    )(scalars, *args)


def solution(mesh):
    n_dev = mesh.shape['sp']
    swap_perm = [(d, d ^ 1) for d in range(n_dev)]
    cross_perm = [(d, d + 2) for d in range(n_dev - 2)]
    row_spec = P(('dp', 'sp'), None)
    tok_spec = P(('dp', 'sp'))
    replicated = P()

    def layers(x_rows, seg_ids, norm_gains, w_in, ssm_head, y_gain, w_out, mlp_up, mlp_down, w_qkv, w_attn_out):
        dev = lax.axis_index('sp')
        tokens, dim = x_rows.shape
        inner = y_gain.shape[0]
        n_heads = ssm_head.shape[1]
        n_query, head_dim = w_attn_out.shape[:2]

        counts = jnp.sum((seg_ids[None, :] <= jnp.arange(4, dtype=jnp.int32)[:, None]).astype(jnp.int32), axis=1)
        earlier = [lax.ppermute(counts, 'sp', [(d, d + k) for d in range(n_dev - k)]) for k in range(1, n_dev)]
        seg_wide = jnp.broadcast_to(seg_ids[:, None], (tokens, 128))
        head_pad = jnp.pad(ssm_head, ((0, 5), (0, 128 - n_heads)))
        skip = jnp.repeat(ssm_head[2:3], inner // n_heads, axis=1)
        w_in_t = w_in.T
        hid, xs, bc, dt, cum = in_proj(x_rows, norm_gains, w_in_t, head_pad, inner, n_heads)
        first_pos = dev * tokens
        far = jnp.int32(1 << 24)
        pair_pos = (dev ^ 1) * tokens
        earlier, cum = lax.optimization_barrier((earlier, cum))
        doc_starts = counts + sum(earlier)
        slot = jnp.arange(4, dtype=jnp.int32)
        bases = jnp.where(slot == 3, first_pos, pair_pos)
        bases = jnp.where(slot >= 2, bases, jnp.where(dev >= 2, jnp.where(slot == 0, first_pos, pair_pos) - 2 * tokens, far))
        edge_seg = jnp.pad(seg_ids[::BLOCK], (0, 8 - tokens // BLOCK))
        scalars = jnp.concatenate([bases, doc_starts, edge_seg])
        state_end, decay = ssd_state(scalars, xs, bc, dt, cum, seg_wide)

        odd = (dev % 2) == 1
        pair_state = lax.ppermute(state_end, 'sp', swap_perm)
        pair_decay = lax.ppermute(decay, 'sp', swap_perm)
        chip_state = jnp.where(odd, decay * pair_state + state_end, pair_decay * state_end + pair_state)
        half = state_end.shape[0] // 2
        mine = jnp.where(odd, chip_state[half:], chip_state[:half])
        mine, hid = lax.optimization_barrier((mine, hid))
        got = lax.ppermute(mine, 'sp', cross_perm)
        z = z_proj(hid, w_in_t, inner)
        pos = (first_pos + jnp.arange(tokens)).astype(F32)
        cos, sin = rope_tables(pos, head_dim)
        cos_far, sin_far = rope_tables(pos - 2.0 * tokens, head_dim)
        got, z, cos, sin, cos_far, sin_far = lax.optimization_barrier((got, z, cos, sin, cos_far, sin_far))
        other = lax.ppermute(got, 'sp', swap_perm)
        chip_in = jnp.where(odd, jnp.concatenate([other, got], axis=0), jnp.concatenate([got, other], axis=0))
        h_in = jnp.where(odd, pair_decay * chip_in + pair_state, chip_in)

        gated = ssd_full(scalars, xs, bc, dt, cum, seg_wide, z, h_in, skip, y_gain[None, :])
        x_one = proj_add(gated, w_out, [x_rows])
        x_a = mlp(x_one, norm_gains, mlp_up, mlp_down, 0, 0, 2)
        far_a = lax.ppermute(x_a, 'sp', cross_perm)
        x_one, x_a = lax.optimization_barrier((x_one, x_a))
        x_b = mlp(x_one, norm_gains, mlp_up, mlp_down, 0, 1, 2)
        far_b = lax.ppermute(x_b, 'sp', cross_perm)
        w_heads = w_qkv.transpose(1, 0, 2)
        q, kv = qkv_proj([x_a, x_b], norm_gains, cos, sin, 0, w_heads, n_query, True)
        kv_pair = lax.ppermute(kv, 'sp', swap_perm)
        far_a, q = lax.optimization_barrier((far_a, q))
        kv_far_a, = qkv_proj([far_a], norm_gains, cos_far, sin_far, 0, w_heads, n_query, False)
        kv_fp_a = lax.ppermute(kv_far_a, 'sp', swap_perm)
        far_b, kv_far_a = lax.optimization_barrier((far_b, kv_far_a))
        kv_far_b, = qkv_proj([far_b], norm_gains, cos_far, sin_far, 1, w_heads, n_query, False)
        kv_fp_b = lax.ppermute(kv_far_b, 'sp', swap_perm)
        attn = attention(scalars, q, seg_wide, [kv_far_a, kv_far_b, kv_fp_a, kv_fp_b, kv_pair, kv])
        x_three = proj_add(attn, w_attn_out.reshape(n_query * head_dim, dim), [x_a, x_b])
        return mlp(x_three, norm_gains, mlp_up, mlp_down, 1, 0, 1)

    return jax.shard_map(layers, mesh=mesh, in_specs=(row_spec, tok_spec) + (replicated,) * 9, out_specs=row_spec, check_vma=False)
```

```python
import functools
import math

import jax
import jax.numpy as jnp
from jax import lax
from jax.experimental import pallas as pl
from jax.experimental.pallas import tpu as pltpu
from jax.sharding import PartitionSpec as P


CHUNK = 64
NORM_EPS = 1e-6
ROPE_BASE = 10000.0
LANES = 128
F32 = jnp.float32
BF16 = jnp.bfloat16
NT = (((1,), (1,)), ((), ()))


def dot(a, b, dims=(((1,), (0,)), ((), ()))):
    return lax.dot_general(a, b, dims, preferred_element_type=F32)


def params(sem, mib):
    return pltpu.CompilerParams(dimension_semantics=sem, vmem_limit_bytes=mib * 1024 * 1024)


def cost(flops, bytes_accessed, trans=0):
    return pl.CostEstimate(flops=int(flops), bytes_accessed=int(bytes_accessed), transcendentals=int(trans))


def norm_rows(values, gain):
    wide = values.astype(F32)
    inv = lax.rsqrt(jnp.mean(wide * wide, axis=-1, keepdims=True) + NORM_EPS)
    return (wide * inv * gain).astype(BF16)


SMEM_SPEC = pl.BlockSpec(memory_space=pltpu.SMEM)


def full_spec(shape):
    zeros = (0,) * len(shape)
    return pl.BlockSpec(shape, lambda *_: zeros)


def in_proj_kernel(n_heads, x_ref, gain_ref, w_ref, head_ref, h_ref, xs_ref, bc_ref, dt_ref, cum_ref):
    step = pl.program_id(0)

    @pl.when(step == 0)
    def _():
        hid = norm_rows(x_ref[...], gain_ref[0:1, :])
        h_ref[...] = hid
        n_bc = bc_ref.shape[1]
        out = dot(hid, w_ref[:n_bc + dt_ref.shape[1], :], NT)
        bc_ref[...] = out[:, :n_bc].astype(BF16)
        lanes = dt_ref.shape[1]
        raw = out[:, n_bc:n_bc + lanes] + head_ref[0:1, :]
        dt = jnp.maximum(raw, 0.0) + jnp.log1p(jnp.exp(-jnp.abs(raw)))
        lane = lax.broadcasted_iota(jnp.int32, dt.shape, 1)
        dt = jnp.where(lane < n_heads, dt, 0.0)
        dt_ref[...] = dt
        cum = dt * head_ref[1:2, :]
        row = lax.broadcasted_iota(jnp.int32, dt.shape, 0) % CHUNK
        shift = 1
        while shift < CHUNK:
            cum = cum + jnp.where(row >= shift, pltpu.roll(cum, shift, 0), 0.0)
            shift *= 2
        cum_ref[...] = cum

    @pl.when(step > 0)
    def _():
        xs_ref[...] = dot(h_ref[...], w_ref[...], NT).astype(BF16)


def in_proj(x_rows, gains, w_in_t, head_pad, inner, n_heads):
    tokens, dim = x_rows.shape
    tile = 1024
    n_x = inner // tile
    last = 2 * inner // tile
    out_shape = (
        jax.ShapeDtypeStruct((tokens, dim), BF16),
        jax.ShapeDtypeStruct((tokens, inner), BF16),
        jax.ShapeDtypeStruct((tokens, 256), BF16),
        jax.ShapeDtypeStruct((tokens, LANES), F32),
        jax.ShapeDtypeStruct((tokens, LANES), F32),
    )
    return pl.pallas_call(
        functools.partial(in_proj_kernel, n_heads),
        grid=(n_x + 1,),
        in_specs=[
            full_spec((tokens, dim)),
            full_spec(gains.shape),
            pl.BlockSpec((tile, dim), lambda i: (jnp.where(i == 0, last, i - 1), 0)),
            full_spec((8, LANES)),
        ],
        out_specs=(
            full_spec((tokens, dim)),
            pl.BlockSpec((tokens, tile), lambda i: (0, jnp.maximum(i - 1, 0))),
            full_spec((tokens, 256)),
            full_spec((tokens, LANES)),
            full_spec((tokens, LANES)),
        ),
        out_shape=out_shape,
        compiler_params=params(("arbitrary",), 40),
        cost_estimate=cost(2 * tokens * dim * (inner + tile), 16e6),
        name="in_proj",
    )(x_rows, gains, w_in_t, head_pad)


def z_proj_kernel(h_ref, w_ref, z_ref):
    z = dot(h_ref[...], w_ref[...], NT)
    z_ref[...] = z * jax.nn.sigmoid(z)


def z_proj(hid, w_in_t, inner):
    tokens, dim = hid.shape
    tile = 1024
    first = inner // tile
    return pl.pallas_call(
        z_proj_kernel,
        grid=(inner // tile,),
        in_specs=[full_spec((tokens, dim)), pl.BlockSpec((tile, dim), lambda i: (i + first, 0))],
        out_specs=pl.BlockSpec((tokens, tile), lambda i: (0, i)),
        out_shape=jax.ShapeDtypeStruct((tokens, inner), F32),
        compiler_params=params(("arbitrary",), 60),
        cost_estimate=cost(2 * tokens * dim * inner, 21e6),
        name="z_proj",
    )(hid, w_in_t)


STEP = 2 * CHUNK
LOG2E = math.log2(math.e)


def split3(x):
    hi = x.astype(BF16).astype(F32)
    rest = x - hi
    mid = rest.astype(BF16).astype(F32)
    low = rest - mid
    return jnp.concatenate([hi + pltpu.roll(mid, 64, 1), low], axis=1).astype(BF16)


def fill_spread(e_ref):
    rows, width = e_ref.shape
    for g in range(width // 512):
        head = lax.broadcasted_iota(jnp.int32, (rows, 512), 0) % 64
        lane = lax.broadcasted_iota(jnp.int32, (rows, 512), 1) + g * 512
        e_ref[:, g * 512:(g + 1) * 512] = jnp.where(head == lane // 64, 1.0, 0.0).astype(BF16)


def step_weights(sc_ref, seg_ref, dt, cum2):
    row = lax.broadcasted_iota(jnp.int32, (STEP, LANES), 0)
    start = doc_start(seg_ref[...], sc_ref, N_SRC) - (sc_ref[N_SRC - 1] + pl.program_id(0) * STEP)
    upper = row < CHUNK
    last = lambda v: jnp.where(upper, v[CHUNK - 1:CHUNK, :], v[STEP - 1:STEP, :])
    end_w = jnp.where(row >= last(start), jnp.exp2(last(cum2) - cum2), 0.0) * dt
    rel = jnp.where(upper, start, start - CHUNK)
    return rel, end_w


def half_rows(c):
    return slice(c * CHUNK, (c + 1) * CHUNK)


def b_transposed(bc_ref, c):
    return bc_ref[half_rows(c), :LANES].astype(F32).T.astype(BF16)


def ssd_state_kernel(sc_ref, x_ref, bc_ref, dt_ref, cum_ref, seg_ref, end_ref, decay_ref, e_ref, xp_ref, xw_ref):
    @pl.when(pl.program_id(0) == 0)
    def _():
        end_ref[...] = jnp.zeros_like(end_ref)
        decay_ref[...] = jnp.ones_like(decay_ref)
        fill_spread(e_ref)

    cum2 = cum_ref[...] * LOG2E
    rel, end_w = step_weights(sc_ref, seg_ref, dt_ref[...], cum2)
    lane = lax.broadcasted_iota(jnp.int32, (STEP, LANES), 1)
    carry = jnp.where((rel < 0) & (lane < 64), jnp.exp2(cum2), 0.0)
    ends = [jnp.broadcast_to(carry[r:r + 1, :], (8, LANES)) for r in (CHUNK - 1, STEP - 1)]
    xp_ref[...] = dot(split3(jnp.concatenate([end_w] + ends, axis=0)), e_ref[...])
    xw_ref[...] = (x_ref[...].astype(F32) * xp_ref[:STEP, :]).astype(BF16)
    add = [dot(b_transposed(bc_ref, c), xw_ref[half_rows(c), :]) for c in range(2)]
    dec = [xp_ref[STEP + 8 * c:STEP + 8 * c + 1, :] for c in range(2)]
    end_ref[...] = dec[1] * (dec[0] * end_ref[...] + add[0]) + add[1]
    decay_ref[...] = decay_ref[...] * dec[0] * dec[1]


def ssd_state(scalars, xs, bc, dt, cum, seg_wide):
    tokens, inner = xs.shape
    row = lambda width: pl.BlockSpec((STEP, width), lambda i: (i, 0))
    return pl.pallas_call(
        ssd_state_kernel,
        grid=(tokens // STEP,),
        in_specs=[SMEM_SPEC, row(inner), row(256), row(LANES), row(LANES), row(LANES)],
        out_specs=(full_spec((LANES, inner)), full_spec((1, inner))),
        out_shape=(jax.ShapeDtypeStruct((LANES, inner), F32), jax.ShapeDtypeStruct((1, inner), F32)),
        scratch_shapes=[pltpu.VMEM((256, inner), BF16), pltpu.VMEM((STEP + 16, inner), F32), pltpu.VMEM((STEP, inner), BF16)],
        compiler_params=params(("arbitrary",), 40),
        cost_estimate=cost(2 * tokens * 256 * inner, 8e6),
        name="ssd_state",
    )(scalars, xs, bc, dt, cum, seg_wide)


def ssd_full_kernel(sc_ref, x_ref, bc_ref, dt_ref, cum_ref, seg_ref, z_ref, got_ref, other_ref, pair_ref, pdecay_ref, head_ref, gain_ref, out_ref,
                    skip_ref, state_ref, y_ref, e_ref, xp_ref, xw_ref, turn_ref, pack_ref):
    @pl.when(pl.program_id(0) == 0)
    def _():
        odd = sc_ref[N_SRC + 10] == 1
        decay = jnp.where(odd, jnp.where(sc_ref[N_SRC + 11] == 1, pdecay_ref[...], 0.0), 1.0)
        half = got_ref.shape[0]
        for k, same, turned in ((0, got_ref, other_ref), (1, other_ref, got_ref)):
            rows = slice(k * half, (k + 1) * half)
            chip_in = jnp.where(odd, turned[...], same[...])
            state_ref[rows, :] = decay * chip_in + jnp.where(odd, pair_ref[rows, :], 0.0)
        fill_spread(e_ref)
        skip_ref[...] = dot(split3(head_ref[...]), e_ref[...])

    inner = x_ref.shape[1]
    n_heads = inner // 64
    dt = dt_ref[...]
    cum2 = cum_ref[...] * LOG2E
    rel, end_w = step_weights(sc_ref, seg_ref, dt, cum2)
    xp_ref[...] = dot(split3(jnp.concatenate([cum2, end_w], axis=0)), e_ref[...])
    xw_ref[...] = (x_ref[...].astype(F32) * xp_ref[STEP:, :]).astype(BF16)

    turn_ref[0] = cum2.T
    turn_ref[1] = dt.T
    left = lax.broadcasted_iota(jnp.int32, (n_heads // 2, STEP), 1) < 64
    for k in range(2):
        even = turn_ref[k, pl.ds(0, n_heads // 2, stride=2), :]
        odd = turn_ref[k, pl.ds(1, n_heads // 2, stride=2), :]
        pack_ref[0, k] = jnp.where(left, even, pltpu.roll(odd, 64, 1))
        pack_ref[1, k] = jnp.where(left, pltpu.roll(even, 64, 1), odd)

    row_id = lax.broadcasted_iota(jnp.int32, (CHUNK, LANES), 0)
    lane_id = lax.broadcasted_iota(jnp.int32, (CHUNK, LANES), 1)
    left = lane_id < 64
    src = jnp.where(left, lane_id, lane_id - 64)
    for c in range(2):
        rows = half_rows(c)
        state = state_ref[...]
        opens = rel[rows] < 0
        c_open = jnp.where(opens, bc_ref[rows, LANES:].astype(F32), 0.0).astype(BF16)
        carried = dot(c_open, state.astype(BF16))
        carry_x = jnp.exp2(xp_ref[rows, :])
        keep = jnp.where(opens[CHUNK - 1:CHUNK, :], 1.0, 0.0)
        dec = carry_x[CHUNK - 1:CHUNK, :] * jnp.concatenate([keep] * (inner // LANES), axis=1)
        y_ref[rows, :] = carried * carry_x + skip_ref[2:3, :] * x_ref[rows, :].astype(F32)
        state_ref[...] = dec * state + dot(b_transposed(bc_ref, c), xw_ref[rows, :])

    for c in range(2):
        rows = half_rows(c)
        visible = (src >= rel[rows]) & (src <= row_id)
        b_blk = bc_ref[rows, :LANES]
        scores = dot(bc_ref[rows, LANES:], jnp.concatenate([b_blk, b_blk], axis=0), NT)
        scores = jnp.where(visible, scores, 0.0)
        left16 = lax.broadcasted_iota(jnp.int32, (CHUNK, LANES), 1) < 64
        zero = jnp.zeros((CHUNK, LANES), BF16)
        for g in range(inner // 256):
            cols = slice(g * 256, (g + 1) * 256)
            mixes, diag = [], []
            for k in range(2):
                pair = 2 * g + k
                sub = slice(pair * LANES, (pair + 1) * LANES)
                cum_s = pack_ref[c, 0, pair:pair + 1, :]
                dt_s = pack_ref[c, 1, pair:pair + 1, :]
                decay = jnp.exp2(jnp.minimum(xp_ref[rows, sub] - cum_s, 0.0))
                mixes.append((scores * decay * dt_s).astype(BF16))
                xk = x_ref[rows, sub]
                for keep in (jnp.where(left16, xk, zero), jnp.where(left16, zero, xk)):
                    diag.append(jnp.concatenate([keep, zero] if k == 0 else [zero, keep], axis=1))
            y_ref[rows, cols] += dot(jnp.concatenate(mixes, axis=1), jnp.concatenate(diag, axis=0))

    y = y_ref[...]
    inv = lax.rsqrt(jnp.mean(y * y, axis=-1, keepdims=True) + NORM_EPS)
    out_ref[...] = (y * inv * gain_ref[...] * z_ref[...]).astype(BF16)


def ssd_full(scalars, xs, bc, dt, cum, seg_wide, z, got, other, pair_state, pair_decay, head_pad, gain):
    tokens, inner = xs.shape
    row = lambda width: pl.BlockSpec((STEP, width), lambda i: (i, 0))
    return pl.pallas_call(
        ssd_full_kernel,
        grid=(tokens // STEP,),
        in_specs=[
            SMEM_SPEC, row(inner), row(256), row(LANES), row(LANES), row(LANES),
            row(inner), full_spec(got.shape), full_spec(got.shape), full_spec((LANES, inner)), full_spec((1, inner)), full_spec((8, LANES)),
            full_spec((1, inner)),
        ],
        out_specs=row(inner),
        out_shape=jax.ShapeDtypeStruct((tokens, inner), BF16),
        scratch_shapes=[
            pltpu.VMEM((8, inner), F32), pltpu.VMEM((LANES, inner), F32), pltpu.VMEM((STEP, inner), F32), pltpu.VMEM((256, inner), BF16),
            pltpu.VMEM((2 * STEP, inner), F32), pltpu.VMEM((STEP, inner), BF16), pltpu.VMEM((2, LANES, STEP), F32),
            pltpu.VMEM((2, 2, inner // LANES, STEP), F32),
        ],
        compiler_params=params(("arbitrary",), 44),
        cost_estimate=cost(12e9, 20e6),
        name="ssd_full",
    )(scalars, xs, bc, dt, cum, seg_wide, z, got, other, pair_state, pair_decay, head_pad, gain)


def proj_add_kernel(a_ref, w_ref, *refs):
    out_ref = refs[-1]
    res = jnp.concatenate([r[...] for r in refs[:-1]], axis=0)
    out_ref[...] = (res.astype(F32) + dot(a_ref[...], w_ref[...])).astype(BF16)


def proj_add(a, w, res):
    tokens, depth = a.shape
    dim = w.shape[1]
    tile = 512
    col = lambda rows: pl.BlockSpec((rows, tile), lambda i: (0, i))
    return pl.pallas_call(
        proj_add_kernel,
        grid=(dim // tile,),
        in_specs=[full_spec((tokens, depth)), col(depth)] + [col(r.shape[0]) for r in res],
        out_specs=col(tokens),
        out_shape=jax.ShapeDtypeStruct((tokens, dim), BF16),
        compiler_params=params(("arbitrary",), 44),
        cost_estimate=cost(2 * tokens * depth * dim, 2 * (tokens * depth + depth * dim + 2 * tokens * dim)),
        name="proj_add",
    )(a, w, *res)


def mlp_kernel(layer, x_ref, gain_ref, wg_ref, wu_ref, wd_ref, out_ref, h_ref, acc_ref):
    step = pl.program_id(0)

    @pl.when(step == 0)
    def _():
        h_ref[...] = norm_rows(x_ref[...], gain_ref[2 * layer + 1:2 * layer + 2, :])
        acc_ref[...] = jnp.zeros_like(acc_ref)

    hid = h_ref[...]
    gate = dot(hid, wg_ref[0])
    up = dot(hid, wu_ref[0])
    act = (gate * jax.nn.sigmoid(gate) * up).astype(BF16)
    acc_ref[...] += dot(act, wd_ref[0])

    @pl.when(step == pl.num_programs(0) - 1)
    def _():
        out_ref[...] = (x_ref[...].astype(F32) + acc_ref[...]).astype(BF16)


def mlp(x_rows, gains, mlp_up, mlp_down, layer, part, parts):
    tokens, dim = x_rows.shape
    tokens //= parts
    ff = mlp_down.shape[1]
    tile = 512 * parts
    n_ff = ff // tile
    return pl.pallas_call(
        functools.partial(mlp_kernel, layer),
        grid=(n_ff,),
        in_specs=[
            pl.BlockSpec((tokens, dim), lambda i: (part, 0)),
            full_spec(gains.shape),
            pl.BlockSpec((1, dim, tile), lambda i: (layer, 0, i)),
            pl.BlockSpec((1, dim, tile), lambda i: (layer, 0, i + n_ff)),
            pl.BlockSpec((1, tile, dim), lambda i: (layer, i, 0)),
        ],
        out_specs=full_spec((tokens, dim)),
        out_shape=jax.ShapeDtypeStruct((tokens, dim), BF16),
        scratch_shapes=[pltpu.VMEM((tokens, dim), BF16), pltpu.VMEM((tokens, dim), F32)],
        compiler_params=params(("arbitrary",), 44),
        cost_estimate=cost(6 * tokens * dim * ff, 6 * dim * ff),
        name="mlp",
    )(x_rows, gains, mlp_up, mlp_up, mlp_down)


def rope_tables(positions, head_dim):
    half = head_dim // 2
    inv_freq = ROPE_BASE ** (-jnp.arange(half, dtype=F32) * 2.0 / head_dim)
    angle = positions[:, None] * inv_freq[None, :]
    cos, sin = jnp.cos(angle), jnp.sin(angle)
    return jnp.concatenate([cos, cos], axis=1), jnp.concatenate([-sin, sin], axis=1)


def qkv_kernel(n_q, n_rot, n_parts, *refs):
    x_refs = refs[:n_parts]
    gain_ref, cos_ref, sin_ref, w_ref = refs[n_parts:n_parts + 4]
    kv_ref, h_ref = refs[-2:]
    step = pl.program_id(0)

    @pl.when(step == 0)
    def _():
        first = 0
        for x_ref in x_refs:
            h_ref[first:first + x_ref.shape[0]] = norm_rows(x_ref[...], gain_ref[2:3, :])
            first += x_ref.shape[0]

    heads, _, head_dim = w_ref.shape
    turns = step < n_rot
    cos = jnp.where(turns, cos_ref[...], 1.0)
    sin = jnp.where(turns, sin_ref[...], 0.0)
    for k in range(0, heads, 2):
        out = dot(h_ref[...], jnp.concatenate([w_ref[k], w_ref[k + 1]], axis=1))
        for i in range(2):
            val = out[:, i * head_dim:(i + 1) * head_dim]
            kv_ref[k + i] = (val * cos + pltpu.roll(val, head_dim // 2, 1) * sin).astype(BF16)

    if n_q:
        @pl.when(step < n_q)
        def _():
            refs[n_parts + 4][...] = kv_ref[...]


def qkv_proj(parts, gains, cos, sin, table_part, w_heads, n_query, with_q):
    tokens = sum(x.shape[0] for x in parts)
    dim = parts[0].shape[1]
    n_heads, _, head_dim = w_heads.shape
    n_kv = n_heads - n_query
    per = 6
    n_q = n_query // per if with_q else 0
    skip = 0 if with_q else n_query // per
    n_rot = n_q + n_kv // 2 // per
    steps = n_heads // per - skip
    out_specs = [pl.BlockSpec((per, tokens, head_dim), lambda i: (jnp.maximum(i - n_q, 0), 0, 0))]
    out_shape = [jax.ShapeDtypeStruct((n_kv, tokens, head_dim), BF16)]
    if with_q:
        out_specs.insert(0, pl.BlockSpec((per, tokens, head_dim), lambda i: (jnp.minimum(i, n_q - 1), 0, 0)))
        out_shape.insert(0, jax.ShapeDtypeStruct((n_query, tokens, head_dim), BF16))
    table = pl.BlockSpec((tokens, head_dim), lambda i: (table_part, 0))
    return pl.pallas_call(
        functools.partial(qkv_kernel, n_q, n_rot, len(parts)),
        grid=(steps,),
        in_specs=[full_spec(x.shape) for x in parts] + [
            full_spec(gains.shape), table, table, pl.BlockSpec((per, dim, head_dim), lambda i: (i + skip, 0, 0)),
        ],
        out_specs=tuple(out_specs),
        out_shape=tuple(out_shape),
        scratch_shapes=[pltpu.VMEM((tokens, dim), BF16)],
        compiler_params=params(("arbitrary",), 40),
        cost_estimate=cost(2 * tokens * dim * steps * per * head_dim, 2 * dim * steps * per * head_dim + 8e6),
        name="qkv" if with_q else "kv",
    )(*parts, gains, cos, sin, w_heads)


BLOCK = 256
HEAD_GROUP = 4
N_SRC = 4
NEG = -1e30


def doc_start(seg, sc_ref, first):
    start = jnp.zeros_like(seg)
    for doc in range(4):
        start = jnp.where(seg > doc, sc_ref[first + doc], start)
    return start


def attn_kernel(sc_ref, q_ref, seg_ref, *refs):
    far_refs, near_refs = refs[:8], refs[8:12]
    o_ref, m_ref, l_ref, acc_ref, bias_ref = refs[12:]
    j = pl.program_id(1)
    heads, _, head_dim = q_ref.shape
    every = range(heads)
    scale = (head_dim ** -0.5) * math.log2(math.e)
    q0 = sc_ref[N_SRC - 1] + j * BLOCK
    first_start = doc_start(sc_ref[N_SRC + 4 + j], sc_ref, N_SRC)
    start = doc_start(seg_ref[...], sc_ref, N_SRC)

    def lanes(x, width):
        return jnp.concatenate([x] * (width // LANES), axis=1)

    def fold(x):
        return sum(x[:, i:i + LANES] for i in range(LANES, x.shape[1], LANES)) + x[:, :LANES]

    def weights(h, k_ref, rows, bias):
        s = dot(q_ref[h], k_ref[h, rows, :], NT) + bias
        return s, jnp.max(s, axis=-1, keepdims=True)

    k_ref, v_ref = near_refs[2:]
    rows = pl.ds(pl.multiple_of(j * BLOCK, BLOCK), BLOCK)
    col_id = lax.broadcasted_iota(jnp.int32, (BLOCK, BLOCK), 1)
    row_id = lax.broadcasted_iota(jnp.int32, (BLOCK, BLOCK), 0)
    bias_ref[...] = jnp.where((col_id + q0 >= lanes(start, BLOCK)) & (col_id <= row_id), 0.0, NEG)
    for h in every:
        s, top = weights(h, k_ref, rows, bias_ref[...])
        m_new = jnp.broadcast_to(top, (BLOCK, LANES))
        p = jnp.exp2((s - lanes(m_new, BLOCK)) * scale)
        m_ref[h] = m_new
        l_ref[h] = fold(p)
        acc_ref[h] = dot(p.astype(BF16), v_ref[h, rows, :])

    def update(k_ref, v_ref, rows, width, first_col):
        col = lax.broadcasted_iota(jnp.int32, (BLOCK, width), 1) + first_col
        bias = jnp.where(col >= lanes(start, width), 0.0, NEG)
        old = [(m_ref[h], l_ref[h], acc_ref[h]) for h in every]
        scored = [weights(h, k_ref, rows, bias) for h in every]
        m_new = [jnp.maximum(old[h][0], scored[h][1]) for h in every]
        p = [jnp.exp2((scored[h][0] - lanes(m_new[h], width)) * scale) for h in every]
        alpha = [jnp.exp2((old[h][0] - m_new[h]) * scale) for h in every]
        l_new = [old[h][1] * alpha[h] + fold(p[h]) for h in every]
        a_new = [old[h][2] * alpha[h] + dot(p[h].astype(BF16), v_ref[h, rows, :]) for h in every]
        for h in every:
            m_ref[h] = m_new[h]
            l_ref[h] = l_new[h]
            acc_ref[h] = a_new[h]

    for i in (1, 0):
        base = sc_ref[N_SRC - 2 + i]
        k_ref, v_ref = near_refs[2 * i], near_refs[2 * i + 1]
        lo = jnp.maximum(first_start - base, 0) // BLOCK
        hi = jnp.clip(q0 - base, 0, k_ref.shape[1]) // BLOCK

        def body(kb, carry, k_ref=k_ref, v_ref=v_ref, base=base):
            update(k_ref, v_ref, pl.ds(pl.multiple_of(kb * BLOCK, BLOCK), BLOCK), BLOCK, base + kb * BLOCK)
            return carry

        lax.fori_loop(lo, hi, body, 0)

    for i in range(4):
        k_ref, v_ref = far_refs[2 * i], far_refs[2 * i + 1]
        width = k_ref.shape[1]
        base = sc_ref[i // 2] + (i % 2) * width

        @pl.when((base < q0) & (first_start < base + width))
        def _(k_ref=k_ref, v_ref=v_ref, base=base, width=width):
            update(k_ref, v_ref, slice(None), width, base)

    for h in every:
        total = jnp.sum(l_ref[h], axis=-1, keepdims=True)
        o_ref[:, h * head_dim:(h + 1) * head_dim] = (acc_ref[h] / total).astype(BF16)


def attention(scalars, q, seg_wide, kv_list):
    n_heads, tokens, head_dim = q.shape
    per = HEAD_GROUP
    groups = n_heads // per
    in_specs = [
        pl.BlockSpec((per, BLOCK, head_dim), lambda h, j, sc: (h, j, 0)),
        pl.BlockSpec((BLOCK, LANES), lambda h, j, sc: (j, 0)),
    ]
    args = [q, seg_wide]
    for kv in kv_list:
        rows = kv.shape[1]
        in_specs.append(pl.BlockSpec((per, rows, head_dim), lambda h, j, sc: (h, 0, 0)))
        in_specs.append(pl.BlockSpec((per, rows, head_dim), lambda h, j, sc: (h + groups, 0, 0)))
        args += [kv, kv]
    return pl.pallas_call(
        attn_kernel,
        grid_spec=pltpu.PrefetchScalarGridSpec(
            num_scalar_prefetch=1,
            grid=(groups, tokens // BLOCK),
            in_specs=in_specs,
            out_specs=pl.BlockSpec((BLOCK, per * head_dim), lambda h, j, sc: (j, h)),
            scratch_shapes=[pltpu.VMEM((per, BLOCK, LANES), F32)] * 2
            + [pltpu.VMEM((per, BLOCK, head_dim), F32), pltpu.VMEM((BLOCK, BLOCK), F32)],
        ),
        out_shape=jax.ShapeDtypeStruct((tokens, n_heads * head_dim), BF16),
        compiler_params=params(("arbitrary", "arbitrary"), 40),
        cost_estimate=cost(4 * n_heads * tokens * 2 * tokens * head_dim, 20e6, n_heads * tokens * tokens),
        name="attention",
    )(scalars, *args)


def solution(mesh):
    n_dev = mesh.shape['sp']
    swap_perm = [(d, d ^ 1) for d in range(n_dev)]
    cross_perm = [(d, d + 2) for d in range(n_dev - 2)]
    row_spec = P(('dp', 'sp'), None)
    tok_spec = P(('dp', 'sp'))
    replicated = P()

    def layers(x_rows, seg_ids, norm_gains, w_in, ssm_head, y_gain, w_out, mlp_up, mlp_down, w_qkv, w_attn_out):
        dev = lax.axis_index('sp')
        tokens, dim = x_rows.shape
        inner = y_gain.shape[0]
        n_heads = ssm_head.shape[1]
        n_query, head_dim = w_attn_out.shape[:2]

        odd = (dev % 2) == 1
        counts = jnp.sum((seg_ids[None, :] <= jnp.arange(4, dtype=jnp.int32)[:, None]).astype(jnp.int32), axis=1)
        ends = jnp.stack([seg_ids[0], seg_ids[tokens - 1]])
        seg_wide = jnp.broadcast_to(seg_ids[:, None], (tokens, LANES))
        head_pad = jnp.pad(ssm_head, ((0, 5), (0, LANES - n_heads)))
        w_in_t = w_in.T
        hid, xs, bc, dt, cum = in_proj(x_rows, norm_gains, w_in_t, head_pad, inner, n_heads)
        local = jnp.pad(jnp.where(counts > 0, counts + 1, 0), (N_SRC, 8))
        local = jnp.where(jnp.arange(16) == N_SRC - 1, 1, local)
        state_end, decay = ssd_state(local, xs, bc, dt, cum, seg_wide)

        pair_state = lax.ppermute(state_end, 'sp', swap_perm)
        pair_decay = lax.ppermute(decay, 'sp', swap_perm)
        info, decay = lax.optimization_barrier((jnp.concatenate([counts, ends, ends]), decay))
        pair_info = lax.ppermute(info, 'sp', swap_perm)
        joins = jnp.where(odd, seg_ids[0] == pair_info[5], pair_info[4] == seg_ids[tokens - 1])
        half = state_end.shape[0] // 2
        first = jnp.where(odd, half, 0)
        own_half = lax.dynamic_slice_in_dim(state_end, first, half, 0)
        pair_half = lax.dynamic_slice_in_dim(pair_state, first, half, 0)
        odd_decay = jnp.where(joins, jnp.where(odd, decay, pair_decay), 0.0)
        mine = odd_decay * jnp.where(odd, pair_half, own_half) + jnp.where(odd, own_half, pair_half)
        mine, hid = lax.optimization_barrier((mine, hid))
        got = lax.ppermute(mine, 'sp', cross_perm)
        slot8 = jnp.arange(8, dtype=jnp.int32)
        chip_info = jnp.where(slot8 < 4, info + pair_info, jnp.where(odd, info, pair_info))
        far_info = lax.ppermute(chip_info, 'sp', cross_perm)
        z = z_proj(hid, w_in_t, inner)
        pos = (dev * tokens + jnp.arange(tokens)).astype(F32)
        cos, sin = rope_tables(pos, head_dim)
        cos_far, sin_far = rope_tables(pos - 2.0 * tokens, head_dim)
        got, z, cos, sin, cos_far, sin_far = lax.optimization_barrier((got, z, cos, sin, cos_far, sin_far))
        other = lax.ppermute(got, 'sp', swap_perm)

        first_pos = dev * tokens
        far = jnp.int32(1 << 24)
        pair_pos = (dev ^ 1) * tokens
        doc_starts = counts + jnp.where(odd, pair_info[:4], 0) + far_info[:4]
        slot = jnp.arange(4, dtype=jnp.int32)
        bases = jnp.where(slot == 3, first_pos, pair_pos)
        bases = jnp.where(slot >= 2, bases, jnp.where(dev >= 2, jnp.where(slot == 0, first_pos, pair_pos) - 2 * tokens, far))
        edge_seg = jnp.pad(seg_ids[::BLOCK], (0, 8 - tokens // BLOCK))
        edge_seg = jnp.where(jnp.arange(8) == 6, odd.astype(jnp.int32), edge_seg)
        edge_seg = jnp.where(jnp.arange(8) == 7, (pair_info[4] == far_info[5]).astype(jnp.int32), edge_seg)
        scalars = jnp.concatenate([bases, doc_starts, edge_seg])

        gated = ssd_full(scalars, xs, bc, dt, cum, seg_wide, z, got, other, pair_state, pair_decay, head_pad, y_gain[None, :])
        x_one = proj_add(gated, w_out, [x_rows])
        x_a = mlp(x_one, norm_gains, mlp_up, mlp_down, 0, 0, 2)
        far_a = lax.ppermute(x_a, 'sp', cross_perm)
        x_one, x_a = lax.optimization_barrier((x_one, x_a))
        x_b = mlp(x_one, norm_gains, mlp_up, mlp_down, 0, 1, 2)
        far_b = lax.ppermute(x_b, 'sp', cross_perm)
        w_heads = w_qkv.transpose(1, 0, 2)
        q, kv = qkv_proj([x_a, x_b], norm_gains, cos, sin, 0, w_heads, n_query, True)
        kv_pair = lax.ppermute(kv, 'sp', swap_perm)
        far_a, q = lax.optimization_barrier((far_a, q))
        kv_far_a, = qkv_proj([far_a], norm_gains, cos_far, sin_far, 0, w_heads, n_query, False)
        kv_fp_a = lax.ppermute(kv_far_a, 'sp', swap_perm)
        far_b, kv_far_a = lax.optimization_barrier((far_b, kv_far_a))
        kv_far_b, = qkv_proj([far_b], norm_gains, cos_far, sin_far, 1, w_heads, n_query, False)
        kv_fp_b = lax.ppermute(kv_far_b, 'sp', swap_perm)
        attn = attention(scalars, q, seg_wide, [kv_far_a, kv_far_b, kv_fp_a, kv_fp_b, kv_pair, kv])
        x_three = proj_add(attn, w_attn_out.reshape(n_query * head_dim, dim), [x_a, x_b])
        return mlp(x_three, norm_gains, mlp_up, mlp_down, 1, 0, 1)

    return jax.shard_map(layers, mesh=mesh, in_specs=(row_spec, tok_spec) + (replicated,) * 9, out_specs=row_spec, check_vma=False)
```

```python
import functools
import math

import jax
import jax.numpy as jnp
from jax import lax
from jax.experimental import pallas as pl
from jax.experimental.pallas import tpu as pltpu
from jax.sharding import PartitionSpec as P


CHUNK = 64
NORM_EPS = 1e-6
ROPE_BASE = 10000.0
LANES = 128
F32 = jnp.float32
BF16 = jnp.bfloat16
NT = (((1,), (1,)), ((), ()))


def dot(a, b, dims=(((1,), (0,)), ((), ()))):
    return lax.dot_general(a, b, dims, preferred_element_type=F32)


def params(sem, mib):
    return pltpu.CompilerParams(dimension_semantics=sem, vmem_limit_bytes=mib * 1024 * 1024)


def cost(flops, bytes_accessed, trans=0):
    return pl.CostEstimate(flops=int(flops), bytes_accessed=int(bytes_accessed), transcendentals=int(trans))


def norm_rows(values, gain):
    wide = values.astype(F32)
    inv = lax.rsqrt(jnp.mean(wide * wide, axis=-1, keepdims=True) + NORM_EPS)
    return (wide * inv * gain).astype(BF16)


SMEM_SPEC = pl.BlockSpec(memory_space=pltpu.SMEM)


def full_spec(shape):
    zeros = (0,) * len(shape)
    return pl.BlockSpec(shape, lambda *_: zeros)


def in_proj_kernel(n_heads, x_ref, gain_ref, w_ref, head_ref, h_ref, xs_ref, bc_ref, dt_ref, cum_ref):
    step = pl.program_id(0)

    @pl.when(step == 0)
    def _():
        hid = norm_rows(x_ref[...], gain_ref[0:1, :])
        h_ref[...] = hid
        n_bc = bc_ref.shape[1]
        out = dot(hid, w_ref[:n_bc + dt_ref.shape[1], :], NT)
        bc_ref[...] = out[:, :n_bc].astype(BF16)
        lanes = dt_ref.shape[1]
        raw = out[:, n_bc:n_bc + lanes] + head_ref[0:1, :]
        dt = jnp.maximum(raw, 0.0) + jnp.log1p(jnp.exp(-jnp.abs(raw)))
        lane = lax.broadcasted_iota(jnp.int32, dt.shape, 1)
        dt = jnp.where(lane < n_heads, dt, 0.0)
        dt_ref[...] = dt
        cum = dt * head_ref[1:2, :]
        row = lax.broadcasted_iota(jnp.int32, dt.shape, 0) % CHUNK
        shift = 1
        while shift < CHUNK:
            cum = cum + jnp.where(row >= shift, pltpu.roll(cum, shift, 0), 0.0)
            shift *= 2
        cum_ref[...] = cum

    @pl.when(step > 0)
    def _():
        xs_ref[...] = dot(h_ref[...], w_ref[...], NT).astype(BF16)


def in_proj(x_rows, gains, w_in_t, head_pad, inner, n_heads):
    tokens, dim = x_rows.shape
    tile = 1024
    n_x = inner // tile
    last = 2 * inner // tile
    out_shape = (
        jax.ShapeDtypeStruct((tokens, dim), BF16),
        jax.ShapeDtypeStruct((tokens, inner), BF16),
        jax.ShapeDtypeStruct((tokens, 256), BF16),
        jax.ShapeDtypeStruct((tokens, LANES), F32),
        jax.ShapeDtypeStruct((tokens, LANES), F32),
    )
    return pl.pallas_call(
        functools.partial(in_proj_kernel, n_heads),
        grid=(n_x + 1,),
        in_specs=[
            full_spec((tokens, dim)),
            full_spec(gains.shape),
            pl.BlockSpec((tile, dim), lambda i: (jnp.where(i == 0, last, i - 1), 0)),
            full_spec((8, LANES)),
        ],
        out_specs=(
            full_spec((tokens, dim)),
            pl.BlockSpec((tokens, tile), lambda i: (0, jnp.maximum(i - 1, 0))),
            full_spec((tokens, 256)),
            full_spec((tokens, LANES)),
            full_spec((tokens, LANES)),
        ),
        out_shape=out_shape,
        compiler_params=params(("arbitrary",), 52),
        cost_estimate=cost(2 * tokens * dim * (inner + tile), 16e6),
        name="in_proj",
    )(x_rows, gains, w_in_t, head_pad)


def z_proj_kernel(h_ref, w_ref, z_ref):
    z = dot(h_ref[...], w_ref[...], NT)
    z_ref[...] = z * jax.nn.sigmoid(z)


def z_proj(hid, w_in_t, inner):
    tokens, dim = hid.shape
    tile = 1024
    first = inner // tile
    return pl.pallas_call(
        z_proj_kernel,
        grid=(inner // tile,),
        in_specs=[full_spec((tokens, dim)), pl.BlockSpec((tile, dim), lambda i: (i + first, 0))],
        out_specs=pl.BlockSpec((tokens, tile), lambda i: (0, i)),
        out_shape=jax.ShapeDtypeStruct((tokens, inner), F32),
        compiler_params=params(("arbitrary",), 56),
        cost_estimate=cost(2 * tokens * dim * inner, 21e6),
        name="z_proj",
    )(hid, w_in_t)


STEP = 2 * CHUNK
LOG2E = math.log2(math.e)


def split3(x):
    hi = x.astype(BF16).astype(F32)
    rest = x - hi
    mid = rest.astype(BF16).astype(F32)
    low = rest - mid
    return jnp.concatenate([hi + pltpu.roll(mid, 64, 1), low], axis=1).astype(BF16)


def fill_spread(e_ref):
    rows, width = e_ref.shape
    for g in range(width // 512):
        head = lax.broadcasted_iota(jnp.int32, (rows, 512), 0) % 64
        lane = lax.broadcasted_iota(jnp.int32, (rows, 512), 1) + g * 512
        e_ref[:, g * 512:(g + 1) * 512] = jnp.where(head == lane // 64, 1.0, 0.0).astype(BF16)


def step_weights(sc_ref, seg_ref, dt, cum2):
    row = lax.broadcasted_iota(jnp.int32, (STEP, LANES), 0)
    start = doc_start(seg_ref[...], sc_ref, N_SRC) - (sc_ref[N_SRC - 1] + pl.program_id(0) * STEP)
    upper = row < CHUNK
    last = lambda v: jnp.where(upper, v[CHUNK - 1:CHUNK, :], v[STEP - 1:STEP, :])
    end_w = jnp.where(row >= last(start), jnp.exp2(last(cum2) - cum2), 0.0) * dt
    rel = jnp.where(upper, start, start - CHUNK)
    return rel, end_w


def half_rows(c):
    return slice(c * CHUNK, (c + 1) * CHUNK)


def b_transposed(bc_ref, c):
    return bc_ref[half_rows(c), :LANES].astype(F32).T.astype(BF16)


def ssd_state_kernel(sc_ref, x_ref, bc_ref, dt_ref, cum_ref, seg_ref, end_ref, decay_ref, e_ref, xp_ref, xw_ref):
    @pl.when(pl.program_id(0) == 0)
    def _():
        end_ref[...] = jnp.zeros_like(end_ref)
        decay_ref[...] = jnp.ones_like(decay_ref)
        fill_spread(e_ref)

    cum2 = cum_ref[...] * LOG2E
    rel, end_w = step_weights(sc_ref, seg_ref, dt_ref[...], cum2)
    lane = lax.broadcasted_iota(jnp.int32, (STEP, LANES), 1)
    carry = jnp.where((rel < 0) & (lane < 64), jnp.exp2(cum2), 0.0)
    ends = [jnp.broadcast_to(carry[r:r + 1, :], (8, LANES)) for r in (CHUNK - 1, STEP - 1)]
    xp_ref[...] = dot(split3(jnp.concatenate([end_w] + ends, axis=0)), e_ref[...])
    xw_ref[...] = (x_ref[...].astype(F32) * xp_ref[:STEP, :]).astype(BF16)
    add = [dot(b_transposed(bc_ref, c), xw_ref[half_rows(c), :]) for c in range(2)]
    dec = [xp_ref[STEP + 8 * c:STEP + 8 * c + 1, :] for c in range(2)]
    end_ref[...] = dec[1] * (dec[0] * end_ref[...] + add[0]) + add[1]
    decay_ref[...] = decay_ref[...] * dec[0] * dec[1]


def ssd_state(scalars, xs, bc, dt, cum, seg_wide):
    tokens, inner = xs.shape
    row = lambda width: pl.BlockSpec((STEP, width), lambda i: (i, 0))
    return pl.pallas_call(
        ssd_state_kernel,
        grid=(tokens // STEP,),
        in_specs=[SMEM_SPEC, row(inner), row(256), row(LANES), row(LANES), row(LANES)],
        out_specs=(full_spec((LANES, inner)), full_spec((1, inner))),
        out_shape=(jax.ShapeDtypeStruct((LANES, inner), F32), jax.ShapeDtypeStruct((1, inner), F32)),
        scratch_shapes=[pltpu.VMEM((256, inner), BF16), pltpu.VMEM((STEP + 16, inner), F32), pltpu.VMEM((STEP, inner), BF16)],
        compiler_params=params(("arbitrary",), 52),
        cost_estimate=cost(2 * tokens * 256 * inner, 8e6),
        name="ssd_state",
    )(scalars, xs, bc, dt, cum, seg_wide)


def ssd_full_kernel(sc_ref, x_ref, bc_ref, dt_ref, cum_ref, seg_ref, z_ref, got_ref, other_ref, pair_ref, pdecay_ref, head_ref, gain_ref, out_ref,
                    skip_ref, state_ref, y_ref, e_ref, xp_ref, xw_ref, turn_ref, pack_ref):
    @pl.when(pl.program_id(0) == 0)
    def _():
        odd = sc_ref[N_SRC + 7] == 1
        starts_there = jnp.int32(0)
        for k in range(N_SRC):
            starts_there += (sc_ref[N_SRC + k] == sc_ref[2]).astype(jnp.int32)
        decay = jnp.where(odd, jnp.where(starts_there == 0, pdecay_ref[...], 0.0), 1.0)
        half = got_ref.shape[0]
        for k, same, turned in ((0, got_ref, other_ref), (1, other_ref, got_ref)):
            rows = slice(k * half, (k + 1) * half)
            chip_in = jnp.where(odd, turned[...], same[...])
            state_ref[rows, :] = decay * chip_in + jnp.where(odd, pair_ref[rows, :], 0.0)
        fill_spread(e_ref)
        skip_ref[...] = dot(split3(head_ref[...]), e_ref[...])

    inner = x_ref.shape[1]
    n_heads = inner // 64
    dt = dt_ref[...]
    cum2 = cum_ref[...] * LOG2E
    rel, end_w = step_weights(sc_ref, seg_ref, dt, cum2)
    xp_ref[...] = dot(split3(jnp.concatenate([cum2, end_w], axis=0)), e_ref[...])
    xw_ref[...] = (x_ref[...].astype(F32) * xp_ref[STEP:, :]).astype(BF16)

    turn_ref[0] = cum2.T
    turn_ref[1] = dt.T
    left = lax.broadcasted_iota(jnp.int32, (n_heads // 2, STEP), 1) < 64
    for k in range(2):
        even = turn_ref[k, pl.ds(0, n_heads // 2, stride=2), :]
        odd = turn_ref[k, pl.ds(1, n_heads // 2, stride=2), :]
        pack_ref[0, k] = jnp.where(left, even, pltpu.roll(odd, 64, 1))
        pack_ref[1, k] = jnp.where(left, pltpu.roll(even, 64, 1), odd)

    row_id = lax.broadcasted_iota(jnp.int32, (CHUNK, LANES), 0)
    lane_id = lax.broadcasted_iota(jnp.int32, (CHUNK, LANES), 1)
    left = lane_id < 64
    src = jnp.where(left, lane_id, lane_id - 64)
    for c in range(2):
        rows = half_rows(c)
        state = state_ref[...]
        opens = rel[rows] < 0
        c_open = jnp.where(opens, bc_ref[rows, LANES:].astype(F32), 0.0).astype(BF16)
        carried = dot(c_open, state.astype(BF16))
        carry_x = jnp.exp2(xp_ref[rows, :])
        keep = jnp.where(opens[CHUNK - 1:CHUNK, :], 1.0, 0.0)
        dec = carry_x[CHUNK - 1:CHUNK, :] * jnp.concatenate([keep] * (inner // LANES), axis=1)
        y_ref[rows, :] = carried * carry_x + skip_ref[2:3, :] * x_ref[rows, :].astype(F32)
        state_ref[...] = dec * state + dot(b_transposed(bc_ref, c), xw_ref[rows, :])

    for c in range(2):
        rows = half_rows(c)
        visible = (src >= rel[rows]) & (src <= row_id)
        b_blk = bc_ref[rows, :LANES]
        scores = dot(bc_ref[rows, LANES:], jnp.concatenate([b_blk, b_blk], axis=0), NT)
        scores = jnp.where(visible, scores, 0.0)
        left16 = lax.broadcasted_iota(jnp.int32, (CHUNK, LANES), 1) < 64
        zero = jnp.zeros((CHUNK, LANES), BF16)
        for g in range(inner // 256):
            cols = slice(g * 256, (g + 1) * 256)
            mixes, diag = [], []
            for k in range(2):
                pair = 2 * g + k
                sub = slice(pair * LANES, (pair + 1) * LANES)
                cum_s = pack_ref[c, 0, pair:pair + 1, :]
                dt_s = pack_ref[c, 1, pair:pair + 1, :]
                decay = jnp.exp2(jnp.minimum(xp_ref[rows, sub] - cum_s, 0.0))
                mixes.append((scores * decay * dt_s).astype(BF16))
                xk = x_ref[rows, sub]
                for keep in (jnp.where(left16, xk, zero), jnp.where(left16, zero, xk)):
                    diag.append(jnp.concatenate([keep, zero] if k == 0 else [zero, keep], axis=1))
            y_ref[rows, cols] += dot(jnp.concatenate(mixes, axis=1), jnp.concatenate(diag, axis=0))

    y = y_ref[...]
    inv = lax.rsqrt(jnp.mean(y * y, axis=-1, keepdims=True) + NORM_EPS)
    out_ref[...] = (y * inv * gain_ref[...] * z_ref[...]).astype(BF16)


def ssd_full(scalars, xs, bc, dt, cum, seg_wide, z, got, other, pair_state, pair_decay, head_pad, gain):
    tokens, inner = xs.shape
    row = lambda width: pl.BlockSpec((STEP, width), lambda i: (i, 0))
    return pl.pallas_call(
        ssd_full_kernel,
        grid=(tokens // STEP,),
        in_specs=[
            SMEM_SPEC, row(inner), row(256), row(LANES), row(LANES), row(LANES),
            row(inner), full_spec(got.shape), full_spec(got.shape), full_spec((LANES, inner)), full_spec((1, inner)), full_spec((8, LANES)),
            full_spec((1, inner)),
        ],
        out_specs=row(inner),
        out_shape=jax.ShapeDtypeStruct((tokens, inner), BF16),
        scratch_shapes=[
            pltpu.VMEM((8, inner), F32), pltpu.VMEM((LANES, inner), F32), pltpu.VMEM((STEP, inner), F32), pltpu.VMEM((256, inner), BF16),
            pltpu.VMEM((2 * STEP, inner), F32), pltpu.VMEM((STEP, inner), BF16), pltpu.VMEM((2, LANES, STEP), F32),
            pltpu.VMEM((2, 2, inner // LANES, STEP), F32),
        ],
        compiler_params=params(("arbitrary",), 44),
        cost_estimate=cost(12e9, 20e6),
        name="ssd_full",
    )(scalars, xs, bc, dt, cum, seg_wide, z, got, other, pair_state, pair_decay, head_pad, gain)


def proj_add_kernel(a_ref, w_ref, *refs):
    out_ref = refs[-1]
    res = jnp.concatenate([r[...] for r in refs[:-1]], axis=0)
    out_ref[...] = (res.astype(F32) + dot(a_ref[...], w_ref[...])).astype(BF16)


def proj_add(a, w, res):
    tokens, depth = a.shape
    dim = w.shape[1]
    tile = 512
    col = lambda rows: pl.BlockSpec((rows, tile), lambda i: (0, i))
    return pl.pallas_call(
        proj_add_kernel,
        grid=(dim // tile,),
        in_specs=[full_spec((tokens, depth)), col(depth)] + [col(r.shape[0]) for r in res],
        out_specs=col(tokens),
        out_shape=jax.ShapeDtypeStruct((tokens, dim), BF16),
        compiler_params=params(("arbitrary",), 44),
        cost_estimate=cost(2 * tokens * depth * dim, 2 * (tokens * depth + depth * dim + 2 * tokens * dim)),
        name="proj_add",
    )(a, w, *res)


def mlp_kernel(layer, x_ref, gain_ref, wg_ref, wu_ref, wd_ref, out_ref, h_ref, acc_ref):
    step = pl.program_id(0)

    @pl.when(step == 0)
    def _():
        h_ref[...] = norm_rows(x_ref[...], gain_ref[2 * layer + 1:2 * layer + 2, :])
        acc_ref[...] = jnp.zeros_like(acc_ref)

    hid = h_ref[...]
    gate = dot(hid, wg_ref[0])
    up = dot(hid, wu_ref[0])
    act = (gate * jax.nn.sigmoid(gate) * up).astype(BF16)
    acc_ref[...] += dot(act, wd_ref[0])

    @pl.when(step == pl.num_programs(0) - 1)
    def _():
        out_ref[...] = (x_ref[...].astype(F32) + acc_ref[...]).astype(BF16)


def mlp(x_rows, gains, mlp_up, mlp_down, layer, part, parts):
    tokens, dim = x_rows.shape
    tokens //= parts
    ff = mlp_down.shape[1]
    tile = 512 * parts
    n_ff = ff // tile
    return pl.pallas_call(
        functools.partial(mlp_kernel, layer),
        grid=(n_ff,),
        in_specs=[
            pl.BlockSpec((tokens, dim), lambda i: (part, 0)),
            full_spec(gains.shape),
            pl.BlockSpec((1, dim, tile), lambda i: (layer, 0, i)),
            pl.BlockSpec((1, dim, tile), lambda i: (layer, 0, i + n_ff)),
            pl.BlockSpec((1, tile, dim), lambda i: (layer, i, 0)),
        ],
        out_specs=full_spec((tokens, dim)),
        out_shape=jax.ShapeDtypeStruct((tokens, dim), BF16),
        scratch_shapes=[pltpu.VMEM((tokens, dim), BF16), pltpu.VMEM((tokens, dim), F32)],
        compiler_params=params(("arbitrary",), 44),
        cost_estimate=cost(6 * tokens * dim * ff, 6 * dim * ff),
        name="mlp",
    )(x_rows, gains, mlp_up, mlp_up, mlp_down)


def rope_tables(positions, head_dim):
    half = head_dim // 2
    inv_freq = ROPE_BASE ** (-jnp.arange(half, dtype=F32) * 2.0 / head_dim)
    angle = positions[:, None] * inv_freq[None, :]
    cos, sin = jnp.cos(angle), jnp.sin(angle)
    return jnp.concatenate([cos, cos], axis=1), jnp.concatenate([-sin, sin], axis=1)


def qkv_kernel(n_q, n_rot, n_parts, *refs):
    x_refs = refs[:n_parts]
    gain_ref, cos_ref, sin_ref, w_ref = refs[n_parts:n_parts + 4]
    kv_ref, h_ref = refs[-2:]
    step = pl.program_id(0)

    @pl.when(step == 0)
    def _():
        first = 0
        for x_ref in x_refs:
            h_ref[first:first + x_ref.shape[0]] = norm_rows(x_ref[...], gain_ref[2:3, :])
            first += x_ref.shape[0]

    heads, _, head_dim = w_ref.shape
    turns = step < n_rot
    cos = jnp.where(turns, cos_ref[...], 1.0)
    sin = jnp.where(turns, sin_ref[...], 0.0)
    for k in range(0, heads, 2):
        out = dot(h_ref[...], jnp.concatenate([w_ref[k], w_ref[k + 1]], axis=1))
        for i in range(2):
            val = out[:, i * head_dim:(i + 1) * head_dim]
            kv_ref[k + i] = (val * cos + pltpu.roll(val, head_dim // 2, 1) * sin).astype(BF16)

    if n_q:
        @pl.when(step < n_q)
        def _():
            refs[n_parts + 4][...] = kv_ref[...]


def qkv_proj(parts, gains, cos, sin, table_part, w_heads, n_query, with_q):
    tokens = sum(x.shape[0] for x in parts)
    dim = parts[0].shape[1]
    n_heads, _, head_dim = w_heads.shape
    n_kv = n_heads - n_query
    per = 6
    n_q = n_query // per if with_q else 0
    skip = 0 if with_q else n_query // per
    n_rot = n_q + n_kv // 2 // per
    steps = n_heads // per - skip
    out_specs = [pl.BlockSpec((per, tokens, head_dim), lambda i: (jnp.maximum(i - n_q, 0), 0, 0))]
    out_shape = [jax.ShapeDtypeStruct((n_kv, tokens, head_dim), BF16)]
    if with_q:
        out_specs.insert(0, pl.BlockSpec((per, tokens, head_dim), lambda i: (jnp.minimum(i, n_q - 1), 0, 0)))
        out_shape.insert(0, jax.ShapeDtypeStruct((n_query, tokens, head_dim), BF16))
    table = pl.BlockSpec((tokens, head_dim), lambda i: (table_part, 0))
    return pl.pallas_call(
        functools.partial(qkv_kernel, n_q, n_rot, len(parts)),
        grid=(steps,),
        in_specs=[full_spec(x.shape) for x in parts] + [
            full_spec(gains.shape), table, table, pl.BlockSpec((per, dim, head_dim), lambda i: (i + skip, 0, 0)),
        ],
        out_specs=tuple(out_specs),
        out_shape=tuple(out_shape),
        scratch_shapes=[pltpu.VMEM((tokens, dim), BF16)],
        compiler_params=params(("arbitrary",), 40),
        cost_estimate=cost(2 * tokens * dim * steps * per * head_dim, 2 * dim * steps * per * head_dim + 8e6),
        name="qkv" if with_q else "kv",
    )(*parts, gains, cos, sin, w_heads)


BLOCK = 256
HEAD_GROUP = 4
N_SRC = 4
NEG = -1e30


def doc_start(seg, sc_ref, first):
    start = jnp.zeros_like(seg)
    for doc in range(4):
        start = jnp.where(seg > doc, sc_ref[first + doc], start)
    return start


def attn_kernel(sc_ref, q_ref, seg_ref, *refs):
    far_refs, near_refs = refs[:8], refs[8:12]
    o_ref, m_ref, l_ref, acc_ref = refs[12:]
    j = pl.program_id(1)
    heads, _, head_dim = q_ref.shape
    every = range(heads)
    scale = (head_dim ** -0.5) * math.log2(math.e)
    q0 = sc_ref[N_SRC - 1] + j * BLOCK
    first_start = doc_start(sc_ref[N_SRC + 4 + j], sc_ref, N_SRC)
    start = doc_start(seg_ref[...], sc_ref, N_SRC)

    def lanes(x, width):
        return jnp.concatenate([x] * (width // LANES), axis=1)

    def fold(x):
        return sum(x[:, i:i + LANES] for i in range(LANES, x.shape[1], LANES)) + x[:, :LANES]

    def weights(h, k_ref, rows, bias):
        s = dot(q_ref[h], k_ref[h, rows, :], NT) + bias
        return s, jnp.max(s, axis=-1, keepdims=True)

    k_ref, v_ref = near_refs[2:]
    rows = pl.ds(pl.multiple_of(j * BLOCK, BLOCK), BLOCK)
    col_id = lax.broadcasted_iota(jnp.int32, (BLOCK, BLOCK), 1)
    row_id = lax.broadcasted_iota(jnp.int32, (BLOCK, BLOCK), 0)
    bias = jnp.where((col_id + q0 >= lanes(start, BLOCK)) & (col_id <= row_id), 0.0, NEG)
    scored = [weights(h, k_ref, rows, bias) for h in every]
    tops = [jnp.broadcast_to(top, (BLOCK, LANES)) for _, top in scored]
    p = [jnp.exp2((scored[h][0] - lanes(tops[h], BLOCK)) * scale) for h in every]
    acc = [dot(p[h].astype(BF16), v_ref[h, rows, :]) for h in every]
    for h in every:
        m_ref[h] = tops[h]
        l_ref[h] = fold(p[h])
        acc_ref[h] = acc[h]

    def update(k_ref, v_ref, rows, width, first_col):
        col = lax.broadcasted_iota(jnp.int32, (BLOCK, width), 1) + first_col
        bias = jnp.where(col >= lanes(start, width), 0.0, NEG)
        old = [(m_ref[h], l_ref[h], acc_ref[h]) for h in every]
        scored = [weights(h, k_ref, rows, bias) for h in every]
        m_new = [jnp.maximum(old[h][0], scored[h][1]) for h in every]
        p = [jnp.exp2((scored[h][0] - lanes(m_new[h], width)) * scale) for h in every]
        alpha = [jnp.exp2((old[h][0] - m_new[h]) * scale) for h in every]
        l_new = [old[h][1] * alpha[h] + fold(p[h]) for h in every]
        a_new = [old[h][2] * alpha[h] + dot(p[h].astype(BF16), v_ref[h, rows, :]) for h in every]
        for h in every:
            m_ref[h] = m_new[h]
            l_ref[h] = l_new[h]
            acc_ref[h] = a_new[h]

    for i in (1, 0):
        base = sc_ref[N_SRC - 2 + i]
        k_ref, v_ref = near_refs[2 * i], near_refs[2 * i + 1]
        lo = jnp.maximum(first_start - base, 0) // BLOCK
        hi = jnp.clip(q0 - base, 0, k_ref.shape[1]) // BLOCK

        def body(kb, carry, k_ref=k_ref, v_ref=v_ref, base=base):
            update(k_ref, v_ref, pl.ds(pl.multiple_of(kb * BLOCK, BLOCK), BLOCK), BLOCK, base + kb * BLOCK)
            return carry

        lax.fori_loop(lo, hi, body, 0)

    for i in range(4):
        k_ref, v_ref = far_refs[2 * i], far_refs[2 * i + 1]
        width = k_ref.shape[1]
        base = sc_ref[i // 2] + (i % 2) * width

        @pl.when((base < q0) & (first_start < base + width))
        def _(k_ref=k_ref, v_ref=v_ref, base=base, width=width):
            update(k_ref, v_ref, slice(None), width, base)

    for h in every:
        total = jnp.sum(l_ref[h], axis=-1, keepdims=True)
        o_ref[:, h * head_dim:(h + 1) * head_dim] = (acc_ref[h] / total).astype(BF16)


def attention(scalars, q, seg_wide, kv_list):
    n_heads, tokens, head_dim = q.shape
    per = HEAD_GROUP
    groups = n_heads // per
    in_specs = [
        pl.BlockSpec((per, BLOCK, head_dim), lambda h, j, sc: (h, j, 0)),
        pl.BlockSpec((BLOCK, LANES), lambda h, j, sc: (j, 0)),
    ]
    args = [q, seg_wide]
    for kv in kv_list:
        rows = kv.shape[1]
        in_specs.append(pl.BlockSpec((per, rows, head_dim), lambda h, j, sc: (h, 0, 0)))
        in_specs.append(pl.BlockSpec((per, rows, head_dim), lambda h, j, sc: (h + groups, 0, 0)))
        args += [kv, kv]
    return pl.pallas_call(
        attn_kernel,
        grid_spec=pltpu.PrefetchScalarGridSpec(
            num_scalar_prefetch=1,
            grid=(groups, tokens // BLOCK),
            in_specs=in_specs,
            out_specs=pl.BlockSpec((BLOCK, per * head_dim), lambda h, j, sc: (j, h)),
            scratch_shapes=[pltpu.VMEM((per, BLOCK, LANES), F32)] * 2
            + [pltpu.VMEM((per, BLOCK, head_dim), F32)],
        ),
        out_shape=jax.ShapeDtypeStruct((tokens, n_heads * head_dim), BF16),
        compiler_params=params(("arbitrary", "arbitrary"), 40),
        cost_estimate=cost(4 * n_heads * tokens * 2 * tokens * head_dim, 20e6, n_heads * tokens * tokens),
        name="attention",
    )(scalars, *args)


def solution(mesh):
    n_dev = mesh.shape['sp']
    swap_perm = [(d, d ^ 1) for d in range(n_dev)]
    cross_perm = [(d, d + 2) for d in range(n_dev - 2)]
    turned_perm = [(d, (d ^ 1) + 2) for d in range(n_dev - 2)]
    row_spec = P(('dp', 'sp'), None)
    tok_spec = P(('dp', 'sp'))
    replicated = P()

    def layers(x_rows, seg_ids, norm_gains, w_in, ssm_head, y_gain, w_out, mlp_up, mlp_down, w_qkv, w_attn_out):
        dev = lax.axis_index('sp')
        tokens, dim = x_rows.shape
        inner = y_gain.shape[0]
        n_heads = ssm_head.shape[1]
        n_query, head_dim = w_attn_out.shape[:2]

        odd = (dev % 2) == 1
        counts = jnp.sum((seg_ids[None, :] <= jnp.arange(4, dtype=jnp.int32)[:, None]).astype(jnp.int32), axis=1)
        seg_wide = jnp.broadcast_to(seg_ids[:, None], (tokens, LANES))
        head_pad = jnp.pad(ssm_head, ((0, 5), (0, LANES - n_heads)))
        w_in_t = w_in.T
        hid, xs, bc, dt, cum = in_proj(x_rows, norm_gains, w_in_t, head_pad, inner, n_heads)
        counts, cum = lax.optimization_barrier((counts, cum))
        got_counts = []
        for perm in (swap_perm, cross_perm, turned_perm):
            got_counts.append(lax.ppermute(counts, 'sp', perm))
        pair_counts, *far_counts = got_counts
        local = jnp.pad(jnp.where(counts > 0, counts + 1, 0), (N_SRC, 8))
        local = jnp.where(jnp.arange(16) == N_SRC - 1, 1, local)
        state_end, decay = ssd_state(local, xs, bc, dt, cum, seg_wide)

        pair_state = lax.ppermute(state_end, 'sp', swap_perm)
        pair_decay = lax.ppermute(decay, 'sp', swap_perm)
        even_counts = jnp.where(odd, pair_counts, counts)
        odd_counts = jnp.where(odd, counts, pair_counts)
        joins = jnp.sum((even_counts < tokens).astype(jnp.int32) - (odd_counts == 0).astype(jnp.int32)) == 0
        half = state_end.shape[0] // 2
        first = jnp.where(odd, half, 0)
        own_half = lax.dynamic_slice_in_dim(state_end, first, half, 0)
        pair_half = lax.dynamic_slice_in_dim(pair_state, first, half, 0)
        odd_decay = jnp.where(joins, jnp.where(odd, decay, pair_decay), 0.0)
        mine = odd_decay * jnp.where(odd, pair_half, own_half) + jnp.where(odd, own_half, pair_half)
        mine, hid = lax.optimization_barrier((mine, hid))
        got = lax.ppermute(mine, 'sp', cross_perm)
        z = z_proj(hid, w_in_t, inner)
        pos = (dev * tokens + jnp.arange(tokens)).astype(F32)
        cos, sin = rope_tables(pos, head_dim)
        cos_far, sin_far = rope_tables(pos - 2.0 * tokens, head_dim)
        got, z, cos, sin, cos_far, sin_far = lax.optimization_barrier((got, z, cos, sin, cos_far, sin_far))
        other = lax.ppermute(got, 'sp', swap_perm)

        first_pos = dev * tokens
        far = jnp.int32(1 << 24)
        pair_pos = (dev ^ 1) * tokens
        doc_starts = counts + jnp.where(odd, pair_counts, 0) + far_counts[0] + far_counts[1]
        slot = jnp.arange(4, dtype=jnp.int32)
        bases = jnp.where(slot == 3, first_pos, pair_pos)
        bases = jnp.where(slot >= 2, bases, jnp.where(dev >= 2, jnp.where(slot == 0, first_pos, pair_pos) - 2 * tokens, far))
        edge_seg = jnp.pad(seg_ids[::BLOCK], (0, 4 - tokens // BLOCK))
        edge_seg = jnp.where(slot == 3, odd.astype(jnp.int32), edge_seg)
        scalars = jnp.concatenate([bases, doc_starts, edge_seg, jnp.zeros_like(slot)])

        gated = ssd_full(scalars, xs, bc, dt, cum, seg_wide, z, got, other, pair_state, pair_decay, head_pad, y_gain[None, :])
        x_one = proj_add(gated, w_out, [x_rows])
        x_a = mlp(x_one, norm_gains, mlp_up, mlp_down, 0, 0, 2)
        far_a = lax.ppermute(x_a, 'sp', cross_perm)
        x_one, x_a = lax.optimization_barrier((x_one, x_a))
        x_b = mlp(x_one, norm_gains, mlp_up, mlp_down, 0, 1, 2)
        far_b = lax.ppermute(x_b, 'sp', cross_perm)
        w_heads = w_qkv.transpose(1, 0, 2)
        q, kv = qkv_proj([x_a, x_b], norm_gains, cos, sin, 0, w_heads, n_query, True)
        kv_pair = lax.ppermute(kv, 'sp', swap_perm)
        far_a, q = lax.optimization_barrier((far_a, q))
        kv_far_a, = qkv_proj([far_a], norm_gains, cos_far, sin_far, 0, w_heads, n_query, False)
        kv_fp_a = lax.ppermute(kv_far_a, 'sp', swap_perm)
        far_b, kv_far_a = lax.optimization_barrier((far_b, kv_far_a))
        kv_far_b, = qkv_proj([far_b], norm_gains, cos_far, sin_far, 1, w_heads, n_query, False)
        kv_fp_b = lax.ppermute(kv_far_b, 'sp', swap_perm)
        attn = attention(scalars, q, seg_wide, [kv_far_a, kv_far_b, kv_fp_a, kv_fp_b, kv_pair, kv])
        x_three = proj_add(attn, w_attn_out.reshape(n_query * head_dim, dim), [x_a, x_b])
        return mlp(x_three, norm_gains, mlp_up, mlp_down, 1, 0, 1)

    return jax.shard_map(layers, mesh=mesh, in_specs=(row_spec, tok_spec) + (replicated,) * 9, out_specs=row_spec, check_vma=False)
```

```python
import functools
import math

import jax
import jax.numpy as jnp
from jax import lax
from jax.experimental import pallas as pl
from jax.experimental.pallas import tpu as pltpu
from jax.sharding import PartitionSpec as P


CHUNK = 64
NORM_EPS = 1e-6
ROPE_BASE = 10000.0
LANES = 128
F32 = jnp.float32
BF16 = jnp.bfloat16
NT = (((1,), (1,)), ((), ()))


def dot(a, b, dims=(((1,), (0,)), ((), ()))):
    return lax.dot_general(a, b, dims, preferred_element_type=F32)


def params(sem, mib):
    return pltpu.CompilerParams(dimension_semantics=sem, vmem_limit_bytes=mib * 1024 * 1024)


def cost(flops, bytes_accessed, trans=0):
    return pl.CostEstimate(flops=int(flops), bytes_accessed=int(bytes_accessed), transcendentals=int(trans))


def norm_rows(values, gain):
    wide = values.astype(F32)
    inv = lax.rsqrt(jnp.mean(wide * wide, axis=-1, keepdims=True) + NORM_EPS)
    return (wide * inv * gain).astype(BF16)


SMEM_SPEC = pl.BlockSpec(memory_space=pltpu.SMEM)


def full_spec(shape):
    zeros = (0,) * len(shape)
    return pl.BlockSpec(shape, lambda *_: zeros)


def in_proj_kernel(n_heads, x_ref, gain_ref, w_ref, head_ref, h_ref, xs_ref, bc_ref, dt_ref, cum_ref):
    step = pl.program_id(0)

    @pl.when(step == 0)
    def _():
        hid = norm_rows(x_ref[...], gain_ref[0:1, :])
        h_ref[...] = hid
        n_bc = bc_ref.shape[1]
        out = dot(hid, w_ref[:n_bc + dt_ref.shape[1], :], NT)
        bc_ref[...] = out[:, :n_bc].astype(BF16)
        lanes = dt_ref.shape[1]
        raw = out[:, n_bc:n_bc + lanes] + head_ref[0:1, :]
        dt = jnp.maximum(raw, 0.0) + jnp.log1p(jnp.exp(-jnp.abs(raw)))
        lane = lax.broadcasted_iota(jnp.int32, dt.shape, 1)
        dt = jnp.where(lane < n_heads, dt, 0.0)
        dt_ref[...] = dt
        cum = dt * head_ref[1:2, :]
        row = lax.broadcasted_iota(jnp.int32, dt.shape, 0) % CHUNK
        shift = 1
        while shift < CHUNK:
            cum = cum + jnp.where(row >= shift, pltpu.roll(cum, shift, 0), 0.0)
            shift *= 2
        cum_ref[...] = cum

    @pl.when(step > 0)
    def _():
        xs_ref[...] = dot(h_ref[...], w_ref[...], NT).astype(BF16)


def in_proj(x_rows, gains, w_in_t, head_pad, inner, n_heads):
    tokens, dim = x_rows.shape
    tile = 1024
    n_x = inner // tile
    last = 2 * inner // tile
    out_shape = (
        jax.ShapeDtypeStruct((tokens, dim), BF16),
        jax.ShapeDtypeStruct((tokens, inner), BF16),
        jax.ShapeDtypeStruct((tokens, 256), BF16),
        jax.ShapeDtypeStruct((tokens, LANES), F32),
        jax.ShapeDtypeStruct((tokens, LANES), F32),
    )
    return pl.pallas_call(
        functools.partial(in_proj_kernel, n_heads),
        grid=(n_x + 1,),
        in_specs=[
            full_spec((tokens, dim)),
            full_spec(gains.shape),
            pl.BlockSpec((tile, dim), lambda i: (jnp.where(i == 0, last, i - 1), 0)),
            full_spec((8, LANES)),
        ],
        out_specs=(
            full_spec((tokens, dim)),
            pl.BlockSpec((tokens, tile), lambda i: (0, jnp.maximum(i - 1, 0))),
            full_spec((tokens, 256)),
            full_spec((tokens, LANES)),
            full_spec((tokens, LANES)),
        ),
        out_shape=out_shape,
        compiler_params=params(("arbitrary",), 52),
        cost_estimate=cost(2 * tokens * dim * (inner + tile), 16e6),
        name="in_proj",
    )(x_rows, gains, w_in_t, head_pad)


def z_proj_kernel(h_ref, w_ref, z_ref):
    z = dot(h_ref[...], w_ref[...], NT)
    z_ref[...] = z * jax.nn.sigmoid(z)


def z_proj(hid, w_in_t, inner):
    tokens, dim = hid.shape
    tile = 1024
    first = inner // tile
    return pl.pallas_call(
        z_proj_kernel,
        grid=(inner // tile,),
        in_specs=[full_spec((tokens, dim)), pl.BlockSpec((tile, dim), lambda i: (i + first, 0))],
        out_specs=pl.BlockSpec((tokens, tile), lambda i: (0, i)),
        out_shape=jax.ShapeDtypeStruct((tokens, inner), F32),
        compiler_params=params(("arbitrary",), 56),
        cost_estimate=cost(2 * tokens * dim * inner, 21e6),
        name="z_proj",
    )(hid, w_in_t)


STEP = 2 * CHUNK
LOG2E = math.log2(math.e)


def split3(x):
    hi = x.astype(BF16).astype(F32)
    rest = x - hi
    mid = rest.astype(BF16).astype(F32)
    low = rest - mid
    return jnp.concatenate([hi + pltpu.roll(mid, 64, 1), low], axis=1).astype(BF16)


def fill_spread(e_ref):
    rows, width = e_ref.shape
    for g in range(width // 512):
        head = lax.broadcasted_iota(jnp.int32, (rows, 512), 0) % 64
        lane = lax.broadcasted_iota(jnp.int32, (rows, 512), 1) + g * 512
        e_ref[:, g * 512:(g + 1) * 512] = jnp.where(head == lane // 64, 1.0, 0.0).astype(BF16)


def step_weights(sc_ref, seg_ref, dt, cum2):
    row = lax.broadcasted_iota(jnp.int32, (STEP, LANES), 0)
    start = doc_start(seg_ref[...], sc_ref, N_SRC) - (sc_ref[N_SRC - 1] + pl.program_id(0) * STEP)
    upper = row < CHUNK
    last = lambda v: jnp.where(upper, v[CHUNK - 1:CHUNK, :], v[STEP - 1:STEP, :])
    end_w = jnp.where(row >= last(start), jnp.exp2(last(cum2) - cum2), 0.0) * dt
    rel = jnp.where(upper, start, start - CHUNK)
    return rel, end_w


def half_rows(c):
    return slice(c * CHUNK, (c + 1) * CHUNK)


def b_transposed(bc_ref, c):
    return bc_ref[half_rows(c), :LANES].astype(F32).T.astype(BF16)


def ssd_state_kernel(sc_ref, x_ref, bc_ref, dt_ref, cum_ref, seg_ref, end_ref, decay_ref, e_ref, xp_ref, xw_ref):
    @pl.when(pl.program_id(0) == 0)
    def _():
        end_ref[...] = jnp.zeros_like(end_ref)
        decay_ref[...] = jnp.ones_like(decay_ref)
        fill_spread(e_ref)

    cum2 = cum_ref[...] * LOG2E
    rel, end_w = step_weights(sc_ref, seg_ref, dt_ref[...], cum2)
    lane = lax.broadcasted_iota(jnp.int32, (STEP, LANES), 1)
    carry = jnp.where((rel < 0) & (lane < 64), jnp.exp2(cum2), 0.0)
    ends = [jnp.broadcast_to(carry[r:r + 1, :], (8, LANES)) for r in (CHUNK - 1, STEP - 1)]
    xp_ref[...] = dot(split3(jnp.concatenate([end_w] + ends, axis=0)), e_ref[...])
    xw_ref[...] = (x_ref[...].astype(F32) * xp_ref[:STEP, :]).astype(BF16)
    add = [dot(b_transposed(bc_ref, c), xw_ref[half_rows(c), :]) for c in range(2)]
    dec = [xp_ref[STEP + 8 * c:STEP + 8 * c + 1, :] for c in range(2)]
    end_ref[...] = dec[1] * (dec[0] * end_ref[...] + add[0]) + add[1]
    decay_ref[...] = decay_ref[...] * dec[0] * dec[1]


def ssd_state(scalars, xs, bc, dt, cum, seg_wide):
    tokens, inner = xs.shape
    row = lambda width: pl.BlockSpec((STEP, width), lambda i: (i, 0))
    return pl.pallas_call(
        ssd_state_kernel,
        grid=(tokens // STEP,),
        in_specs=[SMEM_SPEC, row(inner), row(256), row(LANES), row(LANES), row(LANES)],
        out_specs=(full_spec((LANES, inner)), full_spec((1, inner))),
        out_shape=(jax.ShapeDtypeStruct((LANES, inner), F32), jax.ShapeDtypeStruct((1, inner), F32)),
        scratch_shapes=[pltpu.VMEM((256, inner), BF16), pltpu.VMEM((STEP + 16, inner), F32), pltpu.VMEM((STEP, inner), BF16)],
        compiler_params=params(("arbitrary",), 52),
        cost_estimate=cost(2 * tokens * 256 * inner, 8e6),
        name="ssd_state",
    )(scalars, xs, bc, dt, cum, seg_wide)


def ssd_full_kernel(sc_ref, x_ref, bc_ref, dt_ref, cum_ref, seg_ref, z_ref, got_ref, other_ref, pair_ref, pdecay_ref, head_ref, gain_ref, out_ref,
                    skip_ref, state_ref, y_ref, e_ref, xp_ref, xw_ref, turn_ref, pack_ref):
    @pl.when(pl.program_id(0) == 0)
    def _():
        odd = sc_ref[N_SRC + 7] == 1
        starts_there = jnp.int32(0)
        for k in range(N_SRC):
            starts_there += (sc_ref[N_SRC + k] == sc_ref[2]).astype(jnp.int32)
        decay = jnp.where(odd, jnp.where(starts_there == 0, pdecay_ref[...], 0.0), 1.0)
        half = got_ref.shape[0]
        for k, same, turned in ((0, got_ref, other_ref), (1, other_ref, got_ref)):
            rows = slice(k * half, (k + 1) * half)
            chip_in = jnp.where(odd, turned[...], same[...])
            state_ref[rows, :] = decay * chip_in + jnp.where(odd, pair_ref[rows, :], 0.0)
        fill_spread(e_ref)
        skip_ref[...] = dot(split3(head_ref[...]), e_ref[...])

    inner = x_ref.shape[1]
    n_heads = inner // 64
    dt = dt_ref[...]
    cum2 = cum_ref[...] * LOG2E
    rel, end_w = step_weights(sc_ref, seg_ref, dt, cum2)
    xp_ref[...] = dot(split3(jnp.concatenate([cum2, end_w], axis=0)), e_ref[...])
    xw_ref[...] = (x_ref[...].astype(F32) * xp_ref[STEP:, :]).astype(BF16)

    turn_ref[0] = cum2.T
    turn_ref[1] = dt.T
    left = lax.broadcasted_iota(jnp.int32, (n_heads // 2, STEP), 1) < 64
    for k in range(2):
        even = turn_ref[k, pl.ds(0, n_heads // 2, stride=2), :]
        odd = turn_ref[k, pl.ds(1, n_heads // 2, stride=2), :]
        pack_ref[0, k] = jnp.where(left, even, pltpu.roll(odd, 64, 1))
        pack_ref[1, k] = jnp.where(left, pltpu.roll(even, 64, 1), odd)

    row_id = lax.broadcasted_iota(jnp.int32, (CHUNK, LANES), 0)
    lane_id = lax.broadcasted_iota(jnp.int32, (CHUNK, LANES), 1)
    left = lane_id < 64
    src = jnp.where(left, lane_id, lane_id - 64)
    for c in range(2):
        rows = half_rows(c)
        state = state_ref[...]
        opens = rel[rows] < 0
        c_open = jnp.where(opens, bc_ref[rows, LANES:].astype(F32), 0.0).astype(BF16)
        carried = dot(c_open, state.astype(BF16))
        carry_x = jnp.exp2(xp_ref[rows, :])
        keep = jnp.where(opens[CHUNK - 1:CHUNK, :], 1.0, 0.0)
        dec = carry_x[CHUNK - 1:CHUNK, :] * jnp.concatenate([keep] * (inner // LANES), axis=1)
        y_ref[rows, :] = carried * carry_x + skip_ref[2:3, :] * x_ref[rows, :].astype(F32)
        state_ref[...] = dec * state + dot(b_transposed(bc_ref, c), xw_ref[rows, :])

    for c in range(2):
        rows = half_rows(c)
        visible = (src >= rel[rows]) & (src <= row_id)
        b_blk = bc_ref[rows, :LANES]
        scores = dot(bc_ref[rows, LANES:], jnp.concatenate([b_blk, b_blk], axis=0), NT)
        scores = jnp.where(visible, scores, 0.0)
        left16 = lax.broadcasted_iota(jnp.int32, (CHUNK, LANES), 1) < 64
        zero = jnp.zeros((CHUNK, LANES), BF16)
        for g in range(inner // 256):
            cols = slice(g * 256, (g + 1) * 256)
            mixes, diag = [], []
            for k in range(2):
                pair = 2 * g + k
                sub = slice(pair * LANES, (pair + 1) * LANES)
                cum_s = pack_ref[c, 0, pair:pair + 1, :]
                dt_s = pack_ref[c, 1, pair:pair + 1, :]
                decay = jnp.exp2(jnp.minimum(xp_ref[rows, sub] - cum_s, 0.0))
                mixes.append((scores * decay * dt_s).astype(BF16))
                xk = x_ref[rows, sub]
                for keep in (jnp.where(left16, xk, zero), jnp.where(left16, zero, xk)):
                    diag.append(jnp.concatenate([keep, zero] if k == 0 else [zero, keep], axis=1))
            y_ref[rows, cols] += dot(jnp.concatenate(mixes, axis=1), jnp.concatenate(diag, axis=0))

    y = y_ref[...]
    inv = lax.rsqrt(jnp.mean(y * y, axis=-1, keepdims=True) + NORM_EPS)
    out_ref[...] = (y * inv * gain_ref[...] * z_ref[...]).astype(BF16)


def ssd_full(scalars, xs, bc, dt, cum, seg_wide, z, got, other, pair_state, pair_decay, head_pad, gain):
    tokens, inner = xs.shape
    row = lambda width: pl.BlockSpec((STEP, width), lambda i: (i, 0))
    return pl.pallas_call(
        ssd_full_kernel,
        grid=(tokens // STEP,),
        in_specs=[
            SMEM_SPEC, row(inner), row(256), row(LANES), row(LANES), row(LANES),
            row(inner), full_spec(got.shape), full_spec(got.shape), full_spec((LANES, inner)), full_spec((1, inner)), full_spec((8, LANES)),
            full_spec((1, inner)),
        ],
        out_specs=row(inner),
        out_shape=jax.ShapeDtypeStruct((tokens, inner), BF16),
        scratch_shapes=[
            pltpu.VMEM((8, inner), F32), pltpu.VMEM((LANES, inner), F32), pltpu.VMEM((STEP, inner), F32), pltpu.VMEM((256, inner), BF16),
            pltpu.VMEM((2 * STEP, inner), F32), pltpu.VMEM((STEP, inner), BF16), pltpu.VMEM((2, LANES, STEP), F32),
            pltpu.VMEM((2, 2, inner // LANES, STEP), F32),
        ],
        compiler_params=params(("arbitrary",), 44),
        cost_estimate=cost(12e9, 20e6),
        name="ssd_full",
    )(scalars, xs, bc, dt, cum, seg_wide, z, got, other, pair_state, pair_decay, head_pad, gain)


def proj_add_kernel(a_ref, w_ref, *refs):
    out_ref = refs[-1]
    res = jnp.concatenate([r[...] for r in refs[:-1]], axis=0)
    out_ref[...] = (res.astype(F32) + dot(a_ref[...], w_ref[...])).astype(BF16)


def proj_add(a, w, res):
    tokens, depth = a.shape
    dim = w.shape[1]
    tile = 512
    col = lambda rows: pl.BlockSpec((rows, tile), lambda i: (0, i))
    return pl.pallas_call(
        proj_add_kernel,
        grid=(dim // tile,),
        in_specs=[full_spec((tokens, depth)), col(depth)] + [col(r.shape[0]) for r in res],
        out_specs=col(tokens),
        out_shape=jax.ShapeDtypeStruct((tokens, dim), BF16),
        compiler_params=params(("arbitrary",), 44),
        cost_estimate=cost(2 * tokens * depth * dim, 2 * (tokens * depth + depth * dim + 2 * tokens * dim)),
        name="proj_add",
    )(a, w, *res)


def mlp_kernel(layer, x_ref, gain_ref, wg_ref, wu_ref, wd_ref, out_ref, h_ref, acc_ref):
    step = pl.program_id(0)

    @pl.when(step == 0)
    def _():
        h_ref[...] = norm_rows(x_ref[...], gain_ref[2 * layer + 1:2 * layer + 2, :])
        acc_ref[...] = jnp.zeros_like(acc_ref)

    hid = h_ref[...]
    gate = dot(hid, wg_ref[0])
    up = dot(hid, wu_ref[0])
    act = (gate * jax.nn.sigmoid(gate) * up).astype(BF16)
    acc_ref[...] += dot(act, wd_ref[0])

    @pl.when(step == pl.num_programs(0) - 1)
    def _():
        out_ref[...] = (x_ref[...].astype(F32) + acc_ref[...]).astype(BF16)


def mlp(x_rows, gains, mlp_up, mlp_down, layer, part, parts):
    tokens, dim = x_rows.shape
    tokens //= parts
    ff = mlp_down.shape[1]
    tile = 512 * parts
    n_ff = ff // tile
    return pl.pallas_call(
        functools.partial(mlp_kernel, layer),
        grid=(n_ff,),
        in_specs=[
            pl.BlockSpec((tokens, dim), lambda i: (part, 0)),
            full_spec(gains.shape),
            pl.BlockSpec((1, dim, tile), lambda i: (layer, 0, i)),
            pl.BlockSpec((1, dim, tile), lambda i: (layer, 0, i + n_ff)),
            pl.BlockSpec((1, tile, dim), lambda i: (layer, i, 0)),
        ],
        out_specs=full_spec((tokens, dim)),
        out_shape=jax.ShapeDtypeStruct((tokens, dim), BF16),
        scratch_shapes=[pltpu.VMEM((tokens, dim), BF16), pltpu.VMEM((tokens, dim), F32)],
        compiler_params=params(("arbitrary",), 40),
        cost_estimate=cost(6 * tokens * dim * ff, 6 * dim * ff),
        name="mlp",
    )(x_rows, gains, mlp_up, mlp_up, mlp_down)


def rope_tables(positions, head_dim):
    half = head_dim // 2
    inv_freq = ROPE_BASE ** (-jnp.arange(half, dtype=F32) * 2.0 / head_dim)
    angle = positions[:, None] * inv_freq[None, :]
    cos, sin = jnp.cos(angle), jnp.sin(angle)
    return jnp.concatenate([cos, cos], axis=1), jnp.concatenate([-sin, sin], axis=1)


def qkv_kernel(n_q, n_rot, n_parts, *refs):
    x_refs = refs[:n_parts]
    gain_ref, cos_ref, sin_ref, w_ref = refs[n_parts:n_parts + 4]
    kv_ref, h_ref = refs[-2:]
    step = pl.program_id(0)

    @pl.when(step == 0)
    def _():
        first = 0
        for x_ref in x_refs:
            h_ref[first:first + x_ref.shape[0]] = norm_rows(x_ref[...], gain_ref[2:3, :])
            first += x_ref.shape[0]

    heads, _, head_dim = w_ref.shape
    turns = step < n_rot
    cos = jnp.where(turns, cos_ref[...], 1.0)
    sin = jnp.where(turns, sin_ref[...], 0.0)
    for k in range(0, heads, 2):
        out = dot(h_ref[...], jnp.concatenate([w_ref[k], w_ref[k + 1]], axis=1))
        for i in range(2):
            val = out[:, i * head_dim:(i + 1) * head_dim]
            kv_ref[k + i] = (val * cos + pltpu.roll(val, head_dim // 2, 1) * sin).astype(BF16)

    if n_q:
        @pl.when(step < n_q)
        def _():
            refs[n_parts + 4][...] = kv_ref[...]


def qkv_proj(parts, gains, cos, sin, table_part, w_heads, n_query, with_q):
    tokens = sum(x.shape[0] for x in parts)
    dim = parts[0].shape[1]
    n_heads, _, head_dim = w_heads.shape
    n_kv = n_heads - n_query
    per = 6
    n_q = n_query // per if with_q else 0
    skip = 0 if with_q else n_query // per
    n_rot = n_q + n_kv // 2 // per
    steps = n_heads // per - skip
    out_specs = [pl.BlockSpec((per, tokens, head_dim), lambda i: (jnp.maximum(i - n_q, 0), 0, 0))]
    out_shape = [jax.ShapeDtypeStruct((n_kv, tokens, head_dim), BF16)]
    if with_q:
        out_specs.insert(0, pl.BlockSpec((per, tokens, head_dim), lambda i: (jnp.minimum(i, n_q - 1), 0, 0)))
        out_shape.insert(0, jax.ShapeDtypeStruct((n_query, tokens, head_dim), BF16))
    table = pl.BlockSpec((tokens, head_dim), lambda i: (table_part, 0))
    return pl.pallas_call(
        functools.partial(qkv_kernel, n_q, n_rot, len(parts)),
        grid=(steps,),
        in_specs=[full_spec(x.shape) for x in parts] + [
            full_spec(gains.shape), table, table, pl.BlockSpec((per, dim, head_dim), lambda i: (i + skip, 0, 0)),
        ],
        out_specs=tuple(out_specs),
        out_shape=tuple(out_shape),
        scratch_shapes=[pltpu.VMEM((tokens, dim), BF16)],
        compiler_params=params(("arbitrary",), 24),
        cost_estimate=cost(2 * tokens * dim * steps * per * head_dim, 2 * dim * steps * per * head_dim + 8e6),
        name="qkv" if with_q else "kv",
    )(*parts, gains, cos, sin, w_heads)


BLOCK = 256
HEAD_GROUP = 6
N_SRC = 4
NEG = -1e30


def doc_start(seg, sc_ref, first):
    start = jnp.zeros_like(seg)
    for doc in range(4):
        start = jnp.where(seg > doc, sc_ref[first + doc], start)
    return start


def attn_kernel(sc_ref, q_ref, seg_ref, *refs):
    far_refs, near_refs = refs[:8], refs[8:12]
    o_ref, m_ref, l_ref, acc_ref = refs[12:]
    j = pl.program_id(1)
    heads, _, head_dim = q_ref.shape
    every = range(heads)
    scale = (head_dim ** -0.5) * math.log2(math.e)
    q0 = sc_ref[N_SRC - 1] + j * BLOCK
    first_start = doc_start(sc_ref[N_SRC + 4 + j], sc_ref, N_SRC)
    start = doc_start(seg_ref[...], sc_ref, N_SRC)

    def lanes(x, width):
        return jnp.concatenate([x] * (width // LANES), axis=1)

    def fold(x):
        return sum(x[:, i:i + LANES] for i in range(LANES, x.shape[1], LANES)) + x[:, :LANES]

    def weights(h, k_ref, rows, bias):
        s = dot(q_ref[h], k_ref[h, rows, :], NT) + bias
        return s, jnp.max(s, axis=-1, keepdims=True)

    k_ref, v_ref = near_refs[2:]
    rows = pl.ds(pl.multiple_of(j * BLOCK, BLOCK), BLOCK)
    col_id = lax.broadcasted_iota(jnp.int32, (BLOCK, BLOCK), 1)
    row_id = lax.broadcasted_iota(jnp.int32, (BLOCK, BLOCK), 0)
    bias = jnp.where((col_id + q0 >= lanes(start, BLOCK)) & (col_id <= row_id), 0.0, NEG)
    scored = [weights(h, k_ref, rows, bias) for h in every]
    tops = [jnp.broadcast_to(top, (BLOCK, LANES)) for _, top in scored]
    p = [jnp.exp2((scored[h][0] - lanes(tops[h], BLOCK)) * scale) for h in every]
    acc = [dot(p[h].astype(BF16), v_ref[h, rows, :]) for h in every]
    for h in every:
        m_ref[h] = tops[h]
        l_ref[h] = fold(p[h])
        acc_ref[h] = acc[h]

    def update(k_ref, v_ref, rows, width, first_col):
        col = lax.broadcasted_iota(jnp.int32, (BLOCK, width), 1) + first_col
        bias = jnp.where(col >= lanes(start, width), 0.0, NEG)
        old = [(m_ref[h], l_ref[h], acc_ref[h]) for h in every]
        scored = [weights(h, k_ref, rows, bias) for h in every]
        m_new = [jnp.maximum(old[h][0], scored[h][1]) for h in every]
        p = [jnp.exp2((scored[h][0] - lanes(m_new[h], width)) * scale) for h in every]
        alpha = [jnp.exp2((old[h][0] - m_new[h]) * scale) for h in every]
        l_new = [old[h][1] * alpha[h] + fold(p[h]) for h in every]
        a_new = [old[h][2] * alpha[h] + dot(p[h].astype(BF16), v_ref[h, rows, :]) for h in every]
        for h in every:
            m_ref[h] = m_new[h]
            l_ref[h] = l_new[h]
            acc_ref[h] = a_new[h]

    for i in (1, 0):
        base = sc_ref[N_SRC - 2 + i]
        k_ref, v_ref = near_refs[2 * i], near_refs[2 * i + 1]
        lo = jnp.maximum(first_start - base, 0) // BLOCK
        hi = jnp.clip(q0 - base, 0, k_ref.shape[1]) // BLOCK

        def body(kb, carry, k_ref=k_ref, v_ref=v_ref, base=base):
            update(k_ref, v_ref, pl.ds(pl.multiple_of(kb * BLOCK, BLOCK), BLOCK), BLOCK, base + kb * BLOCK)
            return carry

        lax.fori_loop(lo, hi, body, 0)

    for i in range(4):
        k_ref, v_ref = far_refs[2 * i], far_refs[2 * i + 1]
        width = k_ref.shape[1]
        base = sc_ref[i // 2] + (i % 2) * width

        @pl.when((base < q0) & (first_start < base + width))
        def _(k_ref=k_ref, v_ref=v_ref, base=base, width=width):
            update(k_ref, v_ref, slice(None), width, base)

    for h in every:
        total = jnp.sum(l_ref[h], axis=-1, keepdims=True)
        o_ref[:, h * head_dim:(h + 1) * head_dim] = (acc_ref[h] / total).astype(BF16)


def attention(scalars, q, seg_wide, kv_list):
    n_heads, tokens, head_dim = q.shape
    per = HEAD_GROUP
    groups = n_heads // per
    in_specs = [
        pl.BlockSpec((per, BLOCK, head_dim), lambda h, j, sc: (h, j, 0)),
        pl.BlockSpec((BLOCK, LANES), lambda h, j, sc: (j, 0)),
    ]
    args = [q, seg_wide]
    for kv in kv_list:
        rows = kv.shape[1]
        in_specs.append(pl.BlockSpec((per, rows, head_dim), lambda h, j, sc: (h, 0, 0)))
        in_specs.append(pl.BlockSpec((per, rows, head_dim), lambda h, j, sc: (h + groups, 0, 0)))
        args += [kv, kv]
    return pl.pallas_call(
        attn_kernel,
        grid_spec=pltpu.PrefetchScalarGridSpec(
            num_scalar_prefetch=1,
            grid=(groups, tokens // BLOCK),
            in_specs=in_specs,
            out_specs=pl.BlockSpec((BLOCK, per * head_dim), lambda h, j, sc: (j, h)),
            scratch_shapes=[pltpu.VMEM((per, BLOCK, LANES), F32)] * 2
            + [pltpu.VMEM((per, BLOCK, head_dim), F32)],
        ),
        out_shape=jax.ShapeDtypeStruct((tokens, n_heads * head_dim), BF16),
        compiler_params=params(("arbitrary", "arbitrary"), 40),
        cost_estimate=cost(4 * n_heads * tokens * 2 * tokens * head_dim, 20e6, n_heads * tokens * tokens),
        name="attention",
    )(scalars, *args)


def solution(mesh):
    n_dev = mesh.shape['sp']
    swap_perm = [(d, d ^ 1) for d in range(n_dev)]
    cross_perm = [(d, d + 2) for d in range(n_dev - 2)]
    turned_perm = [(d, (d ^ 1) + 2) for d in range(n_dev - 2)]
    row_spec = P(('dp', 'sp'), None)
    tok_spec = P(('dp', 'sp'))
    replicated = P()

    def layers(x_rows, seg_ids, norm_gains, w_in, ssm_head, y_gain, w_out, mlp_up, mlp_down, w_qkv, w_attn_out):
        dev = lax.axis_index('sp')
        tokens, dim = x_rows.shape
        inner = y_gain.shape[0]
        n_heads = ssm_head.shape[1]
        n_query, head_dim = w_attn_out.shape[:2]

        odd = (dev % 2) == 1
        counts = jnp.sum((seg_ids[None, :] <= jnp.arange(4, dtype=jnp.int32)[:, None]).astype(jnp.int32), axis=1)
        seg_wide = jnp.broadcast_to(seg_ids[:, None], (tokens, LANES))
        head_pad = jnp.pad(ssm_head, ((0, 5), (0, LANES - n_heads)))
        w_in_t = w_in.T
        hid, xs, bc, dt, cum = in_proj(x_rows, norm_gains, w_in_t, head_pad, inner, n_heads)
        local = jnp.pad(jnp.where(counts > 0, counts + 1, 0), (N_SRC, 8))
        local = jnp.where(jnp.arange(16) == N_SRC - 1, 1, local)
        state_end, decay = ssd_state(local, xs, bc, dt, cum, seg_wide)

        pair_state = lax.ppermute(state_end, 'sp', swap_perm)
        pair_decay = lax.ppermute(decay, 'sp', swap_perm)
        counts, decay = lax.optimization_barrier((counts, decay))
        pair_counts = lax.ppermute(counts, 'sp', swap_perm)
        far_counts = [lax.ppermute(counts, 'sp', perm) for perm in (cross_perm, turned_perm)]
        even_counts = jnp.where(odd, pair_counts, counts)
        odd_counts = jnp.where(odd, counts, pair_counts)
        joins = jnp.sum((even_counts < tokens).astype(jnp.int32) - (odd_counts == 0).astype(jnp.int32)) == 0
        half = state_end.shape[0] // 2
        first = jnp.where(odd, half, 0)
        own_half = lax.dynamic_slice_in_dim(state_end, first, half, 0)
        pair_half = lax.dynamic_slice_in_dim(pair_state, first, half, 0)
        odd_decay = jnp.where(joins, jnp.where(odd, decay, pair_decay), 0.0)
        mine = odd_decay * jnp.where(odd, pair_half, own_half) + jnp.where(odd, own_half, pair_half)
        mine, hid = lax.optimization_barrier((mine, hid))
        got = lax.ppermute(mine, 'sp', cross_perm)
        z = z_proj(hid, w_in_t, inner)
        pos = (dev * tokens + jnp.arange(tokens)).astype(F32)
        cos, sin = rope_tables(pos, head_dim)
        cos_far, sin_far = rope_tables(pos - 2.0 * tokens, head_dim)
        got, z, cos, sin, cos_far, sin_far = lax.optimization_barrier((got, z, cos, sin, cos_far, sin_far))
        other = lax.ppermute(got, 'sp', swap_perm)

        first_pos = dev * tokens
        far = jnp.int32(1 << 24)
        pair_pos = (dev ^ 1) * tokens
        doc_starts = counts + jnp.where(odd, pair_counts, 0) + far_counts[0] + far_counts[1]
        slot = jnp.arange(4, dtype=jnp.int32)
        bases = jnp.where(slot == 3, first_pos, pair_pos)
        bases = jnp.where(slot >= 2, bases, jnp.where(dev >= 2, jnp.where(slot == 0, first_pos, pair_pos) - 2 * tokens, far))
        edge_seg = jnp.pad(seg_ids[::BLOCK], (0, 4 - tokens // BLOCK))
        edge_seg = jnp.where(slot == 3, odd.astype(jnp.int32), edge_seg)
        scalars = jnp.concatenate([bases, doc_starts, edge_seg, jnp.zeros_like(slot)])

        gated = ssd_full(scalars, xs, bc, dt, cum, seg_wide, z, got, other, pair_state, pair_decay, head_pad, y_gain[None, :])
        x_one = proj_add(gated, w_out, [x_rows])
        x_a = mlp(x_one, norm_gains, mlp_up, mlp_down, 0, 0, 2)
        far_a = lax.ppermute(x_a, 'sp', cross_perm)
        x_one, x_a = lax.optimization_barrier((x_one, x_a))
        x_b = mlp(x_one, norm_gains, mlp_up, mlp_down, 0, 1, 2)
        far_b = lax.ppermute(x_b, 'sp', cross_perm)
        w_heads = w_qkv.transpose(1, 0, 2)
        q, kv = qkv_proj([x_a, x_b], norm_gains, cos, sin, 0, w_heads, n_query, True)
        kv_pair = lax.ppermute(kv, 'sp', swap_perm)
        far_a, q = lax.optimization_barrier((far_a, q))
        kv_far_a, = qkv_proj([far_a], norm_gains, cos_far, sin_far, 0, w_heads, n_query, False)
        kv_fp_a = lax.ppermute(kv_far_a, 'sp', swap_perm)
        far_b, kv_far_a = lax.optimization_barrier((far_b, kv_far_a))
        kv_far_b, = qkv_proj([far_b], norm_gains, cos_far, sin_far, 1, w_heads, n_query, False)
        kv_fp_b = lax.ppermute(kv_far_b, 'sp', swap_perm)
        attn = attention(scalars, q, seg_wide, [kv_far_a, kv_far_b, kv_fp_a, kv_fp_b, kv_pair, kv])
        x_three = proj_add(attn, w_attn_out.reshape(n_query * head_dim, dim), [x_a, x_b])
        return mlp(x_three, norm_gains, mlp_up, mlp_down, 1, 0, 1)

    return jax.shard_map(layers, mesh=mesh, in_specs=(row_spec, tok_spec) + (replicated,) * 9, out_specs=row_spec, check_vma=False)
```

```python
import functools
import math

import jax
import jax.numpy as jnp
from jax import lax
from jax.experimental import pallas as pl
from jax.experimental.pallas import tpu as pltpu
from jax.sharding import PartitionSpec as P


CHUNK = 64
NORM_EPS = 1e-6
ROPE_BASE = 10000.0
LANES = 128
F32 = jnp.float32
BF16 = jnp.bfloat16
NT = (((1,), (1,)), ((), ()))


def dot(a, b, dims=(((1,), (0,)), ((), ()))):
    return lax.dot_general(a, b, dims, preferred_element_type=F32)


def params(sem, mib):
    return pltpu.CompilerParams(dimension_semantics=sem, vmem_limit_bytes=mib * 1024 * 1024)


def cost(flops, bytes_accessed, trans=0):
    return pl.CostEstimate(flops=int(flops), bytes_accessed=int(bytes_accessed), transcendentals=int(trans))


def norm_rows(values, gain):
    wide = values.astype(F32)
    inv = lax.rsqrt(jnp.mean(wide * wide, axis=-1, keepdims=True) + NORM_EPS)
    return (wide * inv * gain).astype(BF16)


SMEM_SPEC = pl.BlockSpec(memory_space=pltpu.SMEM)


def full_spec(shape):
    zeros = (0,) * len(shape)
    return pl.BlockSpec(shape, lambda *_: zeros)


def in_proj_kernel(n_heads, x_ref, gain_ref, w_ref, head_ref, h_ref, xs_ref, bc_ref, dt_ref, cum_ref):
    step = pl.program_id(0)

    @pl.when(step == 0)
    def _():
        hid = norm_rows(x_ref[...], gain_ref[0:1, :])
        h_ref[...] = hid
        n_bc = bc_ref.shape[1]
        out = dot(hid, w_ref[:n_bc + dt_ref.shape[1], :], NT)
        bc_ref[...] = out[:, :n_bc].astype(BF16)
        lanes = dt_ref.shape[1]
        raw = out[:, n_bc:n_bc + lanes] + head_ref[0:1, :]
        dt = jnp.maximum(raw, 0.0) + jnp.log1p(jnp.exp(-jnp.abs(raw)))
        lane = lax.broadcasted_iota(jnp.int32, dt.shape, 1)
        dt = jnp.where(lane < n_heads, dt, 0.0)
        dt_ref[...] = dt
        cum = dt * head_ref[1:2, :]
        row = lax.broadcasted_iota(jnp.int32, dt.shape, 0) % CHUNK
        shift = 1
        while shift < CHUNK:
            cum = cum + jnp.where(row >= shift, pltpu.roll(cum, shift, 0), 0.0)
            shift *= 2
        cum_ref[...] = cum

    @pl.when(step > 0)
    def _():
        xs_ref[...] = dot(h_ref[...], w_ref[...], NT).astype(BF16)


def in_proj(x_rows, gains, w_in_t, head_pad, inner, n_heads):
    tokens, dim = x_rows.shape
    tile = 1024
    n_x = inner // tile
    last = 2 * inner // tile
    out_shape = (
        jax.ShapeDtypeStruct((tokens, dim), BF16),
        jax.ShapeDtypeStruct((tokens, inner), BF16),
        jax.ShapeDtypeStruct((tokens, 256), BF16),
        jax.ShapeDtypeStruct((tokens, LANES), F32),
        jax.ShapeDtypeStruct((tokens, LANES), F32),
    )
    return pl.pallas_call(
        functools.partial(in_proj_kernel, n_heads),
        grid=(n_x + 1,),
        in_specs=[
            full_spec((tokens, dim)),
            full_spec(gains.shape),
            pl.BlockSpec((tile, dim), lambda i: (jnp.where(i == 0, last, i - 1), 0)),
            full_spec((8, LANES)),
        ],
        out_specs=(
            full_spec((tokens, dim)),
            pl.BlockSpec((tokens, tile), lambda i: (0, jnp.maximum(i - 1, 0))),
            full_spec((tokens, 256)),
            full_spec((tokens, LANES)),
            full_spec((tokens, LANES)),
        ),
        out_shape=out_shape,
        compiler_params=params(("arbitrary",), 52),
        cost_estimate=cost(2 * tokens * dim * (inner + tile), 16e6),
        name="in_proj",
    )(x_rows, gains, w_in_t, head_pad)


def z_proj_kernel(h_ref, w_ref, z_ref):
    z = dot(h_ref[...], w_ref[...], NT)
    z_ref[...] = z * jax.nn.sigmoid(z)


def z_proj(hid, w_in_t, inner):
    tokens, dim = hid.shape
    tile = 1024
    first = inner // tile
    return pl.pallas_call(
        z_proj_kernel,
        grid=(inner // tile,),
        in_specs=[full_spec((tokens, dim)), pl.BlockSpec((tile, dim), lambda i: (i + first, 0))],
        out_specs=pl.BlockSpec((tokens, tile), lambda i: (0, i)),
        out_shape=jax.ShapeDtypeStruct((tokens, inner), F32),
        compiler_params=params(("arbitrary",), 56),
        cost_estimate=cost(2 * tokens * dim * inner, 21e6),
        name="z_proj",
    )(hid, w_in_t)


STEP = 2 * CHUNK
LOG2E = math.log2(math.e)


def split3(x):
    hi = x.astype(BF16).astype(F32)
    rest = x - hi
    mid = rest.astype(BF16).astype(F32)
    low = rest - mid
    return jnp.concatenate([hi + pltpu.roll(mid, 64, 1), low], axis=1).astype(BF16)


def fill_spread(e_ref):
    rows, width = e_ref.shape
    for g in range(width // 512):
        head = lax.broadcasted_iota(jnp.int32, (rows, 512), 0) % 64
        lane = lax.broadcasted_iota(jnp.int32, (rows, 512), 1) + g * 512
        e_ref[:, g * 512:(g + 1) * 512] = jnp.where(head == lane // 64, 1.0, 0.0).astype(BF16)


def step_weights(sc_ref, seg_ref, dt, cum2):
    row = lax.broadcasted_iota(jnp.int32, (STEP, LANES), 0)
    start = doc_start(seg_ref[...], sc_ref, N_SRC) - (sc_ref[N_SRC - 1] + pl.program_id(0) * STEP)
    upper = row < CHUNK
    last = lambda v: jnp.where(upper, v[CHUNK - 1:CHUNK, :], v[STEP - 1:STEP, :])
    end_w = jnp.where(row >= last(start), jnp.exp2(last(cum2) - cum2), 0.0) * dt
    rel = jnp.where(upper, start, start - CHUNK)
    return rel, end_w


def half_rows(c):
    return slice(c * CHUNK, (c + 1) * CHUNK)


def b_transposed(bc_ref, c):
    return bc_ref[half_rows(c), :LANES].astype(F32).T.astype(BF16)


def ssd_state_kernel(sc_ref, x_ref, bc_ref, dt_ref, cum_ref, seg_ref, end_ref, decay_ref, e_ref, xp_ref, xw_ref):
    @pl.when(pl.program_id(0) == 0)
    def _():
        end_ref[...] = jnp.zeros_like(end_ref)
        decay_ref[...] = jnp.ones_like(decay_ref)
        fill_spread(e_ref)

    cum2 = cum_ref[...] * LOG2E
    rel, end_w = step_weights(sc_ref, seg_ref, dt_ref[...], cum2)
    lane = lax.broadcasted_iota(jnp.int32, (STEP, LANES), 1)
    carry = jnp.where((rel < 0) & (lane < 64), jnp.exp2(cum2), 0.0)
    ends = [jnp.broadcast_to(carry[r:r + 1, :], (8, LANES)) for r in (CHUNK - 1, STEP - 1)]
    xp_ref[...] = dot(split3(jnp.concatenate([end_w] + ends, axis=0)), e_ref[...])
    xw_ref[...] = (x_ref[...].astype(F32) * xp_ref[:STEP, :]).astype(BF16)
    add = [dot(b_transposed(bc_ref, c), xw_ref[half_rows(c), :]) for c in range(2)]
    dec = [xp_ref[STEP + 8 * c:STEP + 8 * c + 1, :] for c in range(2)]
    end_ref[...] = dec[1] * (dec[0] * end_ref[...] + add[0]) + add[1]
    decay_ref[...] = decay_ref[...] * dec[0] * dec[1]


def ssd_state(scalars, xs, bc, dt, cum, seg_wide):
    tokens, inner = xs.shape
    row = lambda width: pl.BlockSpec((STEP, width), lambda i: (i, 0))
    return pl.pallas_call(
        ssd_state_kernel,
        grid=(tokens // STEP,),
        in_specs=[SMEM_SPEC, row(inner), row(256), row(LANES), row(LANES), row(LANES)],
        out_specs=(full_spec((LANES, inner)), full_spec((1, inner))),
        out_shape=(jax.ShapeDtypeStruct((LANES, inner), F32), jax.ShapeDtypeStruct((1, inner), F32)),
        scratch_shapes=[pltpu.VMEM((256, inner), BF16), pltpu.VMEM((STEP + 16, inner), F32), pltpu.VMEM((STEP, inner), BF16)],
        compiler_params=params(("arbitrary",), 52),
        cost_estimate=cost(2 * tokens * 256 * inner, 8e6),
        name="ssd_state",
    )(scalars, xs, bc, dt, cum, seg_wide)


def ssd_full_kernel(sc_ref, x_ref, bc_ref, dt_ref, cum_ref, seg_ref, z_ref, got_ref, other_ref, pair_ref, pdecay_ref, head_ref, gain_ref, out_ref,
                    skip_ref, state_ref, y_ref, e_ref, xp_ref, xw_ref, turn_ref, pack_ref):
    @pl.when(pl.program_id(0) == 0)
    def _():
        odd = sc_ref[N_SRC + 7] == 1
        starts_there = jnp.int32(0)
        for k in range(N_SRC):
            starts_there += (sc_ref[N_SRC + k] == sc_ref[2]).astype(jnp.int32)
        decay = jnp.where(odd, jnp.where(starts_there == 0, pdecay_ref[...], 0.0), 1.0)
        half = got_ref.shape[0]
        for k, same, turned in ((0, got_ref, other_ref), (1, other_ref, got_ref)):
            rows = slice(k * half, (k + 1) * half)
            chip_in = jnp.where(odd, turned[...], same[...])
            state_ref[rows, :] = decay * chip_in + jnp.where(odd, pair_ref[rows, :], 0.0)
        fill_spread(e_ref)
        skip_ref[...] = dot(split3(head_ref[...]), e_ref[...])

    inner = x_ref.shape[1]
    n_heads = inner // 64
    dt = dt_ref[...]
    cum2 = cum_ref[...] * LOG2E
    rel, end_w = step_weights(sc_ref, seg_ref, dt, cum2)
    xp_ref[...] = dot(split3(jnp.concatenate([cum2, end_w], axis=0)), e_ref[...])
    xw_ref[...] = (x_ref[...].astype(F32) * xp_ref[STEP:, :]).astype(BF16)

    turn_ref[0] = cum2.T
    turn_ref[1] = dt.T
    left = lax.broadcasted_iota(jnp.int32, (n_heads // 2, STEP), 1) < 64
    for k in range(2):
        even = turn_ref[k, pl.ds(0, n_heads // 2, stride=2), :]
        odd = turn_ref[k, pl.ds(1, n_heads // 2, stride=2), :]
        pack_ref[0, k] = jnp.where(left, even, pltpu.roll(odd, 64, 1))
        pack_ref[1, k] = jnp.where(left, pltpu.roll(even, 64, 1), odd)

    row_id = lax.broadcasted_iota(jnp.int32, (CHUNK, LANES), 0)
    lane_id = lax.broadcasted_iota(jnp.int32, (CHUNK, LANES), 1)
    left = lane_id < 64
    src = jnp.where(left, lane_id, lane_id - 64)
    for c in range(2):
        rows = half_rows(c)
        state = state_ref[...]
        opens = rel[rows] < 0
        c_open = jnp.where(opens, bc_ref[rows, LANES:].astype(F32), 0.0).astype(BF16)
        carried = dot(c_open, state.astype(BF16))
        carry_x = jnp.exp2(xp_ref[rows, :])
        keep = jnp.where(opens[CHUNK - 1:CHUNK, :], 1.0, 0.0)
        dec = carry_x[CHUNK - 1:CHUNK, :] * jnp.concatenate([keep] * (inner // LANES), axis=1)
        y_ref[rows, :] = carried * carry_x + skip_ref[2:3, :] * x_ref[rows, :].astype(F32)
        state_ref[...] = dec * state + dot(b_transposed(bc_ref, c), xw_ref[rows, :])

    for c in range(2):
        rows = half_rows(c)
        visible = (src >= rel[rows]) & (src <= row_id)
        b_blk = bc_ref[rows, :LANES]
        scores = dot(bc_ref[rows, LANES:], jnp.concatenate([b_blk, b_blk], axis=0), NT)
        scores = jnp.where(visible, scores, 0.0)
        left16 = lax.broadcasted_iota(jnp.int32, (CHUNK, LANES), 1) < 64
        zero = jnp.zeros((CHUNK, LANES), BF16)
        for g in range(inner // 256):
            cols = slice(g * 256, (g + 1) * 256)
            mixes, diag = [], []
            for k in range(2):
                pair = 2 * g + k
                sub = slice(pair * LANES, (pair + 1) * LANES)
                cum_s = pack_ref[c, 0, pair:pair + 1, :]
                dt_s = pack_ref[c, 1, pair:pair + 1, :]
                decay = jnp.exp2(jnp.minimum(xp_ref[rows, sub] - cum_s, 0.0))
                mixes.append((scores * decay * dt_s).astype(BF16))
                xk = x_ref[rows, sub]
                for keep in (jnp.where(left16, xk, zero), jnp.where(left16, zero, xk)):
                    diag.append(jnp.concatenate([keep, zero] if k == 0 else [zero, keep], axis=1))
            y_ref[rows, cols] += dot(jnp.concatenate(mixes, axis=1), jnp.concatenate(diag, axis=0))

    y = y_ref[...]
    inv = lax.rsqrt(jnp.mean(y * y, axis=-1, keepdims=True) + NORM_EPS)
    out_ref[...] = (y * inv * gain_ref[...] * z_ref[...]).astype(BF16)


def ssd_full(scalars, xs, bc, dt, cum, seg_wide, z, got, other, pair_state, pair_decay, head_pad, gain):
    tokens, inner = xs.shape
    row = lambda width: pl.BlockSpec((STEP, width), lambda i: (i, 0))
    return pl.pallas_call(
        ssd_full_kernel,
        grid=(tokens // STEP,),
        in_specs=[
            SMEM_SPEC, row(inner), row(256), row(LANES), row(LANES), row(LANES),
            row(inner), full_spec(got.shape), full_spec(got.shape), full_spec((LANES, inner)), full_spec((1, inner)), full_spec((8, LANES)),
            full_spec((1, inner)),
        ],
        out_specs=row(inner),
        out_shape=jax.ShapeDtypeStruct((tokens, inner), BF16),
        scratch_shapes=[
            pltpu.VMEM((8, inner), F32), pltpu.VMEM((LANES, inner), F32), pltpu.VMEM((STEP, inner), F32), pltpu.VMEM((256, inner), BF16),
            pltpu.VMEM((2 * STEP, inner), F32), pltpu.VMEM((STEP, inner), BF16), pltpu.VMEM((2, LANES, STEP), F32),
            pltpu.VMEM((2, 2, inner // LANES, STEP), F32),
        ],
        compiler_params=params(("arbitrary",), 44),
        cost_estimate=cost(12e9, 20e6),
        name="ssd_full",
    )(scalars, xs, bc, dt, cum, seg_wide, z, got, other, pair_state, pair_decay, head_pad, gain)


def proj_add_kernel(a_ref, w_ref, *refs):
    out_ref = refs[-1]
    res = jnp.concatenate([r[...] for r in refs[:-1]], axis=0)
    out_ref[...] = (res.astype(F32) + dot(a_ref[...], w_ref[...])).astype(BF16)


def proj_add(a, w, res):
    tokens, depth = a.shape
    dim = w.shape[1]
    tile = 512
    col = lambda rows: pl.BlockSpec((rows, tile), lambda i: (0, i))
    return pl.pallas_call(
        proj_add_kernel,
        grid=(dim // tile,),
        in_specs=[full_spec((tokens, depth)), col(depth)] + [col(r.shape[0]) for r in res],
        out_specs=col(tokens),
        out_shape=jax.ShapeDtypeStruct((tokens, dim), BF16),
        compiler_params=params(("arbitrary",), 44),
        cost_estimate=cost(2 * tokens * depth * dim, 2 * (tokens * depth + depth * dim + 2 * tokens * dim)),
        name="proj_add",
    )(a, w, *res)


def mlp_kernel(layer, x_ref, gain_ref, wg_ref, wu_ref, wd_ref, out_ref, h_ref, acc_ref):
    step = pl.program_id(0)

    @pl.when(step == 0)
    def _():
        h_ref[...] = norm_rows(x_ref[...], gain_ref[2 * layer + 1:2 * layer + 2, :])
        acc_ref[...] = jnp.zeros_like(acc_ref)

    hid = h_ref[...]
    gate = dot(hid, wg_ref[0])
    up = dot(hid, wu_ref[0])
    act = (gate * jax.nn.sigmoid(gate) * up).astype(BF16)
    acc_ref[...] += dot(act, wd_ref[0])

    @pl.when(step == pl.num_programs(0) - 1)
    def _():
        out_ref[...] = (x_ref[...].astype(F32) + acc_ref[...]).astype(BF16)


def mlp(x_rows, gains, mlp_up, mlp_down, layer, tokens, part):
    dim = x_rows.shape[1]
    ff = mlp_down.shape[1]
    tile = 512 if tokens == x_rows.shape[0] else 1024
    n_ff = ff // tile
    return pl.pallas_call(
        functools.partial(mlp_kernel, layer),
        grid=(n_ff,),
        in_specs=[
            pl.BlockSpec((tokens, dim), lambda i: (part, 0)),
            full_spec(gains.shape),
            pl.BlockSpec((1, dim, tile), lambda i: (layer, 0, i)),
            pl.BlockSpec((1, dim, tile), lambda i: (layer, 0, i + n_ff)),
            pl.BlockSpec((1, tile, dim), lambda i: (layer, i, 0)),
        ],
        out_specs=full_spec((tokens, dim)),
        out_shape=jax.ShapeDtypeStruct((tokens, dim), BF16),
        scratch_shapes=[pltpu.VMEM((tokens, dim), BF16), pltpu.VMEM((tokens, dim), F32)],
        compiler_params=params(("arbitrary",), 40),
        cost_estimate=cost(6 * tokens * dim * ff, 6 * dim * ff),
        name="mlp",
    )(x_rows, gains, mlp_up, mlp_up, mlp_down)


def rope_tables(positions, head_dim):
    half = head_dim // 2
    inv_freq = ROPE_BASE ** (-jnp.arange(half, dtype=F32) * 2.0 / head_dim)
    angle = positions[:, None] * inv_freq[None, :]
    cos, sin = jnp.cos(angle), jnp.sin(angle)
    return jnp.concatenate([cos, cos], axis=1), jnp.concatenate([-sin, sin], axis=1)


def qkv_kernel(n_q, n_rot, n_parts, *refs):
    x_refs = refs[:n_parts]
    gain_ref, cos_ref, sin_ref, w_ref = refs[n_parts:n_parts + 4]
    kv_ref, h_ref = refs[-2:]
    step = pl.program_id(0)

    @pl.when(step == 0)
    def _():
        first = 0
        for x_ref in x_refs:
            h_ref[first:first + x_ref.shape[0]] = norm_rows(x_ref[...], gain_ref[2:3, :])
            first += x_ref.shape[0]

    heads, _, head_dim = w_ref.shape
    turns = step < n_rot
    cos = jnp.where(turns, cos_ref[...], 1.0)
    sin = jnp.where(turns, sin_ref[...], 0.0)
    for k in range(0, heads, 2):
        out = dot(h_ref[...], jnp.concatenate([w_ref[k], w_ref[k + 1]], axis=1))
        for i in range(2):
            val = out[:, i * head_dim:(i + 1) * head_dim]
            kv_ref[k + i] = (val * cos + pltpu.roll(val, head_dim // 2, 1) * sin).astype(BF16)

    if n_q:
        @pl.when(step < n_q)
        def _():
            refs[n_parts + 4][...] = kv_ref[...]


def qkv_proj(parts, gains, cos, sin, table_part, w_heads, n_query, with_q):
    tokens = sum(x.shape[0] for x in parts)
    dim = parts[0].shape[1]
    n_heads, _, head_dim = w_heads.shape
    n_kv = n_heads - n_query
    per = 6
    n_q = n_query // per if with_q else 0
    skip = 0 if with_q else n_query // per
    n_rot = n_q + n_kv // 2 // per
    steps = n_heads // per - skip
    out_specs = [pl.BlockSpec((per, tokens, head_dim), lambda i: (jnp.maximum(i - n_q, 0), 0, 0))]
    out_shape = [jax.ShapeDtypeStruct((n_kv, tokens, head_dim), BF16)]
    if with_q:
        out_specs.insert(0, pl.BlockSpec((per, tokens, head_dim), lambda i: (jnp.minimum(i, n_q - 1), 0, 0)))
        out_shape.insert(0, jax.ShapeDtypeStruct((n_query, tokens, head_dim), BF16))
    table = pl.BlockSpec((tokens, head_dim), lambda i: (table_part, 0))
    return pl.pallas_call(
        functools.partial(qkv_kernel, n_q, n_rot, len(parts)),
        grid=(steps,),
        in_specs=[full_spec(x.shape) for x in parts] + [
            full_spec(gains.shape), table, table, pl.BlockSpec((per, dim, head_dim), lambda i: (i + skip, 0, 0)),
        ],
        out_specs=tuple(out_specs),
        out_shape=tuple(out_shape),
        scratch_shapes=[pltpu.VMEM((tokens, dim), BF16)],
        compiler_params=params(("arbitrary",), 40),
        cost_estimate=cost(2 * tokens * dim * steps * per * head_dim, 2 * dim * steps * per * head_dim + 8e6),
        name="qkv" if with_q else "kv",
    )(*parts, gains, cos, sin, w_heads)


BLOCK = 256
HEAD_GROUP = 6
N_SRC = 4
NEG = -1e30


def doc_start(seg, sc_ref, first):
    start = jnp.zeros_like(seg)
    for doc in range(4):
        start = jnp.where(seg > doc, sc_ref[first + doc], start)
    return start


def attn_kernel(sc_ref, q_ref, seg_ref, *refs):
    far_refs, near_refs = refs[:8], refs[8:12]
    o_ref, m_ref, l_ref, acc_ref = refs[12:]
    j = pl.program_id(1)
    heads, _, head_dim = q_ref.shape
    every = range(heads)
    scale = (head_dim ** -0.5) * math.log2(math.e)
    q0 = sc_ref[N_SRC - 1] + j * BLOCK
    first_start = doc_start(sc_ref[N_SRC + 4 + j], sc_ref, N_SRC)
    start = doc_start(seg_ref[...], sc_ref, N_SRC)

    def lanes(x, width):
        return jnp.concatenate([x] * (width // LANES), axis=1)

    def fold(x):
        return sum(x[:, i:i + LANES] for i in range(LANES, x.shape[1], LANES)) + x[:, :LANES]

    def weights(h, k_ref, rows, bias):
        s = dot(q_ref[h], k_ref[h, rows, :], NT) + bias
        return s, jnp.max(s, axis=-1, keepdims=True)

    k_ref, v_ref = near_refs[2:]
    rows = pl.ds(pl.multiple_of(j * BLOCK, BLOCK), BLOCK)
    col_id = lax.broadcasted_iota(jnp.int32, (BLOCK, BLOCK), 1)
    row_id = lax.broadcasted_iota(jnp.int32, (BLOCK, BLOCK), 0)
    bias = jnp.where((col_id + q0 >= lanes(start, BLOCK)) & (col_id <= row_id), 0.0, NEG)
    scored = [weights(h, k_ref, rows, bias) for h in every]
    tops = [jnp.broadcast_to(top, (BLOCK, LANES)) for _, top in scored]
    p = [jnp.exp2((scored[h][0] - lanes(tops[h], BLOCK)) * scale) for h in every]
    acc = [dot(p[h].astype(BF16), v_ref[h, rows, :]) for h in every]
    for h in every:
        m_ref[h] = tops[h]
        l_ref[h] = fold(p[h])
        acc_ref[h] = acc[h]

    def update(k_ref, v_ref, rows, width, first_col):
        col = lax.broadcasted_iota(jnp.int32, (BLOCK, width), 1) + first_col
        bias = jnp.where(col >= lanes(start, width), 0.0, NEG)
        old = [(m_ref[h], l_ref[h], acc_ref[h]) for h in every]
        scored = [weights(h, k_ref, rows, bias) for h in every]
        m_new = [jnp.maximum(old[h][0], scored[h][1]) for h in every]
        p = [jnp.exp2((scored[h][0] - lanes(m_new[h], width)) * scale) for h in every]
        alpha = [jnp.exp2((old[h][0] - m_new[h]) * scale) for h in every]
        l_new = [old[h][1] * alpha[h] + fold(p[h]) for h in every]
        a_new = [old[h][2] * alpha[h] + dot(p[h].astype(BF16), v_ref[h, rows, :]) for h in every]
        for h in every:
            m_ref[h] = m_new[h]
            l_ref[h] = l_new[h]
            acc_ref[h] = a_new[h]

    for i in (1, 0):
        base = sc_ref[N_SRC - 2 + i]
        k_ref, v_ref = near_refs[2 * i], near_refs[2 * i + 1]
        lo = jnp.maximum(first_start - base, 0) // BLOCK
        hi = jnp.clip(q0 - base, 0, k_ref.shape[1]) // BLOCK

        def body(kb, carry, k_ref=k_ref, v_ref=v_ref, base=base):
            update(k_ref, v_ref, pl.ds(pl.multiple_of(kb * BLOCK, BLOCK), BLOCK), BLOCK, base + kb * BLOCK)
            return carry

        lax.fori_loop(lo, hi, body, 0)

    for i in range(4):
        k_ref, v_ref = far_refs[2 * i], far_refs[2 * i + 1]
        width = k_ref.shape[1]
        base = sc_ref[i // 2] + (i % 2) * far_refs[0].shape[1]

        @pl.when((base < q0) & (first_start < base + width))
        def _(k_ref=k_ref, v_ref=v_ref, base=base, width=width):
            update(k_ref, v_ref, slice(None), width, base)

    for h in every:
        total = jnp.sum(l_ref[h], axis=-1, keepdims=True)
        o_ref[:, h * head_dim:(h + 1) * head_dim] = (acc_ref[h] / total).astype(BF16)


def attention(scalars, q, seg_wide, kv_list):
    n_heads, tokens, head_dim = q.shape
    per = HEAD_GROUP
    groups = n_heads // per
    in_specs = [
        pl.BlockSpec((per, BLOCK, head_dim), lambda h, j, sc: (h, j, 0)),
        pl.BlockSpec((BLOCK, LANES), lambda h, j, sc: (j, 0)),
    ]
    args = [q, seg_wide]
    for kv in kv_list:
        rows = kv.shape[1]
        in_specs.append(pl.BlockSpec((per, rows, head_dim), lambda h, j, sc: (h, 0, 0)))
        in_specs.append(pl.BlockSpec((per, rows, head_dim), lambda h, j, sc: (h + groups, 0, 0)))
        args += [kv, kv]
    return pl.pallas_call(
        attn_kernel,
        grid_spec=pltpu.PrefetchScalarGridSpec(
            num_scalar_prefetch=1,
            grid=(groups, tokens // BLOCK),
            in_specs=in_specs,
            out_specs=pl.BlockSpec((BLOCK, per * head_dim), lambda h, j, sc: (j, h)),
            scratch_shapes=[pltpu.VMEM((per, BLOCK, LANES), F32)] * 2
            + [pltpu.VMEM((per, BLOCK, head_dim), F32)],
        ),
        out_shape=jax.ShapeDtypeStruct((tokens, n_heads * head_dim), BF16),
        compiler_params=params(("arbitrary", "arbitrary"), 40),
        cost_estimate=cost(4 * n_heads * tokens * 2 * tokens * head_dim, 20e6, n_heads * tokens * tokens),
        name="attention",
    )(scalars, *args)


def solution(mesh):
    n_dev = mesh.shape['sp']
    swap_perm = [(d, d ^ 1) for d in range(n_dev)]
    cross_perm = [(d, d + 2) for d in range(n_dev - 2)]
    turned_perm = [(d, (d ^ 1) + 2) for d in range(n_dev - 2)]
    row_spec = P(('dp', 'sp'), None)
    tok_spec = P(('dp', 'sp'))
    replicated = P()

    def layers(x_rows, seg_ids, norm_gains, w_in, ssm_head, y_gain, w_out, mlp_up, mlp_down, w_qkv, w_attn_out):
        dev = lax.axis_index('sp')
        tokens, dim = x_rows.shape
        inner = y_gain.shape[0]
        n_heads = ssm_head.shape[1]
        n_query, head_dim = w_attn_out.shape[:2]

        odd = (dev % 2) == 1
        counts = jnp.sum((seg_ids[None, :] <= jnp.arange(4, dtype=jnp.int32)[:, None]).astype(jnp.int32), axis=1)
        seg_wide = jnp.broadcast_to(seg_ids[:, None], (tokens, LANES))
        head_pad = jnp.pad(ssm_head, ((0, 5), (0, LANES - n_heads)))
        w_in_t = w_in.T
        hid, xs, bc, dt, cum = in_proj(x_rows, norm_gains, w_in_t, head_pad, inner, n_heads)
        local = jnp.pad(jnp.where(counts > 0, counts + 1, 0), (N_SRC, 8))
        local = jnp.where(jnp.arange(16) == N_SRC - 1, 1, local)
        state_end, decay = ssd_state(local, xs, bc, dt, cum, seg_wide)

        pair_state = lax.ppermute(state_end, 'sp', swap_perm)
        pair_decay = lax.ppermute(decay, 'sp', swap_perm)
        counts, decay = lax.optimization_barrier((counts, decay))
        pair_counts = lax.ppermute(counts, 'sp', swap_perm)
        far_counts = [lax.ppermute(counts, 'sp', perm) for perm in (cross_perm, turned_perm)]
        even_counts = jnp.where(odd, pair_counts, counts)
        odd_counts = jnp.where(odd, counts, pair_counts)
        joins = jnp.sum((even_counts < tokens).astype(jnp.int32) - (odd_counts == 0).astype(jnp.int32)) == 0
        half = state_end.shape[0] // 2
        first = jnp.where(odd, half, 0)
        own_half = lax.dynamic_slice_in_dim(state_end, first, half, 0)
        pair_half = lax.dynamic_slice_in_dim(pair_state, first, half, 0)
        odd_decay = jnp.where(joins, jnp.where(odd, decay, pair_decay), 0.0)
        mine = odd_decay * jnp.where(odd, pair_half, own_half) + jnp.where(odd, own_half, pair_half)
        mine, hid = lax.optimization_barrier((mine, hid))
        got = lax.ppermute(mine, 'sp', cross_perm)
        z = z_proj(hid, w_in_t, inner)
        pos = (dev * tokens + jnp.arange(tokens)).astype(F32)
        cos, sin = rope_tables(pos, head_dim)
        cos_far, sin_far = rope_tables(pos - 2.0 * tokens, head_dim)
        got, z, cos, sin, cos_far, sin_far = lax.optimization_barrier((got, z, cos, sin, cos_far, sin_far))
        other = lax.ppermute(got, 'sp', swap_perm)

        first_pos = dev * tokens
        far = jnp.int32(1 << 24)
        pair_pos = (dev ^ 1) * tokens
        doc_starts = counts + jnp.where(odd, pair_counts, 0) + far_counts[0] + far_counts[1]
        slot = jnp.arange(4, dtype=jnp.int32)
        bases = jnp.where(slot == 3, first_pos, pair_pos)
        bases = jnp.where(slot >= 2, bases, jnp.where(dev >= 2, jnp.where(slot == 0, first_pos, pair_pos) - 2 * tokens, far))
        edge_seg = jnp.pad(seg_ids[::BLOCK], (0, 4 - tokens // BLOCK))
        edge_seg = jnp.where(slot == 3, odd.astype(jnp.int32), edge_seg)
        scalars = jnp.concatenate([bases, doc_starts, edge_seg, jnp.zeros_like(slot)])

        gated = ssd_full(scalars, xs, bc, dt, cum, seg_wide, z, got, other, pair_state, pair_decay, head_pad, y_gain[None, :])
        x_one = proj_add(gated, w_out, [x_rows])
        x_a = mlp(x_one, norm_gains, mlp_up, mlp_down, 0, 2 * BLOCK, 0)
        far_a = lax.ppermute(x_a, 'sp', cross_perm)
        x_one, x_a = lax.optimization_barrier((x_one, x_a))
        x_b = mlp(x_one, norm_gains, mlp_up, mlp_down, 0, BLOCK, 2)
        far_b = lax.ppermute(x_b, 'sp', cross_perm)
        w_heads = w_qkv.transpose(1, 0, 2)
        q, kv = qkv_proj([x_a, x_b], norm_gains, cos, sin, 0, w_heads, n_query, True)
        kv_pair = lax.ppermute(kv, 'sp', swap_perm)
        far_a, q = lax.optimization_barrier((far_a, q))
        kv_far_a, = qkv_proj([far_a], norm_gains, cos_far, sin_far, 0, w_heads, n_query, False)
        kv_fp_a = lax.ppermute(kv_far_a, 'sp', swap_perm)
        far_b, kv_far_a = lax.optimization_barrier((far_b, kv_far_a))
        kv_far_b, = qkv_proj([far_b], norm_gains, cos_far, sin_far, 2, w_heads, n_query, False)
        kv_fp_b = lax.ppermute(kv_far_b, 'sp', swap_perm)
        attn = attention(scalars, q, seg_wide, [kv_far_a, kv_far_b, kv_fp_a, kv_fp_b, kv_pair, kv])
        x_three = proj_add(attn, w_attn_out.reshape(n_query * head_dim, dim), [x_a, x_b])
        return mlp(x_three, norm_gains, mlp_up, mlp_down, 1, tokens, 0)

    return jax.shard_map(layers, mesh=mesh, in_specs=(row_spec, tok_spec) + (replicated,) * 9, out_specs=row_spec, check_vma=False)
```
